256 devices in a mesh: gx: 4 (over x), gy: 4 (over z_hi), gz: 16 (over y, z_lo, core).
Axes of the slice: x: 4, y: 4, z: 8 (z_hi: 4, z_lo: 2; z = z_hi * 2 + z_lo), core: 2. Of those that a mesh axis runs over, the one named last changes fastest.
Arguments:
- density: float32 [32, 256, 2048], P('gx', 'gy', 'gz'), may hold values from 0.2 to 6, as said below
- momentum: float32 [3, 32, 256, 2048], P(None, 'gx', 'gy', 'gz'), may hold values from -6 to 6
- energy: float32 [32, 256, 2048], P('gx', 'gy', 'gz'), may hold values from 0.2 to 6, as said below
- displacement: int32 [3, 32, 256, 2048], P(None, 'gx', 'gy', 'gz'), may hold values from -255 to 255
- flags: int32 [6], replicated, may hold values from 0 to 1
Outputs:
- new_density: float32 [32, 256, 2048], P('gx', 'gy', 'gz')
- new_momentum: float32 [3, 32, 256, 2048], P(None, 'gx', 'gy', 'gz')
- new_energy: float32 [32, 256, 2048], P('gx', 'gy', 'gz')
- totals: float32 [2], replicated
The draws below stay inside these ranges and needn't reach their ends.
Inputs may be any that keep to these rules, and one draw needn't show every extreme that they name: density is positive. energy is positive.
All inputs are finite; a program needn't handle non-finite values.
Results may differ from the reference program's by a relative error of at most 0.0003.
Values sent between devices are 32-bit elements; how exact they have to be, the bound alone decides.
A program may use at most 64 MiB of HBM per device.

```python
import jax
import jax.numpy as jnp
from jax import lax

NX = 32
NY = 256
NZ = 2048


def rising_field(key):
    uniform_part = jax.random.uniform(key, (NX, NY, NZ), jnp.float32)
    ramp = 1.0 + 2.0 * jnp.arange(NX, dtype=jnp.float32)[:, None, None] / NX
    base = 0.5 + uniform_part
    return base * ramp


def draw_density(key, part):
    return rising_field(jax.random.fold_in(key, 11))


def draw_energy(key, part):
    return rising_field(jax.random.fold_in(key, 23))


def with_ends(entries, own_key, least, largest):
    shape = entries.shape
    spot = [jax.random.randint(jax.random.fold_in(own_key, axis), (), 0, shape[axis]) for axis in range(len(shape))]
    entries = entries.at[tuple(spot)].set(least)
    longest = shape.index(max(shape))
    spot[longest] = (spot[longest] + 1) % shape[longest]
    return entries.at[tuple(spot)].set(largest)


def shard_levels(key, shape, cuts, least, largest):
    level = 1.0
    for position, shards_of in cuts:
        draws = jax.random.uniform(jax.random.fold_in(jax.random.fold_in(key, 6), position), (shards_of,), jnp.float32, least / len(cuts), largest / len(cuts))
        level = level * jnp.repeat(jnp.exp(draws), shape[position] // shards_of).reshape((-1,) + (1,) * (len(shape) - 1 - position))
    return level


def centred(key, extent, spread, bound, split=(), held_as=jnp.bfloat16):
    level = shard_levels(key, extent, split, -0.22, 0.18) if split else 1.0
    values = jax.random.normal(key, extent, jnp.float32) * spread * level
    return jnp.minimum(jnp.maximum(values, -bound), bound).astype(held_as)


def setup_inputs(seed: int = 0) -> dict:
    streams_of = jax.random.split(jax.random.key(seed), 6)
    return {
        "density": draw_density(jax.random.fold_in(streams_of[5], 71), 0),
        "momentum": centred(streams_of[1], (3, NX, NY, NZ), 1.0, 6.0, ((1, 4), (2, 4), (3, 16)), jnp.float32),
        "energy": draw_energy(jax.random.fold_in(streams_of[5], 71), 0),
        "displacement": with_ends(jax.random.randint(streams_of[3], (3, NX, NY, NZ), -255, 256), jax.random.fold_in(streams_of[3], 1), -255, 255).astype(jnp.int32),
        "flags": with_ends(jax.random.randint(streams_of[4], (6,), 0, 2), jax.random.fold_in(streams_of[4], 1), 0, 1).astype(jnp.int32),
    }


def minmod(left_diff, right_diff):
    return 0.5 * (jnp.sign(left_diff) + jnp.sign(right_diff)) * jnp.minimum(jnp.abs(left_diff), jnp.abs(right_diff))


def flux_change(padded, face_rows, along):
    total_len = padded.shape[along]
    upper_cells = lax.slice_in_dim(padded, 2, total_len, axis=along)
    middle = lax.slice_in_dim(padded, 1, total_len - 1, axis=along)
    lower_cells = lax.slice_in_dim(padded, 0, total_len - 2, axis=along)
    slopes = minmod(upper_cells - middle, middle - lower_cells)
    k = total_len - 2
    low_val = lax.slice_in_dim(middle, 0, k - 1, axis=along)
    high_val = lax.slice_in_dim(middle, 1, k, axis=along)
    low_slope = lax.slice_in_dim(slopes, 0, k - 1, axis=along)
    high_slope = lax.slice_in_dim(slopes, 1, k, axis=along)
    fluxes = face_rows * jnp.where(face_rows > 0, low_val + 0.5 * (1.0 - face_rows) * low_slope,
                                   high_val - 0.5 * (1.0 + face_rows) * high_slope)
    m = k - 1
    return lax.slice_in_dim(fluxes, 0, m - 1, axis=along) - lax.slice_in_dim(fluxes, 1, m, axis=along)


def axis_change(values, face_speed, low_flag, high_flag, along):
    n = values.shape[along]
    first_cell = lax.slice_in_dim(values, 0, 1, axis=along)
    last_cell = lax.slice_in_dim(values, n - 1, n, axis=along)
    padded = jnp.concatenate([first_cell, first_cell, values, last_cell, last_cell], along)
    face_rows = jnp.concatenate([lax.slice_in_dim(face_speed, 0, 1, axis=along) * low_flag,
                                 lax.slice_in_dim(face_speed, 1, n, axis=along),
                                 lax.slice_in_dim(face_speed, n - 1, n, axis=along) * high_flag], along)
    return flux_change(padded, face_rows, along)


def reference(density, momentum, energy, displacement, flags):
    face_speed = displacement.astype(jnp.float32) / 256.0
    flag_open = flags.astype(jnp.float32)

    def remap_field(values):
        updated = values
        for along in range(3):
            updated = updated + axis_change(values, face_speed[along], flag_open[2 * along], flag_open[2 * along + 1], along)
        return updated

    new_density = remap_field(density)
    new_momentum = jnp.stack([remap_field(momentum[comp]) for comp in range(3)])
    new_energy = remap_field(energy)
    cell_total = float(NX * NY * NZ)
    totals = jnp.stack([jnp.sum(new_density), jnp.sum(new_energy)]) / cell_total
    return new_density, new_momentum, new_energy, totals
```

```python
import functools

import jax
import jax.numpy as jnp
from jax import lax
from jax.experimental import pallas as pl
from jax.experimental.pallas import tpu as pltpu
from jax.sharding import PartitionSpec as P

MESH = pl.DeviceIdType.MESH
STEP = 1.0 / 256.0


def minmod(left_diff, right_diff):
    least = jnp.minimum(left_diff, right_diff)
    most = jnp.maximum(left_diff, right_diff)
    return jnp.maximum(least, jnp.minimum(most, 0.0))


def half_weight(v):
    size = jnp.abs(v)
    return 0.5 * size * (1.0 - size)


def shift_down(block, first_row):
    moved = pltpu.roll(block, 1, 0)
    row = lax.broadcasted_iota(jnp.int32, (8, 128), 0)
    top = jnp.where(row == 0, first_row, moved[:8])
    return jnp.concatenate([top, moved[8:]], 0)


def shift_up(block, last_row):
    n = block.shape[0]
    moved = pltpu.roll(block, n - 1, 0)
    row = lax.broadcasted_iota(jnp.int32, (8, 128), 0)
    bottom = jnp.where(row == 7, last_row, moved[n - 8 :])
    return jnp.concatenate([moved[: n - 8], bottom], 0)


def back(block):
    return pltpu.roll(block, 1, 1)


def ahead(block):
    return pltpu.roll(block, 127, 1)


def kernel(
    cells,
    density,
    momentum,
    energy,
    displacement,
    flags,
    new_density,
    new_momentum,
    new_energy,
    totals,
    q,
    disp,
    flag,
    acc,
    vx,
    gx_w,
    xlow,
    xhigh,
    xface,
    yup,
    ydown,
    ylow,
    yhigh,
    yedge,
    zpack,
    zlow,
    zhigh,
    zslope,
    zflow,
    zface,
    part,
    slots_a,
    slots_b,
    slots_c,
    load_sem,
    out_sem,
    xs_sem,
    xr_sem,
    ys_sem,
    yr_sem,
    zs_sem,
    zr_sem,
    ts_sem,
    tr_sem,
):
    px, py, pz = lax.axis_index("gx"), lax.axis_index("gy"), lax.axis_index("gz")
    nx, ny, nz = lax.axis_size("gx"), lax.axis_size("gy"), lax.axis_size("gz")
    core = pz % 2
    zl = (pz // 2) % 2
    field_in = [density, momentum.at[0], momentum.at[1], momentum.at[2], energy]
    field_out = [new_density, new_momentum.at[0], new_momentum.at[1], new_momentum.at[2], new_energy]

    flag_copy = pltpu.make_async_copy(flags, flag, load_sem.at[8])
    flag_copy.start()
    loads = [pltpu.make_async_copy(field_in[f], q.at[f], load_sem.at[f]) for f in range(5)]
    disp_loads = [
        pltpu.make_async_copy(displacement.at[a], disp.at[a], load_sem.at[5 + a]) for a in range(3)
    ]
    loads[0].start()
    loads[4].start()
    for copy in disp_loads:
        copy.start()
    for f in (1, 2, 3):
        loads[f].start()

    def place(x=None, y=None, z=None):
        target = {}
        if x is not None:
            target["gx"] = x
        if y is not None:
            target["gy"] = y
        if z is not None:
            target["gz"] = z
        return target

    def along_z(step):
        chip = lax.rem(py * 2 + zl + step, 2 * ny)
        return place(y=chip // 2, z=pz + 2 * (chip % 2 - zl))

    stage_a = [
        place(x=lax.rem(px + dx, nx), z=pz + dc * (1 - 2 * core))
        for dc in range(2)
        for dx in range(4)
        if dx or dc
    ]
    stage_b = [place(z=lax.rem(pz + 4 * dy, nz)) for dy in range(1, 4)]
    stage_c = [along_z(step) for step in range(1, 8)]
    across = place(z=lax.rem(pz + nz + 2 * core - 1, nz))
    near = stage_a + stage_b + [along_z(step) for step in (1, 2, 6, 7)] + [across]

    barrier = pltpu.get_barrier_semaphore()
    for peer in near:
        pl.semaphore_signal(barrier, inc=1, device_id=peer, device_id_type=MESH)

    flag_copy.wait()
    loads[0].wait()
    loads[4].wait()
    for copy in disp_loads:
        copy.wait()

    flag_open = [flag[i].astype(jnp.float32) for i in range(6)]
    first = [px == 0, py == 0, pz == 0]
    final = [px == nx - 1, py == ny - 1, pz == nz - 1]
    low_scale = [jnp.where(first[a], flag_open[2 * a], 1.0) for a in range(3)]
    gain = [jnp.where(first[a], flag_open[2 * a] * STEP, 0.0) for a in range(3)]
    loss = [jnp.where(final[a], flag_open[2 * a + 1] * -STEP, 0.0) for a in range(3)]

    rows = lax.broadcasted_iota(jnp.int32, (64, 128), 0)
    lanes = lax.broadcasted_iota(jnp.int32, (64, 128), 1)
    weight_y = jnp.where(rows == 0, gain[1], jnp.where(rows == 63, loss[1], 0.0))
    weight_z = jnp.where(lanes == 0, gain[2], jnp.where(lanes == 127, loss[2], 0.0))

    def fold(block):
        return jnp.sum(block.reshape(8, 8, 128), axis=0)

    def plane_sum(x, sums):
        weight = (
            1.0
            + weight_y * disp[1, x].astype(jnp.float32)
            + weight_z * disp[2, x].astype(jnp.float32)
        )
        return (sums[0] + fold(q[0, x] * weight), sums[1] + fold(q[4, x] * weight))

    weight_low = gain[0] * disp[0, 0].astype(jnp.float32)
    weight_high = loss[0] * disp[0, 7].astype(jnp.float32)
    sums = tuple(fold(q[f, 0] * weight_low + q[f, 7] * weight_high) for f in (0, 4))
    sums = lax.fori_loop(0, 8, plane_sum, sums)
    row8 = lax.broadcasted_iota(jnp.int32, (8, 128), 0)
    part[0] = jnp.where(
        row8 == 0,
        jnp.sum(sums[0], axis=0, keepdims=True),
        jnp.where(row8 == 1, jnp.sum(sums[1], axis=0, keepdims=True), 0.0),
    )
    for f in (1, 2, 3):
        loads[f].wait()

    pl.semaphore_wait(barrier, len(near))

    def total_copies(stage, peers, slots, base):
        return [
            pltpu.make_async_remote_copy(
                src_ref=part.at[stage],
                dst_ref=slots.at[i],
                send_sem=ts_sem.at[base + i],
                recv_sem=tr_sem.at[base + i],
                device_id=peer,
                device_id_type=MESH,
            )
            for i, peer in enumerate(peers)
        ]

    copies_a = total_copies(0, stage_a, slots_a, 0)
    copies_b = total_copies(1, stage_b, slots_b, 7)
    copies_c = total_copies(2, stage_c, slots_c, 10)
    for copy in copies_a:
        copy.start()

    def remote(src, dst, send_sem, recv_sem, peer):
        return pltpu.make_async_remote_copy(
            src_ref=src,
            dst_ref=dst,
            send_sem=send_sem,
            recv_sem=recv_sem,
            device_id=peer,
            device_id_type=MESH,
        )

    x_next = place(x=lax.rem(px + 1, nx))
    x_prev = place(x=lax.rem(px + nx - 1, nx))
    face_copy = remote(disp.at[0, 0], xface, xs_sem.at[10], xr_sem.at[10], x_prev)
    up_copies = [
        remote(q.at[f, pl.ds(6, 2)], xlow.at[f], xs_sem.at[f], xr_sem.at[f], x_next) for f in range(5)
    ]
    down_copies = [
        remote(q.at[f, pl.ds(0, 2)], xhigh.at[f], xs_sem.at[5 + f], xr_sem.at[5 + f], x_prev)
        for f in range(5)
    ]

    @pl.when(jnp.logical_not(first[0]))
    def _():
        face_copy.start()

    for f in range(5):

        @pl.when(jnp.logical_not(final[0]))
        def _():
            up_copies[f].start()

        @pl.when(jnp.logical_not(first[0]))
        def _():
            down_copies[f].start()

    for f in range(5):
        for r in range(2):
            yup[2 * f + r] = q[f, :, 62 + r, :]
            ydown[2 * f + r] = q[f, :, r, :]
    ydown[10] = disp[1, :, 0, :].astype(jnp.float32) * STEP

    y_copies = [
        remote(yup, ylow, ys_sem.at[0], yr_sem.at[0], place(y=lax.rem(py + 1, ny))),
        remote(ydown, yhigh, ys_sem.at[1], yr_sem.at[1], place(y=lax.rem(py + ny - 1, ny))),
    ]
    for copy in y_copies:
        copy.start()

    lane8 = lax.broadcasted_iota(jnp.int32, (8, 128), 1)
    slot_of = lane8 // 4
    place4 = lane8 % 4

    def pack(source, base, half):
        packed = jnp.zeros((8, 128), jnp.float32)
        for xx in range(4):
            plane = source[base, half * 4 + xx].astype(jnp.float32)
            for t in range(8):
                k = xx * 8 + t
                moved = pltpu.roll(plane[8 * t : 8 * t + 8], (4 * k + 2) % 128, 1)
                packed = jnp.where(slot_of == k, moved, packed)
        return packed

    for f in range(5):
        for half in range(2):
            zpack[2 * f + half] = pack(q, f, half)
    for half in range(2):
        zpack[10 + half] = pack(disp, 2, half) * STEP

    z_copies = [
        remote(zpack, zlow, zs_sem.at[0], zr_sem.at[0], place(z=lax.rem(pz + 1, nz))),
        remote(zpack, zhigh, zs_sem.at[1], zr_sem.at[1], place(z=lax.rem(pz + nz - 1, nz))),
    ]
    for copy in z_copies:
        copy.start()

    for copy in copies_a:
        copy.wait_recv()
    part[1] = part[0] + jnp.sum(slots_a[...], axis=0)
    for copy in copies_b:
        copy.start()

    for copy in y_copies:
        copy.wait_recv()
    v0 = disp[1, :, 0, :].astype(jnp.float32) * (STEP * low_scale[1])
    v_last = disp[1, :, 63, :].astype(jnp.float32) * (STEP * flag_open[3])
    v64 = jnp.where(final[1], v_last, yhigh[10])
    g64 = half_weight(v64)
    for f in range(5):
        q0, qa, qb = q[f, :, 0, :], q[f, :, 62, :], q[f, :, 63, :]
        lo1 = jnp.where(first[1], q0, ylow[2 * f + 1])
        lo2 = jnp.where(first[1], q0, ylow[2 * f])
        hi0 = jnp.where(final[1], qb, yhigh[2 * f])
        hi1 = jnp.where(final[1], qb, yhigh[2 * f + 1])
        d64 = hi0 - qb
        s63 = minmod(qb - qa, d64)
        s64 = minmod(d64, hi1 - hi0)
        yedge[0, f] = lo1
        yedge[1, f] = d64
        yedge[2, f] = minmod(lo1 - lo2, q0 - lo1)
        yedge[3, f] = v64 * jnp.where(v64 > 0, qb, hi0) + g64 * jnp.where(v64 > 0, s63, s64)

    for copy in z_copies:
        copy.wait_recv()

    def face(four, v):
        behind = back(four)
        diff = four - behind
        slope = minmod(diff, ahead(diff))
        flux = v * jnp.where(v > 0, behind, four) + half_weight(v) * jnp.where(
            v > 0, back(slope), slope
        )
        return slope, flux

    for half in range(2):
        own_v = zpack[10 + half]
        v_low = own_v * low_scale[2]
        v_high = jnp.where(final[2], back(own_v) * flag_open[5], zhigh[10 + half])
        zface[half] = ahead(v_high)
        for f in range(5):
            j = 2 * f + half
            own = zpack[j]
            ghost_low = jnp.where(place4 == 0, pltpu.roll(own, 126, 1), ahead(own))
            ghost_high = jnp.where(place4 == 2, back(own), pltpu.roll(own, 2, 1))
            low = jnp.where(place4 < 2, jnp.where(first[2], ghost_low, zlow[j]), own)
            high = jnp.where(place4 < 2, own, jnp.where(final[2], ghost_high, zhigh[j]))
            slope_low, flux_low = face(low, v_low)
            slope_high, flux_high = face(high, v_high)
            zslope[j] = jnp.where(place4 == 1, slope_high, slope_low)
            zflow[j] = jnp.where(
                place4 == 1,
                ahead(jnp.where(v_high > 0, 0.0, flux_high)),
                jnp.where(v_low > 0, flux_low, 0.0),
            )

    scale_y = jnp.where(rows == 0, STEP * low_scale[1], STEP)
    scale_z = jnp.where(lanes == 0, STEP * low_scale[2], STEP)

    def planes(x, carry):
        half = x // 4
        moves = [lax.rem(128 + 126 - 4 * ((x % 4) * 8 + t), 128) for t in range(8)]

        def spread(packed):
            return jnp.concatenate([pltpu.roll(packed, move, 1) for move in moves], 0)

        vy = disp[1, x].astype(jnp.float32) * scale_y
        gy = half_weight(vy)
        up_y = vy > 0
        vz = disp[2, x].astype(jnp.float32) * scale_z
        vz_next = jnp.where(lanes == 127, spread(zface[half]), ahead(vz))
        right = jnp.maximum(vz_next, 0.0)
        right_w = 0.5 * right * (1.0 - right)
        left = jnp.minimum(vz, 0.0)
        left_w = -0.5 * left * (1.0 + left)
        at_first, at_last = lanes == 0, lanes == 127
        at_edge = jnp.logical_or(at_first, at_last)
        for f in range(5):
            value = q[f, x]

            below = back(value)
            above = ahead(value)
            slope = minmod(value - below, above - value)
            slope = jnp.where(at_edge, spread(zslope[2 * f + half]), slope)
            flow = spread(zflow[2 * f + half])
            out_right = right * value + right_w * slope
            out_left = left * value + left_w * slope
            from_left = jnp.where(at_first, flow, back(out_right))
            from_right = jnp.where(at_last, flow, ahead(out_left))
            change_z = (from_left - out_right) + (out_left - from_right)

            below = shift_down(value, yedge[0, f, pl.ds(x, 1), :])
            diff = value - below
            slope = minmod(diff, shift_up(diff, yedge[1, f, pl.ds(x, 1), :]))
            slope_below = shift_down(slope, yedge[2, f, pl.ds(x, 1), :])
            flux = vy * jnp.where(up_y, below, value) + gy * jnp.where(up_y, slope_below, slope)
            change_y = flux - shift_up(flux, yedge[3, f, pl.ds(x, 1), :])
            acc[f, x] = (value + change_y) + change_z
        return carry

    lax.fori_loop(0, 4, planes, 0)
    for copy in copies_b:
        copy.wait_recv()
    part[2] = part[1] + jnp.sum(slots_b[...], axis=0)
    for copy in copies_c:
        copy.start()
    lax.fori_loop(4, 8, planes, 0)

    @pl.when(jnp.logical_not(final[0]))
    def _():
        face_copy.wait_recv()

    for i in range(9):
        if i == 0:
            v = disp[0, 0].astype(jnp.float32) * (STEP * low_scale[0])
        elif i < 8:
            v = disp[0, i].astype(jnp.float32) * STEP
        else:
            v_last = disp[0, 7].astype(jnp.float32) * (STEP * flag_open[1])
            v = jnp.where(final[0], v_last, xface[...].astype(jnp.float32) * STEP)
        vx[i] = v
        gx_w[i] = half_weight(v)

    stores = []
    for f in range(5):

        @pl.when(jnp.logical_not(first[0]))
        def _():
            up_copies[f].wait_recv()

        @pl.when(jnp.logical_not(final[0]))
        def _():
            down_copies[f].wait_recv()

        def tile(t, carry):
            part_rows = pl.ds(pl.multiple_of(t * 8, 8), 8)
            own = [q[f, i, part_rows] for i in range(8)]
            cell = (
                [jnp.where(first[0], own[0], xlow[f, r, part_rows]) for r in range(2)]
                + own
                + [jnp.where(final[0], own[7], xhigh[f, r, part_rows]) for r in range(2)]
            )
            diff = [cell[i + 1] - cell[i] for i in range(11)]
            slope = [minmod(diff[i], diff[i + 1]) for i in range(10)]
            flux = []
            for i in range(9):
                v = vx[i, part_rows]
                g = gx_w[i, part_rows]
                flux.append(
                    v * jnp.where(v > 0, cell[i + 1], cell[i + 2])
                    + g * jnp.where(v > 0, slope[i], slope[i + 1])
                )
            for i in range(8):
                acc[f, i, part_rows] += flux[i] - flux[i + 1]
            return carry

        lax.fori_loop(0, 8, tile, 0)
        store = pltpu.make_async_copy(acc.at[f], field_out[f], out_sem.at[f])
        store.start()
        stores.append(store)

    for copy in copies_c:
        copy.wait_recv()
    grand = part[2] + jnp.sum(slots_c[...], axis=0)
    totals[0] = jnp.sum(grand[0:1]) / cells
    totals[1] = jnp.sum(grand[1:2]) / cells

    for copy in copies_a + copies_b + copies_c + y_copies + z_copies:
        copy.wait_send()

    @pl.when(jnp.logical_not(first[0]))
    def _():
        face_copy.wait_send()

    for f in range(5):

        @pl.when(jnp.logical_not(final[0]))
        def _():
            up_copies[f].wait_send()

        @pl.when(jnp.logical_not(first[0]))
        def _():
            down_copies[f].wait_send()

    for store in stores:
        store.wait()


def shards(cells, density, momentum, energy, displacement, flags):
    f32, i32 = jnp.float32, jnp.int32
    anywhere = pl.BlockSpec(memory_space=pl.ANY)
    return pl.pallas_call(
        functools.partial(kernel, cells),
        out_shape=(
            jax.ShapeDtypeStruct(density.shape, f32),
            jax.ShapeDtypeStruct(momentum.shape, f32),
            jax.ShapeDtypeStruct(energy.shape, f32),
            jax.ShapeDtypeStruct((2,), f32),
        ),
        in_specs=[anywhere] * 5,
        out_specs=(anywhere, anywhere, anywhere, pl.BlockSpec(memory_space=pltpu.SMEM)),
        scratch_shapes=[
            pltpu.VMEM((5, 8, 64, 128), f32),
            pltpu.VMEM((3, 8, 64, 128), i32),
            pltpu.SMEM((6,), i32),
            pltpu.VMEM((5, 8, 64, 128), f32),
            pltpu.VMEM((9, 64, 128), f32),
            pltpu.VMEM((9, 64, 128), f32),
            pltpu.VMEM((5, 2, 64, 128), f32),
            pltpu.VMEM((5, 2, 64, 128), f32),
            pltpu.VMEM((64, 128), i32),
            pltpu.VMEM((10, 8, 128), f32),
            pltpu.VMEM((11, 8, 128), f32),
            pltpu.VMEM((10, 8, 128), f32),
            pltpu.VMEM((11, 8, 128), f32),
            pltpu.VMEM((4, 5, 8, 128), f32),
            pltpu.VMEM((12, 8, 128), f32),
            pltpu.VMEM((12, 8, 128), f32),
            pltpu.VMEM((12, 8, 128), f32),
            pltpu.VMEM((10, 8, 128), f32),
            pltpu.VMEM((10, 8, 128), f32),
            pltpu.VMEM((2, 8, 128), f32),
            pltpu.VMEM((3, 8, 128), f32),
            pltpu.VMEM((7, 8, 128), f32),
            pltpu.VMEM((3, 8, 128), f32),
            pltpu.VMEM((7, 8, 128), f32),
            pltpu.SemaphoreType.DMA((9,)),
            pltpu.SemaphoreType.DMA((5,)),
            pltpu.SemaphoreType.DMA((11,)),
            pltpu.SemaphoreType.DMA((11,)),
            pltpu.SemaphoreType.DMA((2,)),
            pltpu.SemaphoreType.DMA((2,)),
            pltpu.SemaphoreType.DMA((2,)),
            pltpu.SemaphoreType.DMA((2,)),
            pltpu.SemaphoreType.DMA((17,)),
            pltpu.SemaphoreType.DMA((17,)),
        ],
        compiler_params=pltpu.CompilerParams(collective_id=0, has_side_effects=True),
        name="remap",
    )(density, momentum, energy, displacement, flags)


def solution(mesh):
    cells = float(mesh.shape["gx"] * mesh.shape["gy"] * mesh.shape["gz"] * 8 * 64 * 128)
    block = P("gx", "gy", "gz")
    three = P(None, "gx", "gy", "gz")
    return jax.shard_map(
        functools.partial(shards, cells),
        mesh=mesh,
        in_specs=(block, three, block, three, P()),
        out_specs=(block, three, block, P()),
        check_vma=False,
    )
```

```python
import functools

import jax
import jax.numpy as jnp
from jax import lax
from jax.experimental import pallas as pl
from jax.experimental.pallas import tpu as pltpu
from jax.sharding import PartitionSpec as P

MESH = pl.DeviceIdType.MESH
STEP = 1.0 / 256.0


def minmod(left_diff, right_diff):
    least = jnp.minimum(left_diff, right_diff)
    most = jnp.maximum(left_diff, right_diff)
    return jnp.maximum(least, jnp.minimum(most, 0.0))


def half_weight(v):
    size = jnp.abs(v)
    return 0.5 * size * (1.0 - size)


def shift_down(block, first_row):
    moved = pltpu.roll(block, 1, 0)
    row = lax.broadcasted_iota(jnp.int32, (8, 128), 0)
    top = jnp.where(row == 0, first_row, moved[:8])
    return jnp.concatenate([top, moved[8:]], 0)


def shift_up(block, last_row):
    n = block.shape[0]
    moved = pltpu.roll(block, n - 1, 0)
    row = lax.broadcasted_iota(jnp.int32, (8, 128), 0)
    bottom = jnp.where(row == 7, last_row, moved[n - 8 :])
    return jnp.concatenate([moved[: n - 8], bottom], 0)


def back(block):
    return pltpu.roll(block, 1, 1)


def ahead(block):
    return pltpu.roll(block, 127, 1)


def kernel(
    density,
    momentum,
    energy,
    displacement,
    flags,
    acc,
    grand,
    q,
    disp,
    flag,
    vx,
    gx_w,
    xlow,
    xhigh,
    xface,
    yup,
    ydown,
    ylow,
    yhigh,
    yedge,
    zpack,
    zlow,
    zhigh,
    zslope,
    zflow,
    zface,
    part,
    slots_a,
    slots_b,
    load_sem,
    xs_sem,
    xr_sem,
    ys_sem,
    yr_sem,
    zs_sem,
    zr_sem,
    ts_sem,
    tr_sem,
    round_sem,
):
    px, py, pz = lax.axis_index("gx"), lax.axis_index("gy"), lax.axis_index("gz")
    nx, ny, nz = lax.axis_size("gx"), lax.axis_size("gy"), lax.axis_size("gz")
    core = pz % 2
    zl = (pz // 2) % 2
    field_in = [density, momentum.at[0], momentum.at[1], momentum.at[2], energy]

    flag_copy = pltpu.make_async_copy(flags, flag, load_sem.at[8])
    flag_copy.start()
    loads = [pltpu.make_async_copy(field_in[f], q.at[f], load_sem.at[f]) for f in range(5)]
    disp_loads = [
        pltpu.make_async_copy(displacement.at[a], disp.at[a], load_sem.at[5 + a]) for a in range(3)
    ]
    loads[0].start()
    loads[4].start()
    for copy in disp_loads:
        copy.start()
    for f in (1, 2, 3):
        loads[f].start()

    def place(x=None, y=None, z=None):
        target = {}
        if x is not None:
            target["gx"] = x
        if y is not None:
            target["gy"] = y
        if z is not None:
            target["gz"] = z
        return target

    def along_yz(dy, dz):
        chip = lax.rem(py * 2 + zl + dz, 2 * ny)
        return place(y=chip // 2, z=lax.rem(pz + 4 * dy, nz) + 2 * (chip % 2 - zl))

    stage_a = [
        place(x=lax.rem(px + dx, nx), z=pz + dc * (1 - 2 * core))
        for dc in range(2)
        for dx in range(4)
        if dx or dc
    ]
    stage_b = [along_yz(dy, dz) for dy in range(4) for dz in range(8) if dy or dz]
    beside = [along_yz(0, dz) for dz in (1, 2, 6, 7)] + [along_yz(dy, 0) for dy in (1, 2, 3)]
    across = place(z=lax.rem(pz + nz + 2 * core - 1, nz))
    near = stage_a + beside + [across]

    barrier = pltpu.get_barrier_semaphore()
    for peer in near:
        pl.semaphore_signal(barrier, inc=1, device_id=peer, device_id_type=MESH)

    flag_copy.wait()
    loads[0].wait()
    loads[4].wait()
    for copy in disp_loads:
        copy.wait()

    flag_open = [flag[i].astype(jnp.float32) for i in range(6)]
    first = [px == 0, py == 0, pz == 0]
    final = [px == nx - 1, py == ny - 1, pz == nz - 1]
    low_scale = [jnp.where(first[a], flag_open[2 * a], 1.0) for a in range(3)]
    gain = [jnp.where(first[a], flag_open[2 * a] * STEP, 0.0) for a in range(3)]
    loss = [jnp.where(final[a], flag_open[2 * a + 1] * -STEP, 0.0) for a in range(3)]

    rows = lax.broadcasted_iota(jnp.int32, (64, 128), 0)
    lanes = lax.broadcasted_iota(jnp.int32, (64, 128), 1)
    weight_y = jnp.where(rows == 0, gain[1], jnp.where(rows == 63, loss[1], 0.0))
    weight_z = jnp.where(lanes == 0, gain[2], jnp.where(lanes == 127, loss[2], 0.0))

    def fold(block):
        return jnp.sum(block.reshape(8, 8, 128), axis=0)

    def plane_sum(x, sums):
        weight = (
            1.0
            + weight_y * disp[1, x].astype(jnp.float32)
            + weight_z * disp[2, x].astype(jnp.float32)
        )
        return (sums[0] + fold(q[0, x] * weight), sums[1] + fold(q[4, x] * weight))

    weight_low = gain[0] * disp[0, 0].astype(jnp.float32)
    weight_high = loss[0] * disp[0, 7].astype(jnp.float32)
    sums = tuple(fold(q[f, 0] * weight_low + q[f, 7] * weight_high) for f in (0, 4))
    sums = lax.fori_loop(0, 8, plane_sum, sums)
    lane1 = lax.broadcasted_iota(jnp.int32, (1, 128), 1)

    def halves(low, high):
        low = jnp.sum(low, axis=0, keepdims=True)
        high = jnp.sum(high, axis=0, keepdims=True)
        return jnp.where(lane1 < 64, low + pltpu.roll(low, 64, 1), high + pltpu.roll(high, 64, 1))

    part[0] = halves(*sums)
    for f in (1, 2, 3):
        loads[f].wait()

    pl.semaphore_wait(barrier, len(near))

    def total_copies(stage, peers, slots, base):
        return [
            pltpu.make_async_remote_copy(
                src_ref=part.at[stage],
                dst_ref=slots.at[i],
                send_sem=ts_sem.at[base + i],
                recv_sem=tr_sem.at[base + i],
                device_id=peer,
                device_id_type=MESH,
            )
            for i, peer in enumerate(peers)
        ]

    copies_a = total_copies(0, stage_a, slots_a, 0)
    copies_b = total_copies(1, stage_b, slots_b, 7)
    for copy in copies_a:
        copy.start()
    for peer in beside:
        pl.semaphore_signal(round_sem.at[0], inc=1, device_id=peer, device_id_type=MESH)

    def remote(src, dst, send_sem, recv_sem, peer):
        return pltpu.make_async_remote_copy(
            src_ref=src,
            dst_ref=dst,
            send_sem=send_sem,
            recv_sem=recv_sem,
            device_id=peer,
            device_id_type=MESH,
        )

    x_next = place(x=lax.rem(px + 1, nx))
    x_prev = place(x=lax.rem(px + nx - 1, nx))
    face_copy = remote(disp.at[0, 0], xface, xs_sem.at[10], xr_sem.at[10], x_prev)
    up_copies = [
        remote(q.at[f, pl.ds(6, 2)], xlow.at[f], xs_sem.at[f], xr_sem.at[f], x_next) for f in range(5)
    ]
    down_copies = [
        remote(q.at[f, pl.ds(0, 2)], xhigh.at[f], xs_sem.at[5 + f], xr_sem.at[5 + f], x_prev)
        for f in range(5)
    ]

    @pl.when(jnp.logical_not(first[0]))
    def _():
        face_copy.start()

    for f in range(5):

        @pl.when(jnp.logical_not(final[0]))
        def _():
            up_copies[f].start()

        @pl.when(jnp.logical_not(first[0]))
        def _():
            down_copies[f].start()

    for f in range(5):
        for r in range(2):
            yup[2 * f + r] = q[f, :, 62 + r, :]
            ydown[2 * f + r] = q[f, :, r, :]
    ydown[10] = disp[1, :, 0, :].astype(jnp.float32) * STEP

    y_copies = [
        remote(yup, ylow, ys_sem.at[0], yr_sem.at[0], place(y=lax.rem(py + 1, ny))),
        remote(ydown, yhigh, ys_sem.at[1], yr_sem.at[1], place(y=lax.rem(py + ny - 1, ny))),
    ]
    for copy in y_copies:
        copy.start()

    lane8 = lax.broadcasted_iota(jnp.int32, (8, 128), 1)
    slot_of = lane8 // 4
    place4 = lane8 % 4

    def pack(source, base, half):
        packed = jnp.zeros((8, 128), jnp.float32)
        for xx in range(4):
            plane = source[base, half * 4 + xx].astype(jnp.float32)
            for t in range(8):
                k = xx * 8 + t
                moved = pltpu.roll(plane[8 * t : 8 * t + 8], (4 * k + 2) % 128, 1)
                packed = jnp.where(slot_of == k, moved, packed)
        return packed

    for f in range(5):
        for half in range(2):
            zpack[2 * f + half] = pack(q, f, half)
    for half in range(2):
        zpack[10 + half] = pack(disp, 2, half) * STEP

    z_copies = [
        remote(zpack, zlow, zs_sem.at[0], zr_sem.at[0], place(z=lax.rem(pz + 1, nz))),
        remote(zpack, zhigh, zs_sem.at[1], zr_sem.at[1], place(z=lax.rem(pz + nz - 1, nz))),
    ]
    for copy in z_copies:
        copy.start()

    pl.semaphore_wait(round_sem.at[0], len(beside))
    for peer in beside:
        pl.semaphore_signal(round_sem.at[1], inc=1, device_id=peer, device_id_type=MESH)
    for copy in copies_a:
        copy.wait_recv()
    part[1] = part[0] + jnp.sum(slots_a[...], axis=0)
    pl.semaphore_wait(round_sem.at[1], len(beside))
    for copy in copies_b:
        copy.start()

    for copy in y_copies:
        copy.wait_recv()
    v0 = disp[1, :, 0, :].astype(jnp.float32) * (STEP * low_scale[1])
    v_last = disp[1, :, 63, :].astype(jnp.float32) * (STEP * flag_open[3])
    v64 = jnp.where(final[1], v_last, yhigh[10])
    g64 = half_weight(v64)
    for f in range(5):
        q0, qa, qb = q[f, :, 0, :], q[f, :, 62, :], q[f, :, 63, :]
        lo1 = jnp.where(first[1], q0, ylow[2 * f + 1])
        lo2 = jnp.where(first[1], q0, ylow[2 * f])
        hi0 = jnp.where(final[1], qb, yhigh[2 * f])
        hi1 = jnp.where(final[1], qb, yhigh[2 * f + 1])
        d64 = hi0 - qb
        s63 = minmod(qb - qa, d64)
        s64 = minmod(d64, hi1 - hi0)
        yedge[0, f] = lo1
        yedge[1, f] = d64
        yedge[2, f] = minmod(lo1 - lo2, q0 - lo1)
        yedge[3, f] = v64 * jnp.where(v64 > 0, qb, hi0) + g64 * jnp.where(v64 > 0, s63, s64)

    for copy in z_copies:
        copy.wait_recv()

    def face(four, v):
        behind = back(four)
        diff = four - behind
        slope = minmod(diff, ahead(diff))
        flux = v * jnp.where(v > 0, behind, four) + half_weight(v) * jnp.where(
            v > 0, back(slope), slope
        )
        return slope, flux

    for half in range(2):
        own_v = zpack[10 + half]
        v_low = own_v * low_scale[2]
        v_high = jnp.where(final[2], back(own_v) * flag_open[5], zhigh[10 + half])
        zface[half] = ahead(v_high)
        for f in range(5):
            j = 2 * f + half
            own = zpack[j]
            ghost_low = jnp.where(place4 == 0, pltpu.roll(own, 126, 1), ahead(own))
            ghost_high = jnp.where(place4 == 2, back(own), pltpu.roll(own, 2, 1))
            low = jnp.where(place4 < 2, jnp.where(first[2], ghost_low, zlow[j]), own)
            high = jnp.where(place4 < 2, own, jnp.where(final[2], ghost_high, zhigh[j]))
            slope_low, flux_low = face(low, v_low)
            slope_high, flux_high = face(high, v_high)
            zslope[j] = jnp.where(place4 == 1, slope_high, slope_low)
            zflow[j] = jnp.where(
                place4 == 1,
                ahead(jnp.where(v_high > 0, 0.0, flux_high)),
                jnp.where(v_low > 0, flux_low, 0.0),
            )

    scale_y = jnp.where(rows == 0, STEP * low_scale[1], STEP)
    scale_z = jnp.where(lanes == 0, STEP * low_scale[2], STEP)

    def planes(x, carry):
        half = x // 4
        moves = [lax.rem(128 + 126 - 4 * ((x % 4) * 8 + t), 128) for t in range(8)]

        def spread(packed):
            return jnp.concatenate([pltpu.roll(packed, move, 1) for move in moves], 0)

        vy = disp[1, x].astype(jnp.float32) * scale_y
        gy = half_weight(vy)
        up_y = vy > 0
        vz = disp[2, x].astype(jnp.float32) * scale_z
        vz_next = jnp.where(lanes == 127, spread(zface[half]), ahead(vz))
        right = jnp.maximum(vz_next, 0.0)
        right_w = 0.5 * right * (1.0 - right)
        left = jnp.minimum(vz, 0.0)
        left_w = -0.5 * left * (1.0 + left)
        at_first, at_last = lanes == 0, lanes == 127
        at_edge = jnp.logical_or(at_first, at_last)
        for f in range(5):
            value = q[f, x]

            below = back(value)
            above = ahead(value)
            slope = minmod(value - below, above - value)
            slope = jnp.where(at_edge, spread(zslope[2 * f + half]), slope)
            flow = spread(zflow[2 * f + half])
            out_right = right * value + right_w * slope
            out_left = left * value + left_w * slope
            from_left = jnp.where(at_first, flow, back(out_right))
            from_right = jnp.where(at_last, flow, ahead(out_left))
            change_z = (from_left - out_right) + (out_left - from_right)

            below = shift_down(value, yedge[0, f, pl.ds(x, 1), :])
            diff = value - below
            slope = minmod(diff, shift_up(diff, yedge[1, f, pl.ds(x, 1), :]))
            slope_below = shift_down(slope, yedge[2, f, pl.ds(x, 1), :])
            flux = vy * jnp.where(up_y, below, value) + gy * jnp.where(up_y, slope_below, slope)
            change_y = flux - shift_up(flux, yedge[3, f, pl.ds(x, 1), :])
            acc[f, x] = (value + change_y) + change_z
        return carry

    lax.fori_loop(0, 8, planes, 0)

    @pl.when(jnp.logical_not(final[0]))
    def _():
        face_copy.wait_recv()

    for i in range(9):
        if i == 0:
            v = disp[0, 0].astype(jnp.float32) * (STEP * low_scale[0])
        elif i < 8:
            v = disp[0, i].astype(jnp.float32) * STEP
        else:
            v_last = disp[0, 7].astype(jnp.float32) * (STEP * flag_open[1])
            v = jnp.where(final[0], v_last, xface[...].astype(jnp.float32) * STEP)
        vx[i] = v
        gx_w[i] = half_weight(v)

    for f in range(5):

        @pl.when(jnp.logical_not(first[0]))
        def _():
            up_copies[f].wait_recv()

        @pl.when(jnp.logical_not(final[0]))
        def _():
            down_copies[f].wait_recv()

        def tile(t, carry):
            part_rows = pl.ds(pl.multiple_of(t * 8, 8), 8)
            own = [q[f, i, part_rows] for i in range(8)]
            cell = (
                [jnp.where(first[0], own[0], xlow[f, r, part_rows]) for r in range(2)]
                + own
                + [jnp.where(final[0], own[7], xhigh[f, r, part_rows]) for r in range(2)]
            )
            diff = [cell[i + 1] - cell[i] for i in range(11)]
            slope = [minmod(diff[i], diff[i + 1]) for i in range(10)]
            flux = []
            for i in range(9):
                v = vx[i, part_rows]
                g = gx_w[i, part_rows]
                flux.append(
                    v * jnp.where(v > 0, cell[i + 1], cell[i + 2])
                    + g * jnp.where(v > 0, slope[i], slope[i + 1])
                )
            for i in range(8):
                acc[f, i, part_rows] += flux[i] - flux[i + 1]
            return carry

        lax.fori_loop(0, 8, tile, 0)

    for copy in copies_b:
        copy.wait_recv()
    grand[...] = part[1] + jnp.sum(slots_b[...], axis=0)

    for copy in copies_a + copies_b + y_copies + z_copies:
        copy.wait_send()

    @pl.when(jnp.logical_not(first[0]))
    def _():
        face_copy.wait_send()

    for f in range(5):

        @pl.when(jnp.logical_not(final[0]))
        def _():
            up_copies[f].wait_send()

        @pl.when(jnp.logical_not(first[0]))
        def _():
            down_copies[f].wait_send()


def write_out(cells, acc, grand, new_density, new_momentum, new_energy, totals, pair, sem):
    stores = [
        pltpu.make_async_copy(acc.at[0], new_density, sem.at[0]),
        pltpu.make_async_copy(acc.at[pl.ds(1, 3)], new_momentum, sem.at[1]),
        pltpu.make_async_copy(acc.at[4], new_energy, sem.at[2]),
    ]
    for store in stores:
        store.start()
    lane1 = lax.broadcasted_iota(jnp.int32, (1, 128), 1)
    both = grand[...]
    pair[0] = jnp.sum(jnp.where(lane1 < 64, both, 0.0)) / cells
    pair[1] = jnp.sum(jnp.where(lane1 < 64, 0.0, both)) / cells
    last = pltpu.make_async_copy(pair, totals, sem.at[3])
    last.start()
    for store in stores:
        store.wait()
    last.wait()


def shards(cells, density, momentum, energy, displacement, flags):
    f32, i32 = jnp.float32, jnp.int32
    anywhere = pl.BlockSpec(memory_space=pltpu.HBM)
    local = pl.BlockSpec(memory_space=pltpu.VMEM)
    inputs = [
        pltpu.with_memory_space_constraint(a, pltpu.HBM)
        for a in (density, momentum, energy, displacement, flags)
    ]
    acc, grand = pl.pallas_call(
        kernel,
        out_shape=(
            jax.ShapeDtypeStruct((5, 8, 64, 128), f32),
            jax.ShapeDtypeStruct((1, 128), f32),
        ),
        in_specs=[anywhere] * 5,
        out_specs=(local, local),
        scratch_shapes=[
            pltpu.VMEM((5, 8, 64, 128), f32),
            pltpu.VMEM((3, 8, 64, 128), i32),
            pltpu.SMEM((6,), i32),
            pltpu.VMEM((9, 64, 128), f32),
            pltpu.VMEM((9, 64, 128), f32),
            pltpu.VMEM((5, 2, 64, 128), f32),
            pltpu.VMEM((5, 2, 64, 128), f32),
            pltpu.VMEM((64, 128), i32),
            pltpu.VMEM((10, 8, 128), f32),
            pltpu.VMEM((11, 8, 128), f32),
            pltpu.VMEM((10, 8, 128), f32),
            pltpu.VMEM((11, 8, 128), f32),
            pltpu.VMEM((4, 5, 8, 128), f32),
            pltpu.VMEM((12, 8, 128), f32),
            pltpu.VMEM((12, 8, 128), f32),
            pltpu.VMEM((12, 8, 128), f32),
            pltpu.VMEM((10, 8, 128), f32),
            pltpu.VMEM((10, 8, 128), f32),
            pltpu.VMEM((2, 8, 128), f32),
            pltpu.VMEM((2, 1, 128), f32),
            pltpu.VMEM((7, 1, 128), f32),
            pltpu.VMEM((31, 1, 128), f32),
            pltpu.SemaphoreType.DMA((9,)),
            pltpu.SemaphoreType.DMA((11,)),
            pltpu.SemaphoreType.DMA((11,)),
            pltpu.SemaphoreType.DMA((2,)),
            pltpu.SemaphoreType.DMA((2,)),
            pltpu.SemaphoreType.DMA((2,)),
            pltpu.SemaphoreType.DMA((2,)),
            pltpu.SemaphoreType.DMA((38,)),
            pltpu.SemaphoreType.DMA((38,)),
            pltpu.SemaphoreType.REGULAR((2,)),
        ],
        compiler_params=pltpu.CompilerParams(
            collective_id=0, has_side_effects=True, vmem_limit_bytes=16 * 2**20
        ),
        name="remap",
    )(*inputs)
    return pl.pallas_call(
        functools.partial(write_out, cells),
        out_shape=(
            jax.ShapeDtypeStruct(density.shape, f32),
            jax.ShapeDtypeStruct(momentum.shape, f32),
            jax.ShapeDtypeStruct(energy.shape, f32),
            jax.ShapeDtypeStruct((2,), f32),
        ),
        in_specs=[local, local],
        out_specs=[anywhere] * 4,
        scratch_shapes=[pltpu.SMEM((2,), f32), pltpu.SemaphoreType.DMA((4,))],
        compiler_params=pltpu.CompilerParams(vmem_limit_bytes=4 * 2**20),
        name="write_out",
    )(acc, grand)


def solution(mesh):
    cells = float(mesh.shape["gx"] * mesh.shape["gy"] * mesh.shape["gz"] * 8 * 64 * 128)
    block = P("gx", "gy", "gz")
    three = P(None, "gx", "gy", "gz")
    return jax.shard_map(
        functools.partial(shards, cells),
        mesh=mesh,
        in_specs=(block, three, block, three, P()),
        out_specs=(block, three, block, P()),
        check_vma=False,
    )
```

```python
import functools

import jax
import jax.numpy as jnp
from jax import lax
from jax.experimental import pallas as pl
from jax.experimental.pallas import tpu as pltpu
from jax.sharding import PartitionSpec as P

MESH = pl.DeviceIdType.MESH
STEP = 1.0 / 256.0
EARLY = 3


def minmod(left_diff, right_diff):
    least = jnp.minimum(left_diff, right_diff)
    most = jnp.maximum(left_diff, right_diff)
    return jnp.maximum(least, jnp.minimum(most, 0.0))


def half_weight(v):
    size = jnp.abs(v)
    return 0.5 * size * (1.0 - size)


def back(block):
    return pltpu.roll(block, 1, 1)


def ahead(block):
    return pltpu.roll(block, 127, 1)


def kernel(
    density,
    momentum,
    energy,
    displacement,
    flags,
    acc,
    grand,
    q,
    disp,
    flag,
    vx,
    gx_w,
    xlow,
    xhigh,
    xface,
    yup,
    ydown,
    ylow,
    yhigh,
    zpack,
    zlow,
    zhigh,
    zcorr,
    part,
    slots_a,
    slots_b,
    load_sem,
    xs_sem,
    xr_sem,
    ys_sem,
    yr_sem,
    zs_sem,
    zr_sem,
    ts_sem,
    tr_sem,
    round_sem,
    reply_sem,
):
    px, py, pz = lax.axis_index("gx"), lax.axis_index("gy"), lax.axis_index("gz")
    nx, ny, nz = lax.axis_size("gx"), lax.axis_size("gy"), lax.axis_size("gz")
    core = pz % 2
    zl = (pz // 2) % 2
    field_in = [density, momentum.at[0], momentum.at[1], momentum.at[2], energy]

    flag_copy = pltpu.make_async_copy(flags, flag, load_sem.at[8])
    flag_copy.start()
    loads = [pltpu.make_async_copy(field_in[f], q.at[f], load_sem.at[f]) for f in range(5)]
    disp_loads = [
        pltpu.make_async_copy(displacement.at[a], disp.at[a], load_sem.at[5 + a]) for a in range(3)
    ]
    loads[0].start()
    loads[4].start()
    for copy in disp_loads:
        copy.start()
    for f in (1, 2, 3):
        loads[f].start()

    def place(x=None, y=None, z=None):
        target = {}
        if x is not None:
            target["gx"] = x
        if y is not None:
            target["gy"] = y
        if z is not None:
            target["gz"] = z
        return target

    level = py * 2 + zl
    levels = 2 * ny
    early = level < EARLY

    def along_yz(dy, dz):
        chip = lax.rem(level + dz, levels)
        return place(y=chip // 2, z=lax.rem(pz + 4 * dy, nz) + 2 * (chip % 2 - zl))

    def greet(sem, peer):
        pl.semaphore_signal(sem, inc=1, device_id=peer, device_id_type=MESH)

    stage_a = [
        place(x=lax.rem(px + dx, nx), z=pz + dc * (1 - 2 * core))
        for dc in range(2)
        for dx in range(4)
        if dx or dc
    ]
    stage_b = [along_yz(dy, dz) for dy in range(4) for dz in range(8) if dy or dz]
    along_y = [along_yz(dy, 0) for dy in (1, 2, 3)]
    steps = [-2, -1, 1, 2]
    late_step = [
        jnp.logical_and(level + step >= EARLY, level + step < levels) for step in steps
    ]
    late_steps = sum(ok.astype(jnp.int32) for ok in late_step)
    has_across = jnp.where(core == 1, pz < nz - 1, pz > 0)
    across = place(z=lax.rem(pz + nz + 2 * core - 1, nz))

    def greet_late(sem):
        for step, ok in zip(steps, late_step):

            @pl.when(ok)
            def _():
                greet(sem, along_yz(0, step % 8))

    barrier = pltpu.get_barrier_semaphore()
    for peer in stage_a + along_y:
        greet(barrier, peer)

    @pl.when(has_across)
    def _():
        greet(barrier, across)

    @pl.when(early)
    def _():
        for dz in range(1, 8):

            @pl.when(level + dz < levels)
            def _():
                for dy in range(4):
                    greet(barrier, along_yz(dy, dz))

    @pl.when(jnp.logical_not(early))
    def _():
        greet_late(barrier)

    flag_copy.wait()
    loads[0].wait()
    loads[4].wait()
    for copy in disp_loads:
        copy.wait()

    flag_open = [flag[i].astype(jnp.float32) for i in range(6)]
    first = [px == 0, py == 0, pz == 0]
    final = [px == nx - 1, py == ny - 1, pz == nz - 1]
    low_scale = [jnp.where(first[a], flag_open[2 * a], 1.0) for a in range(3)]
    gain = [jnp.where(first[a], flag_open[2 * a] * STEP, 0.0) for a in range(3)]
    loss = [jnp.where(final[a], flag_open[2 * a + 1] * -STEP, 0.0) for a in range(3)]

    rows = lax.broadcasted_iota(jnp.int32, (64, 128), 0)
    lanes = lax.broadcasted_iota(jnp.int32, (64, 128), 1)
    weight_y = jnp.where(rows == 0, gain[1], jnp.where(rows == 63, loss[1], 0.0))
    weight_z = jnp.where(lanes == 0, gain[2], jnp.where(lanes == 127, loss[2], 0.0))

    def fold(block):
        return jnp.sum(block.reshape(8, 8, 128), axis=0)

    def plane_sum(x, sums):
        weight = (
            1.0
            + weight_y * disp[1, x].astype(jnp.float32)
            + weight_z * disp[2, x].astype(jnp.float32)
        )
        return (sums[0] + fold(q[0, x] * weight), sums[1] + fold(q[4, x] * weight))

    weight_low = gain[0] * disp[0, 0].astype(jnp.float32)
    weight_high = loss[0] * disp[0, 7].astype(jnp.float32)
    sums = tuple(fold(q[f, 0] * weight_low + q[f, 7] * weight_high) for f in (0, 4))
    sums = lax.fori_loop(0, 8, plane_sum, sums)
    lane1 = lax.broadcasted_iota(jnp.int32, (1, 128), 1)

    def halves(low, high):
        low = jnp.sum(low, axis=0, keepdims=True)
        high = jnp.sum(high, axis=0, keepdims=True)
        return jnp.where(lane1 < 64, low + pltpu.roll(low, 64, 1), high + pltpu.roll(high, 64, 1))

    part[0] = halves(*sums)
    for f in (1, 2, 3):
        loads[f].wait()

    greeted = (
        len(stage_a)
        + len(along_y)
        + has_across.astype(jnp.int32)
        + jnp.where(early, 4 * level, 4 * EARLY + late_steps)
    )
    pl.semaphore_wait(barrier, greeted)

    def total_copies(stage, peers, slots, base):
        return [
            pltpu.make_async_remote_copy(
                src_ref=part.at[stage],
                dst_ref=slots.at[i],
                send_sem=ts_sem.at[base + i],
                recv_sem=tr_sem.at[base + i],
                device_id=peer,
                device_id_type=MESH,
            )
            for i, peer in enumerate(peers)
        ]

    copies_a = total_copies(0, stage_a, slots_a, 0)
    copies_b = total_copies(1, stage_b, slots_b, 7)
    for copy in copies_a:
        copy.start()

    def remote(src, dst, send_sem, recv_sem, peer):
        return pltpu.make_async_remote_copy(
            src_ref=src,
            dst_ref=dst,
            send_sem=send_sem,
            recv_sem=recv_sem,
            device_id=peer,
            device_id_type=MESH,
        )

    x_next = place(x=lax.rem(px + 1, nx))
    x_prev = place(x=lax.rem(px + nx - 1, nx))
    face_copy = remote(disp.at[0, 0], xface, xs_sem.at[10], xr_sem.at[10], x_prev)
    up_copies = [
        remote(q.at[f, pl.ds(6, 2)], xlow.at[f], xs_sem.at[f], xr_sem.at[f], x_next) for f in range(5)
    ]
    down_copies = [
        remote(q.at[f, pl.ds(0, 2)], xhigh.at[f], xs_sem.at[5 + f], xr_sem.at[5 + f], x_prev)
        for f in range(5)
    ]

    @pl.when(jnp.logical_not(first[0]))
    def _():
        face_copy.start()

    for f in range(5):

        @pl.when(jnp.logical_not(final[0]))
        def _():
            up_copies[f].start()

        @pl.when(jnp.logical_not(first[0]))
        def _():
            down_copies[f].start()

    for f in range(5):
        for r in range(2):
            yup[2 * f + r] = q[f, :, 62 + r, :]
            ydown[2 * f + r] = q[f, :, r, :]
    ydown[10] = disp[1, :, 0, :].astype(jnp.float32) * STEP

    y_up = remote(yup, ylow, ys_sem.at[0], yr_sem.at[0], place(y=lax.rem(py + 1, ny)))
    y_down = remote(ydown, yhigh, ys_sem.at[1], yr_sem.at[1], place(y=lax.rem(py + ny - 1, ny)))

    for back_step in (1, 2):

        @pl.when(jnp.logical_and(level - back_step >= 0, level - back_step < EARLY))
        def _():
            greet(reply_sem.at[0], along_yz(0, 8 - back_step))

    @pl.when(jnp.logical_not(early))
    def _():
        greet_late(round_sem.at[0])
        for peer in along_y:
            greet(round_sem.at[0], peer)

    @pl.when(jnp.logical_not(first[1]))
    def _():
        y_down.start()

    @pl.when(early)
    def _():
        pl.semaphore_wait(reply_sem.at[0], 2)

    @pl.when(jnp.logical_not(final[1]))
    def _():
        y_up.start()

    lane8 = lax.broadcasted_iota(jnp.int32, (8, 128), 1)
    slot_of = lane8 // 4
    place4 = lane8 % 4

    def pack(source, base, half):
        packed = jnp.zeros((8, 128), jnp.float32)
        for xx in range(4):
            plane = source[base, half * 4 + xx].astype(jnp.float32)
            for t in range(8):
                k = xx * 8 + t
                moved = pltpu.roll(plane[8 * t : 8 * t + 8], (4 * k + 2) % 128, 1)
                packed = jnp.where(slot_of == k, moved, packed)
        return packed

    for f in range(5):
        for half in range(2):
            zpack[2 * f + half] = pack(q, f, half)
    for half in range(2):
        zpack[10 + half] = pack(disp, 2, half) * STEP

    z_up = remote(zpack, zlow, zs_sem.at[0], zr_sem.at[0], place(z=lax.rem(pz + 1, nz)))
    z_down = remote(zpack, zhigh, zs_sem.at[1], zr_sem.at[1], place(z=lax.rem(pz + nz - 1, nz)))

    @pl.when(jnp.logical_not(final[2]))
    def _():
        z_up.start()

    @pl.when(jnp.logical_not(first[2]))
    def _():
        z_down.start()

    for target in range(EARLY):

        @pl.when(target < level)
        def _():
            for dy in range(4):
                greet(reply_sem.at[1], along_yz(dy, lax.rem(levels + target - level, levels)))

    scale_y = jnp.where(
        jnp.logical_or(rows < 2, rows == 63), 0.0, STEP
    )
    scale_z = jnp.where(lanes == 0, STEP * low_scale[2], STEP)

    def planes(x, carry):
        vy = disp[1, x].astype(jnp.float32) * scale_y
        gy = half_weight(vy)
        up_y = vy > 0
        vz = disp[2, x].astype(jnp.float32) * scale_z
        right = jnp.where(lanes == 127, 0.0, jnp.maximum(ahead(vz), 0.0))
        right_w = jnp.where(lanes == 0, 0.0, 0.5 * right * (1.0 - right))
        left = jnp.minimum(vz, 0.0)
        left_w = jnp.where(
            jnp.logical_or(lanes == 0, lanes == 127), 0.0, -0.5 * left * (1.0 + left)
        )
        for f in range(5):
            value = q[f, x]
            below = back(value)
            above = ahead(value)
            slope = minmod(value - below, above - value)
            out_right = right * value + right_w * slope
            out_left = left * value + left_w * slope
            change_z = (back(out_right) - out_right) + (out_left - ahead(out_left))

            below = pltpu.roll(value, 1, 0)
            diff = value - below
            slope = minmod(diff, pltpu.roll(diff, 63, 0))
            flux = vy * jnp.where(up_y, below, value) + gy * jnp.where(
                up_y, pltpu.roll(slope, 1, 0), slope
            )
            acc[f, x] = (value + (flux - pltpu.roll(flux, 63, 0))) + change_z
        return carry

    lax.fori_loop(0, 2, planes, 0)

    @pl.when(jnp.logical_not(early))
    def _():
        pl.semaphore_wait(round_sem.at[0], len(along_y) + late_steps)
        greet_late(round_sem.at[1])
        for peer in along_y:
            greet(round_sem.at[1], peer)

    lax.fori_loop(2, 4, planes, 0)

    for copy in copies_a:
        copy.wait_recv()
    part[1] = part[0] + jnp.sum(slots_a[...], axis=0)

    @pl.when(jnp.logical_not(early))
    def _():
        pl.semaphore_wait(round_sem.at[1], len(along_y) + late_steps)
        for copy in copies_b:
            copy.start()

    lax.fori_loop(4, 8, planes, 0)

    @pl.when(jnp.logical_not(first[1]))
    def _():
        y_up.wait_recv()

    @pl.when(jnp.logical_not(final[1]))
    def _():
        y_down.wait_recv()

    v0, v1, v63 = [disp[1, :, r, :].astype(jnp.float32) * STEP for r in (0, 1, 63)]
    v64 = jnp.where(final[1], v63 * flag_open[3], yhigh[10])
    v0 = v0 * low_scale[1]

    def flux_row(v, behind, at, slope_behind, slope_at):
        return v * jnp.where(v > 0, behind, at) + half_weight(v) * jnp.where(
            v > 0, slope_behind, slope_at
        )

    for f in range(5):
        q0, q1, q2, q61, q62, q63 = [q[f, :, r, :] for r in (0, 1, 2, 61, 62, 63)]
        lo1 = jnp.where(first[1], q0, ylow[2 * f + 1])
        lo2 = jnp.where(first[1], q0, ylow[2 * f])
        hi0 = jnp.where(final[1], q63, yhigh[2 * f])
        hi1 = jnp.where(final[1], q63, yhigh[2 * f + 1])
        s0 = minmod(q0 - lo1, q1 - q0)
        s63 = minmod(q63 - q62, hi0 - q63)
        flux_0 = flux_row(v0, lo1, q0, minmod(lo1 - lo2, q0 - lo1), s0)
        flux_1 = flux_row(v1, q0, q1, s0, minmod(q1 - q0, q2 - q1))
        flux_63 = flux_row(v63, q62, q63, minmod(q62 - q61, q63 - q62), s63)
        flux_64 = flux_row(v64, q63, hi0, s63, minmod(hi0 - q63, hi1 - hi0))
        acc[f, :, 0, :] += flux_0 - flux_1
        acc[f, :, 1, :] += flux_1
        acc[f, :, 62, :] -= flux_63
        acc[f, :, 63, :] += flux_63 - flux_64

    @pl.when(jnp.logical_not(first[2]))
    def _():
        z_up.wait_recv()

    @pl.when(jnp.logical_not(final[2]))
    def _():
        z_down.wait_recv()

    def face(four, v):
        behind = back(four)
        diff = four - behind
        slope = minmod(diff, ahead(diff))
        flux = v * jnp.where(v > 0, behind, four) + half_weight(v) * jnp.where(
            v > 0, back(slope), slope
        )
        return slope, flux

    for half in range(2):
        own_v = zpack[10 + half]
        v_low = jnp.where(place4 == 2, own_v * low_scale[2], own_v)
        v_high = jnp.where(final[2], back(own_v) * flag_open[5], zhigh[10 + half])
        left = jnp.minimum(v_low, 0.0)
        left_w = -0.5 * left * (1.0 + left)
        right = jnp.maximum(ahead(own_v), 0.0)
        right_w = 0.5 * right * (1.0 - right)
        for f in range(5):
            j = 2 * f + half
            own = zpack[j]
            ghost_low = jnp.where(place4 == 0, pltpu.roll(own, 126, 1), ahead(own))
            ghost_high = jnp.where(place4 == 2, back(own), pltpu.roll(own, 2, 1))
            low = jnp.where(place4 < 2, jnp.where(first[2], ghost_low, zlow[j]), own)
            high = jnp.where(place4 < 2, own, jnp.where(final[2], ghost_high, zhigh[j]))
            slope_low, flux_low = face(low, v_low)
            slope_high, flux_high = face(high, v_high)
            by_left = left_w * jnp.where(place4 == 1, slope_high, slope_low)
            by_right = right_w * slope_low
            entering = jnp.where(v_low > 0, flux_low, 0.0)
            zcorr[j] = jnp.where(
                place4 == 0,
                -ahead(by_left),
                jnp.where(
                    place4 == 1,
                    by_left - ahead(flux_high) + ahead(left * own),
                    jnp.where(place4 == 2, entering + by_left - by_right, back(by_right)),
                ),
            )

    @pl.when(early)
    def _():
        pl.semaphore_wait(reply_sem.at[1], 4 * (levels - 1 - level))
        for copy in copies_b:
            copy.start()

    @pl.when(jnp.logical_not(final[0]))
    def _():
        face_copy.wait_recv()

    for i in range(9):
        if i == 0:
            v = disp[0, 0].astype(jnp.float32) * (STEP * low_scale[0])
        elif i < 8:
            v = disp[0, i].astype(jnp.float32) * STEP
        else:
            v_last = disp[0, 7].astype(jnp.float32) * (STEP * flag_open[1])
            v = jnp.where(final[0], v_last, xface[...].astype(jnp.float32) * STEP)
        vx[i] = v
        gx_w[i] = half_weight(v)

    edge_lanes = jnp.logical_or(lane8 < 2, lane8 > 125)
    for f in range(5):

        @pl.when(jnp.logical_not(first[0]))
        def _():
            up_copies[f].wait_recv()

        @pl.when(jnp.logical_not(final[0]))
        def _():
            down_copies[f].wait_recv()

        def tile(t, carry):
            part_rows = pl.ds(pl.multiple_of(t * 8, 8), 8)
            own = [q[f, i, part_rows] for i in range(8)]
            cell = (
                [jnp.where(first[0], own[0], xlow[f, r, part_rows]) for r in range(2)]
                + own
                + [jnp.where(final[0], own[7], xhigh[f, r, part_rows]) for r in range(2)]
            )
            diff = [cell[i + 1] - cell[i] for i in range(11)]
            slope = [minmod(diff[i], diff[i + 1]) for i in range(10)]
            flux = []
            for i in range(9):
                v = vx[i, part_rows]
                g = gx_w[i, part_rows]
                flux.append(
                    v * jnp.where(v > 0, cell[i + 1], cell[i + 2])
                    + g * jnp.where(v > 0, slope[i], slope[i + 1])
                )
            for i in range(8):
                move = lax.rem(254 - 4 * ((i % 4) * 8 + t), 128)
                corr = pltpu.roll(zcorr[2 * f + i // 4], move, 1)
                corr = jnp.where(edge_lanes, corr, 0.0)
                acc[f, i, part_rows] += (flux[i] - flux[i + 1]) + corr
            return carry

        lax.fori_loop(0, 8, tile, 0)

    for copy in copies_b:
        copy.wait_recv()
    grand[...] = part[1] + jnp.sum(slots_b[...], axis=0)

    for copy in copies_a + copies_b:
        copy.wait_send()

    @pl.when(jnp.logical_not(first[0]))
    def _():
        face_copy.wait_send()

    for copy, there in (
        (y_up, final[1]),
        (y_down, first[1]),
        (z_up, final[2]),
        (z_down, first[2]),
    ):

        @pl.when(jnp.logical_not(there))
        def _():
            copy.wait_send()

    for f in range(5):

        @pl.when(jnp.logical_not(final[0]))
        def _():
            up_copies[f].wait_send()

        @pl.when(jnp.logical_not(first[0]))
        def _():
            down_copies[f].wait_send()


def write_out(cells, acc, grand, new_density, new_momentum, new_energy, totals, pair, sem):
    stores = [
        pltpu.make_async_copy(acc.at[0], new_density, sem.at[0]),
        pltpu.make_async_copy(acc.at[pl.ds(1, 3)], new_momentum, sem.at[1]),
        pltpu.make_async_copy(acc.at[4], new_energy, sem.at[2]),
    ]
    for store in stores:
        store.start()
    lane1 = lax.broadcasted_iota(jnp.int32, (1, 128), 1)
    both = grand[...]
    pair[0] = jnp.sum(jnp.where(lane1 < 64, both, 0.0)) / cells
    pair[1] = jnp.sum(jnp.where(lane1 < 64, 0.0, both)) / cells
    last = pltpu.make_async_copy(pair, totals, sem.at[3])
    last.start()
    for store in stores:
        store.wait()
    last.wait()


def shards(cells, density, momentum, energy, displacement, flags):
    f32, i32 = jnp.float32, jnp.int32
    anywhere = pl.BlockSpec(memory_space=pltpu.HBM)
    local = pl.BlockSpec(memory_space=pltpu.VMEM)
    inputs = [
        pltpu.with_memory_space_constraint(a, pltpu.HBM)
        for a in (density, momentum, energy, displacement, flags)
    ]
    acc, grand = pl.pallas_call(
        kernel,
        out_shape=(
            jax.ShapeDtypeStruct((5, 8, 64, 128), f32),
            jax.ShapeDtypeStruct((1, 128), f32),
        ),
        in_specs=[anywhere] * 5,
        out_specs=(local, local),
        scratch_shapes=[
            pltpu.VMEM((5, 8, 64, 128), f32),
            pltpu.VMEM((3, 8, 64, 128), i32),
            pltpu.SMEM((6,), i32),
            pltpu.VMEM((9, 64, 128), f32),
            pltpu.VMEM((9, 64, 128), f32),
            pltpu.VMEM((5, 2, 64, 128), f32),
            pltpu.VMEM((5, 2, 64, 128), f32),
            pltpu.VMEM((64, 128), i32),
            pltpu.VMEM((10, 8, 128), f32),
            pltpu.VMEM((11, 8, 128), f32),
            pltpu.VMEM((10, 8, 128), f32),
            pltpu.VMEM((11, 8, 128), f32),
            pltpu.VMEM((12, 8, 128), f32),
            pltpu.VMEM((12, 8, 128), f32),
            pltpu.VMEM((12, 8, 128), f32),
            pltpu.VMEM((10, 8, 128), f32),
            pltpu.VMEM((2, 1, 128), f32),
            pltpu.VMEM((7, 1, 128), f32),
            pltpu.VMEM((31, 1, 128), f32),
            pltpu.SemaphoreType.DMA((9,)),
            pltpu.SemaphoreType.DMA((11,)),
            pltpu.SemaphoreType.DMA((11,)),
            pltpu.SemaphoreType.DMA((2,)),
            pltpu.SemaphoreType.DMA((2,)),
            pltpu.SemaphoreType.DMA((2,)),
            pltpu.SemaphoreType.DMA((2,)),
            pltpu.SemaphoreType.DMA((38,)),
            pltpu.SemaphoreType.DMA((38,)),
            pltpu.SemaphoreType.REGULAR((2,)),
            pltpu.SemaphoreType.REGULAR((2,)),
        ],
        compiler_params=pltpu.CompilerParams(
            collective_id=0, has_side_effects=True, vmem_limit_bytes=16 * 2**20
        ),
        name="remap",
    )(*inputs)
    return pl.pallas_call(
        functools.partial(write_out, cells),
        out_shape=(
            jax.ShapeDtypeStruct(density.shape, f32),
            jax.ShapeDtypeStruct(momentum.shape, f32),
            jax.ShapeDtypeStruct(energy.shape, f32),
            jax.ShapeDtypeStruct((2,), f32),
        ),
        in_specs=[local, local],
        out_specs=[anywhere] * 4,
        scratch_shapes=[pltpu.SMEM((2,), f32), pltpu.SemaphoreType.DMA((4,))],
        compiler_params=pltpu.CompilerParams(vmem_limit_bytes=4 * 2**20),
        name="write_out",
    )(acc, grand)


def solution(mesh):
    cells = float(mesh.shape["gx"] * mesh.shape["gy"] * mesh.shape["gz"] * 8 * 64 * 128)
    block = P("gx", "gy", "gz")
    three = P(None, "gx", "gy", "gz")
    return jax.shard_map(
        functools.partial(shards, cells),
        mesh=mesh,
        in_specs=(block, three, block, three, P()),
        out_specs=(block, three, block, P()),
        check_vma=False,
    )
```

```python
import functools

import jax
import jax.numpy as jnp
from jax import lax
from jax.experimental import pallas as pl
from jax.experimental.pallas import tpu as pltpu
from jax.sharding import PartitionSpec as P

MESH = pl.DeviceIdType.MESH
STEP = 1.0 / 256.0
EARLY = 3


def minmod(left_diff, right_diff):
    least = jnp.minimum(left_diff, right_diff)
    most = jnp.maximum(left_diff, right_diff)
    return jnp.maximum(least, jnp.minimum(most, 0.0))


def half_weight(v):
    size = jnp.abs(v)
    return 0.5 * size * (1.0 - size)


def back(block):
    return pltpu.roll(block, 1, 1)


def ahead(block):
    return pltpu.roll(block, 127, 1)


def kernel(
    density,
    momentum,
    energy,
    displacement,
    flags,
    acc,
    grand,
    q,
    disp,
    flag,
    vx,
    gx_w,
    xlow,
    xhigh,
    xface,
    yup,
    ydown,
    ylow,
    yhigh,
    zpack,
    zlow,
    zhigh,
    zcorr,
    part,
    slots_a,
    slots_b,
    load_sem,
    xs_sem,
    xr_sem,
    ys_sem,
    yr_sem,
    zs_sem,
    zr_sem,
    ts_sem,
    tr_sem,
    round_sem,
    reply_sem,
):
    px, py, pz = lax.axis_index("gx"), lax.axis_index("gy"), lax.axis_index("gz")
    nx, ny, nz = lax.axis_size("gx"), lax.axis_size("gy"), lax.axis_size("gz")
    core = pz % 2
    zl = (pz // 2) % 2
    field_in = [density, momentum.at[0], momentum.at[1], momentum.at[2], energy]

    flag_copy = pltpu.make_async_copy(flags, flag, load_sem.at[8])
    flag_copy.start()
    loads = [pltpu.make_async_copy(field_in[f], q.at[f], load_sem.at[f]) for f in range(5)]
    disp_loads = [
        pltpu.make_async_copy(displacement.at[a], disp.at[a], load_sem.at[5 + a]) for a in range(3)
    ]
    loads[0].start()
    loads[4].start()
    for copy in disp_loads:
        copy.start()
    for f in (1, 2, 3):
        loads[f].start()

    def place(x=None, y=None, z=None):
        target = {}
        if x is not None:
            target["gx"] = x
        if y is not None:
            target["gy"] = y
        if z is not None:
            target["gz"] = z
        return target

    level = py * 2 + zl
    levels = 2 * ny
    early = level < EARLY

    def along_yz(dy, dz):
        chip = lax.rem(level + dz, levels)
        return place(y=chip // 2, z=lax.rem(pz + 4 * dy, nz) + 2 * (chip % 2 - zl))

    def greet(sem, peer):
        pl.semaphore_signal(sem, inc=1, device_id=peer, device_id_type=MESH)

    stage_a = [
        place(x=lax.rem(px + dx, nx), z=pz + dc * (1 - 2 * core))
        for dc in range(2)
        for dx in range(4)
        if dx or dc
    ]
    offsets_b = sorted(
        [(dy, dz) for dy in range(4) for dz in range(8) if dy or dz],
        key=lambda o: -min(o[0], 4 - o[0]) - min(o[1], 8 - o[1]),
    )
    stage_b = [along_yz(dy, dz) for dy, dz in offsets_b]
    along_y = [along_yz(dy, 0) for dy in (1, 2, 3)]
    steps = [-2, -1, 1, 2]
    late_step = [
        jnp.logical_and(level + step >= EARLY, level + step < levels) for step in steps
    ]
    late_steps = sum(ok.astype(jnp.int32) for ok in late_step)
    has_across = jnp.where(core == 1, pz < nz - 1, pz > 0)
    across = place(z=lax.rem(pz + nz + 2 * core - 1, nz))

    def greet_late(sem):
        for step, ok in zip(steps, late_step):

            @pl.when(ok)
            def _():
                greet(sem, along_yz(0, step % 8))

    barrier = pltpu.get_barrier_semaphore()
    for peer in stage_a + along_y:
        greet(barrier, peer)

    @pl.when(has_across)
    def _():
        greet(barrier, across)

    @pl.when(early)
    def _():
        for dz in range(1, 8):

            @pl.when(level + dz < levels)
            def _():
                for dy in range(4):
                    greet(barrier, along_yz(dy, dz))

    @pl.when(jnp.logical_not(early))
    def _():
        greet_late(barrier)

    flag_copy.wait()
    loads[0].wait()
    loads[4].wait()
    for copy in disp_loads:
        copy.wait()

    flag_open = [flag[i].astype(jnp.float32) for i in range(6)]
    first = [px == 0, py == 0, pz == 0]
    final = [px == nx - 1, py == ny - 1, pz == nz - 1]
    low_scale = [jnp.where(first[a], flag_open[2 * a], 1.0) for a in range(3)]
    gain = [jnp.where(first[a], flag_open[2 * a] * STEP, 0.0) for a in range(3)]
    loss = [jnp.where(final[a], flag_open[2 * a + 1] * -STEP, 0.0) for a in range(3)]

    rows = lax.broadcasted_iota(jnp.int32, (64, 128), 0)
    lanes = lax.broadcasted_iota(jnp.int32, (64, 128), 1)
    weight_y = jnp.where(rows == 0, gain[1], jnp.where(rows == 63, loss[1], 0.0))
    weight_z = jnp.where(lanes == 0, gain[2], jnp.where(lanes == 127, loss[2], 0.0))

    def fold(block):
        return jnp.sum(block.reshape(8, 8, 128), axis=0)

    def plane_sum(x, sums):
        weight = (
            1.0
            + weight_y * disp[1, x].astype(jnp.float32)
            + weight_z * disp[2, x].astype(jnp.float32)
        )
        return (sums[0] + fold(q[0, x] * weight), sums[1] + fold(q[4, x] * weight))

    weight_low = gain[0] * disp[0, 0].astype(jnp.float32)
    weight_high = loss[0] * disp[0, 7].astype(jnp.float32)
    sums = tuple(fold(q[f, 0] * weight_low + q[f, 7] * weight_high) for f in (0, 4))
    sums = lax.fori_loop(0, 8, plane_sum, sums)
    lane1 = lax.broadcasted_iota(jnp.int32, (1, 128), 1)

    def halves(low, high):
        low = jnp.sum(low, axis=0, keepdims=True)
        high = jnp.sum(high, axis=0, keepdims=True)
        return jnp.where(lane1 < 64, low + pltpu.roll(low, 64, 1), high + pltpu.roll(high, 64, 1))

    part[0] = halves(*sums)
    for f in (1, 2, 3):
        loads[f].wait()

    greeted = (
        len(stage_a)
        + len(along_y)
        + has_across.astype(jnp.int32)
        + jnp.where(early, 4 * level, 4 * EARLY + late_steps)
    )
    pl.semaphore_wait(barrier, greeted)

    def total_copies(stage, peers, slots, base):
        return [
            pltpu.make_async_remote_copy(
                src_ref=part.at[stage],
                dst_ref=slots.at[i],
                send_sem=ts_sem.at[base + i],
                recv_sem=tr_sem.at[base + i],
                device_id=peer,
                device_id_type=MESH,
            )
            for i, peer in enumerate(peers)
        ]

    copies_a = total_copies(0, stage_a, slots_a, 0)
    copies_b = total_copies(1, stage_b, slots_b, 7)
    for copy in copies_a:
        copy.start()

    @pl.when(jnp.logical_not(early))
    def _():
        greet_late(round_sem.at[0])
        for peer in along_y:
            greet(round_sem.at[0], peer)

    def remote(src, dst, send_sem, recv_sem, peer):
        return pltpu.make_async_remote_copy(
            src_ref=src,
            dst_ref=dst,
            send_sem=send_sem,
            recv_sem=recv_sem,
            device_id=peer,
            device_id_type=MESH,
        )

    x_next = place(x=lax.rem(px + 1, nx))
    x_prev = place(x=lax.rem(px + nx - 1, nx))
    face_copy = remote(disp.at[0, 0], xface, xs_sem.at[10], xr_sem.at[10], x_prev)
    up_copies = [
        remote(q.at[f, pl.ds(6, 2)], xlow.at[f], xs_sem.at[f], xr_sem.at[f], x_next) for f in range(5)
    ]
    down_copies = [
        remote(q.at[f, pl.ds(0, 2)], xhigh.at[f], xs_sem.at[5 + f], xr_sem.at[5 + f], x_prev)
        for f in range(5)
    ]

    @pl.when(jnp.logical_not(first[0]))
    def _():
        face_copy.start()

    for f in range(5):

        @pl.when(jnp.logical_not(final[0]))
        def _():
            up_copies[f].start()

        @pl.when(jnp.logical_not(first[0]))
        def _():
            down_copies[f].start()

    for f in range(5):
        for r in range(2):
            yup[2 * f + r] = q[f, :, 62 + r, :]
            ydown[2 * f + r] = q[f, :, r, :]
    ydown[10] = disp[1, :, 0, :].astype(jnp.float32) * STEP

    y_up = remote(yup, ylow, ys_sem.at[0], yr_sem.at[0], place(y=lax.rem(py + 1, ny)))
    y_down = remote(ydown, yhigh, ys_sem.at[1], yr_sem.at[1], place(y=lax.rem(py + ny - 1, ny)))

    @pl.when(jnp.logical_not(first[1]))
    def _():
        y_down.start()

    @pl.when(jnp.logical_not(jnp.logical_or(final[1], early)))
    def _():
        y_up.start()

    lane8 = lax.broadcasted_iota(jnp.int32, (8, 128), 1)
    slot_of = lane8 // 4
    place4 = lane8 % 4

    def pack(source, base, half):
        packed = jnp.zeros((8, 128), jnp.float32)
        for xx in range(4):
            plane = source[base, half * 4 + xx].astype(jnp.float32)
            for t in range(8):
                k = xx * 8 + t
                moved = pltpu.roll(plane[8 * t : 8 * t + 8], (4 * k + 2) % 128, 1)
                packed = jnp.where(slot_of == k, moved, packed)
        return packed

    for f in range(5):
        for half in range(2):
            zpack[2 * f + half] = pack(q, f, half)
    for half in range(2):
        zpack[10 + half] = pack(disp, 2, half) * STEP

    z_up = remote(zpack, zlow, zs_sem.at[0], zr_sem.at[0], place(z=lax.rem(pz + 1, nz)))
    z_down = remote(zpack, zhigh, zs_sem.at[1], zr_sem.at[1], place(z=lax.rem(pz + nz - 1, nz)))

    @pl.when(jnp.logical_not(final[2]))
    def _():
        z_up.start()

    @pl.when(jnp.logical_not(first[2]))
    def _():
        z_down.start()

    for back_step in (1, 2):

        @pl.when(jnp.logical_and(level - back_step >= 0, level - back_step < EARLY))
        def _():
            greet(reply_sem.at[0], along_yz(0, 8 - back_step))

    for target in range(EARLY):

        @pl.when(target < level)
        def _():
            for dy in range(4):
                greet(
                    reply_sem.at[jnp.where(early, 2, 1)],
                    along_yz(dy, lax.rem(levels + target - level, levels)),
                )

    scale_y = jnp.where(
        jnp.logical_or(rows < 2, rows == 63), 0.0, STEP
    )
    scale_z = jnp.where(lanes == 0, STEP * low_scale[2], STEP)

    def planes(x, carry):
        vy = disp[1, x].astype(jnp.float32) * scale_y
        gy = half_weight(vy)
        up_y = vy > 0
        vz = disp[2, x].astype(jnp.float32) * scale_z
        right = jnp.where(lanes == 127, 0.0, jnp.maximum(ahead(vz), 0.0))
        right_w = jnp.where(lanes == 0, 0.0, 0.5 * right * (1.0 - right))
        left = jnp.minimum(vz, 0.0)
        left_w = jnp.where(
            jnp.logical_or(lanes == 0, lanes == 127), 0.0, -0.5 * left * (1.0 + left)
        )
        for f in range(5):
            value = q[f, x]
            below = back(value)
            above = ahead(value)
            slope = minmod(value - below, above - value)
            out_right = right * value + right_w * slope
            out_left = left * value + left_w * slope
            change_z = (back(out_right) - out_right) + (out_left - ahead(out_left))

            below = pltpu.roll(value, 1, 0)
            diff = value - below
            slope = minmod(diff, pltpu.roll(diff, 63, 0))
            flux = vy * jnp.where(up_y, below, value) + gy * jnp.where(
                up_y, pltpu.roll(slope, 1, 0), slope
            )
            acc[f, x] = (value + (flux - pltpu.roll(flux, 63, 0))) + change_z
        return carry

    lax.fori_loop(0, 3, planes, 0)

    late = jnp.logical_not(early)

    @pl.when(late)
    def _():
        pl.semaphore_wait(round_sem.at[0], len(along_y) + late_steps)
        greet_late(round_sem.at[1])
        for peer in along_y:
            greet(round_sem.at[1], peer)

    for copy in copies_a:
        copy.wait_recv()
    part[1] = part[0] + jnp.sum(slots_a[...], axis=0)

    def far(dz):
        other = lax.rem(level + dz, levels)
        return jnp.logical_and(other >= EARLY, jnp.abs(other - level) > 2)

    @pl.when(late)
    def _():
        for (dy, dz), copy in zip(offsets_b, copies_b):
            if dz in (3, 4, 5):
                pl.when(jnp.logical_not(far(dz)))(copy.start)
            else:
                copy.start()

    @pl.when(early)
    def _():
        pl.semaphore_wait(reply_sem.at[0], 2)
        y_up.start()

        @pl.when(level < EARLY - 1)
        def _():
            pl.semaphore_wait(reply_sem.at[2], 4 * (EARLY - 1 - level))

        for (dy, dz), copy in zip(offsets_b, copies_b):
            if dz in (0, 1, 2, 6, 7):
                pl.when(lax.rem(level + dz, levels) < EARLY)(copy.start)

    lax.fori_loop(3, 8, planes, 0)

    @pl.when(late)
    def _():
        pl.semaphore_wait(round_sem.at[1], len(along_y) + late_steps)
        for (dy, dz), copy in zip(offsets_b, copies_b):
            if dz in (3, 4, 5):
                pl.when(far(dz))(copy.start)

    @pl.when(jnp.logical_not(first[1]))
    def _():
        y_up.wait_recv()

    @pl.when(jnp.logical_not(final[1]))
    def _():
        y_down.wait_recv()

    v0, v1, v63 = [disp[1, :, r, :].astype(jnp.float32) * STEP for r in (0, 1, 63)]
    v64 = jnp.where(final[1], v63 * flag_open[3], yhigh[10])
    v0 = v0 * low_scale[1]

    def flux_row(v, behind, at, slope_behind, slope_at):
        return v * jnp.where(v > 0, behind, at) + half_weight(v) * jnp.where(
            v > 0, slope_behind, slope_at
        )

    for f in range(5):
        q0, q1, q2, q61, q62, q63 = [q[f, :, r, :] for r in (0, 1, 2, 61, 62, 63)]
        lo1 = jnp.where(first[1], q0, ylow[2 * f + 1])
        lo2 = jnp.where(first[1], q0, ylow[2 * f])
        hi0 = jnp.where(final[1], q63, yhigh[2 * f])
        hi1 = jnp.where(final[1], q63, yhigh[2 * f + 1])
        s0 = minmod(q0 - lo1, q1 - q0)
        s63 = minmod(q63 - q62, hi0 - q63)
        flux_0 = flux_row(v0, lo1, q0, minmod(lo1 - lo2, q0 - lo1), s0)
        flux_1 = flux_row(v1, q0, q1, s0, minmod(q1 - q0, q2 - q1))
        flux_63 = flux_row(v63, q62, q63, minmod(q62 - q61, q63 - q62), s63)
        flux_64 = flux_row(v64, q63, hi0, s63, minmod(hi0 - q63, hi1 - hi0))
        acc[f, :, 0, :] += flux_0 - flux_1
        acc[f, :, 1, :] += flux_1
        acc[f, :, 62, :] -= flux_63
        acc[f, :, 63, :] += flux_63 - flux_64

    @pl.when(jnp.logical_not(first[2]))
    def _():
        z_up.wait_recv()

    @pl.when(jnp.logical_not(final[2]))
    def _():
        z_down.wait_recv()

    def face(four, v):
        behind = back(four)
        diff = four - behind
        slope = minmod(diff, ahead(diff))
        flux = v * jnp.where(v > 0, behind, four) + half_weight(v) * jnp.where(
            v > 0, back(slope), slope
        )
        return slope, flux

    for half in range(2):
        own_v = zpack[10 + half]
        v_low = jnp.where(place4 == 2, own_v * low_scale[2], own_v)
        v_high = jnp.where(final[2], back(own_v) * flag_open[5], zhigh[10 + half])
        left = jnp.minimum(v_low, 0.0)
        left_w = -0.5 * left * (1.0 + left)
        right = jnp.maximum(ahead(own_v), 0.0)
        right_w = 0.5 * right * (1.0 - right)
        for f in range(5):
            j = 2 * f + half
            own = zpack[j]
            ghost_low = jnp.where(place4 == 0, pltpu.roll(own, 126, 1), ahead(own))
            ghost_high = jnp.where(place4 == 2, back(own), pltpu.roll(own, 2, 1))
            low = jnp.where(place4 < 2, jnp.where(first[2], ghost_low, zlow[j]), own)
            high = jnp.where(place4 < 2, own, jnp.where(final[2], ghost_high, zhigh[j]))
            slope_low, flux_low = face(low, v_low)
            slope_high, flux_high = face(high, v_high)
            by_left = left_w * jnp.where(place4 == 1, slope_high, slope_low)
            by_right = right_w * slope_low
            entering = jnp.where(v_low > 0, flux_low, 0.0)
            zcorr[j] = jnp.where(
                place4 == 0,
                -ahead(by_left),
                jnp.where(
                    place4 == 1,
                    by_left - ahead(flux_high) + ahead(left * own),
                    jnp.where(place4 == 2, entering + by_left - by_right, back(by_right)),
                ),
            )

    @pl.when(early)
    def _():
        pl.semaphore_wait(reply_sem.at[1], 4 * (levels - EARLY))
        for (dy, dz), copy in zip(offsets_b, copies_b):
            if dz:
                pl.when(lax.rem(level + dz, levels) >= EARLY)(copy.start)

    @pl.when(jnp.logical_not(final[0]))
    def _():
        face_copy.wait_recv()

    for i in range(9):
        if i == 0:
            v = disp[0, 0].astype(jnp.float32) * (STEP * low_scale[0])
        elif i < 8:
            v = disp[0, i].astype(jnp.float32) * STEP
        else:
            v_last = disp[0, 7].astype(jnp.float32) * (STEP * flag_open[1])
            v = jnp.where(final[0], v_last, xface[...].astype(jnp.float32) * STEP)
        vx[i] = v
        gx_w[i] = half_weight(v)

    edge_lanes = jnp.logical_or(lane8 < 2, lane8 > 125)
    for f in range(5):

        @pl.when(jnp.logical_not(first[0]))
        def _():
            up_copies[f].wait_recv()

        @pl.when(jnp.logical_not(final[0]))
        def _():
            down_copies[f].wait_recv()

        def tile(t, carry):
            part_rows = pl.ds(pl.multiple_of(t * 8, 8), 8)
            own = [q[f, i, part_rows] for i in range(8)]
            cell = (
                [jnp.where(first[0], own[0], xlow[f, r, part_rows]) for r in range(2)]
                + own
                + [jnp.where(final[0], own[7], xhigh[f, r, part_rows]) for r in range(2)]
            )
            diff = [cell[i + 1] - cell[i] for i in range(11)]
            slope = [minmod(diff[i], diff[i + 1]) for i in range(10)]
            flux = []
            for i in range(9):
                v = vx[i, part_rows]
                g = gx_w[i, part_rows]
                flux.append(
                    v * jnp.where(v > 0, cell[i + 1], cell[i + 2])
                    + g * jnp.where(v > 0, slope[i], slope[i + 1])
                )
            for i in range(8):
                move = lax.rem(254 - 4 * ((i % 4) * 8 + t), 128)
                corr = pltpu.roll(zcorr[2 * f + i // 4], move, 1)
                corr = jnp.where(edge_lanes, corr, 0.0)
                acc[f, i, part_rows] += (flux[i] - flux[i + 1]) + corr
            return carry

        lax.fori_loop(0, 8, tile, 0)

    for copy in copies_a:
        copy.wait_send()

    @pl.when(jnp.logical_not(first[0]))
    def _():
        face_copy.wait_send()

    for copy, there in (
        (y_up, final[1]),
        (y_down, first[1]),
        (z_up, final[2]),
        (z_down, first[2]),
    ):

        @pl.when(jnp.logical_not(there))
        def _():
            copy.wait_send()

    for f in range(5):

        @pl.when(jnp.logical_not(final[0]))
        def _():
            up_copies[f].wait_send()

        @pl.when(jnp.logical_not(first[0]))
        def _():
            down_copies[f].wait_send()

    for copy in copies_b:
        copy.wait_send()
    for copy in copies_b:
        copy.wait_recv()
    grand[...] = part[1] + jnp.sum(slots_b[...], axis=0)


def write_out(cells, acc, grand, new_density, new_momentum, new_energy, totals, pair, sem):
    stores = [
        pltpu.make_async_copy(acc.at[0], new_density, sem.at[0]),
        pltpu.make_async_copy(acc.at[pl.ds(1, 3)], new_momentum, sem.at[1]),
        pltpu.make_async_copy(acc.at[4], new_energy, sem.at[2]),
    ]
    for store in stores:
        store.start()
    lane1 = lax.broadcasted_iota(jnp.int32, (1, 128), 1)
    both = grand[...]
    pair[0] = jnp.sum(jnp.where(lane1 < 64, both, 0.0)) / cells
    pair[1] = jnp.sum(jnp.where(lane1 < 64, 0.0, both)) / cells
    last = pltpu.make_async_copy(pair, totals, sem.at[3])
    last.start()
    for store in stores:
        store.wait()
    last.wait()


def shards(cells, density, momentum, energy, displacement, flags):
    f32, i32 = jnp.float32, jnp.int32
    anywhere = pl.BlockSpec(memory_space=pltpu.HBM)
    local = pl.BlockSpec(memory_space=pltpu.VMEM)
    inputs = [
        pltpu.with_memory_space_constraint(a, pltpu.HBM)
        for a in (density, momentum, energy, displacement, flags)
    ]
    acc, grand = pl.pallas_call(
        kernel,
        out_shape=(
            jax.ShapeDtypeStruct((5, 8, 64, 128), f32),
            jax.ShapeDtypeStruct((1, 128), f32),
        ),
        in_specs=[anywhere] * 5,
        out_specs=(local, local),
        scratch_shapes=[
            pltpu.VMEM((5, 8, 64, 128), f32),
            pltpu.VMEM((3, 8, 64, 128), i32),
            pltpu.SMEM((6,), i32),
            pltpu.VMEM((9, 64, 128), f32),
            pltpu.VMEM((9, 64, 128), f32),
            pltpu.VMEM((5, 2, 64, 128), f32),
            pltpu.VMEM((5, 2, 64, 128), f32),
            pltpu.VMEM((64, 128), i32),
            pltpu.VMEM((10, 8, 128), f32),
            pltpu.VMEM((11, 8, 128), f32),
            pltpu.VMEM((10, 8, 128), f32),
            pltpu.VMEM((11, 8, 128), f32),
            pltpu.VMEM((12, 8, 128), f32),
            pltpu.VMEM((12, 8, 128), f32),
            pltpu.VMEM((12, 8, 128), f32),
            pltpu.VMEM((10, 8, 128), f32),
            pltpu.VMEM((2, 1, 128), f32),
            pltpu.VMEM((7, 1, 128), f32),
            pltpu.VMEM((31, 1, 128), f32),
            pltpu.SemaphoreType.DMA((9,)),
            pltpu.SemaphoreType.DMA((11,)),
            pltpu.SemaphoreType.DMA((11,)),
            pltpu.SemaphoreType.DMA((2,)),
            pltpu.SemaphoreType.DMA((2,)),
            pltpu.SemaphoreType.DMA((2,)),
            pltpu.SemaphoreType.DMA((2,)),
            pltpu.SemaphoreType.DMA((38,)),
            pltpu.SemaphoreType.DMA((38,)),
            pltpu.SemaphoreType.REGULAR((2,)),
            pltpu.SemaphoreType.REGULAR((3,)),
        ],
        compiler_params=pltpu.CompilerParams(
            collective_id=0, has_side_effects=True, vmem_limit_bytes=16 * 2**20
        ),
        name="remap",
    )(*inputs)
    return pl.pallas_call(
        functools.partial(write_out, cells),
        out_shape=(
            jax.ShapeDtypeStruct(density.shape, f32),
            jax.ShapeDtypeStruct(momentum.shape, f32),
            jax.ShapeDtypeStruct(energy.shape, f32),
            jax.ShapeDtypeStruct((2,), f32),
        ),
        in_specs=[local, local],
        out_specs=[anywhere] * 4,
        scratch_shapes=[pltpu.SMEM((2,), f32), pltpu.SemaphoreType.DMA((4,))],
        compiler_params=pltpu.CompilerParams(vmem_limit_bytes=4 * 2**20),
        name="write_out",
    )(acc, grand)


def solution(mesh):
    cells = float(mesh.shape["gx"] * mesh.shape["gy"] * mesh.shape["gz"] * 8 * 64 * 128)
    block = P("gx", "gy", "gz")
    three = P(None, "gx", "gy", "gz")
    return jax.shard_map(
        functools.partial(shards, cells),
        mesh=mesh,
        in_specs=(block, three, block, three, P()),
        out_specs=(block, three, block, P()),
        check_vma=False,
    )
```

```python
import functools

import jax
import jax.numpy as jnp
from jax import lax
from jax.experimental import pallas as pl
from jax.experimental.pallas import tpu as pltpu
from jax.sharding import PartitionSpec as P

MESH = pl.DeviceIdType.MESH
STEP = 1.0 / 256.0
EARLY = 3


def minmod(left_diff, right_diff):
    least = jnp.minimum(left_diff, right_diff)
    most = jnp.maximum(left_diff, right_diff)
    return jnp.maximum(least, jnp.minimum(most, 0.0))


def half_weight(v):
    size = jnp.abs(v)
    return 0.5 * size * (1.0 - size)


def back(block):
    return pltpu.roll(block, 1, 1)


def ahead(block):
    return pltpu.roll(block, 127, 1)


def kernel(
    density,
    momentum,
    energy,
    displacement,
    flags,
    acc,
    grand,
    q,
    disp,
    flag,
    vx,
    gx_w,
    xhalo,
    xface,
    yup,
    ydown,
    ylow,
    yhigh,
    zpack,
    zlow,
    zhigh,
    zcorr,
    part,
    slots_a,
    slots_b,
    load_sem,
    xs_sem,
    xr_sem,
    ys_sem,
    yr_sem,
    zs_sem,
    zr_sem,
    ts_sem,
    tr_sem,
    round_sem,
    reply_sem,
):
    px, py, pz = lax.axis_index("gx"), lax.axis_index("gy"), lax.axis_index("gz")
    nx, ny, nz = lax.axis_size("gx"), lax.axis_size("gy"), lax.axis_size("gz")
    core = pz % 2
    zl = (pz // 2) % 2
    flag_copy = pltpu.make_async_copy(flags, flag, load_sem.at[0])
    flag_copy.start()
    pltpu.make_async_copy(density, q.at[0], load_sem.at[1]).start()
    pltpu.make_async_copy(energy, q.at[1], load_sem.at[1]).start()
    disp_load = pltpu.make_async_copy(displacement, disp, load_sem.at[2])
    disp_load.start()
    momentum_load = pltpu.make_async_copy(momentum, q.at[pl.ds(2, 3)], load_sem.at[3])
    momentum_load.start()

    def wait_bytes(of, sem):
        pltpu.make_async_copy(of, of, sem).wait()

    def place(x=None, y=None, z=None):
        target = {}
        if x is not None:
            target["gx"] = x
        if y is not None:
            target["gy"] = y
        if z is not None:
            target["gz"] = z
        return target

    level = py * 2 + zl
    levels = 2 * ny
    early = level < EARLY

    def along_yz(dy, dz):
        chip = lax.rem(level + dz, levels)
        return place(y=chip // 2, z=lax.rem(pz + 4 * dy, nz) + 2 * (chip % 2 - zl))

    def greet(sem, peer):
        pl.semaphore_signal(sem, inc=1, device_id=peer, device_id_type=MESH)

    stage_a = [
        place(x=lax.rem(px + dx, nx), z=pz + dc * (1 - 2 * core))
        for dc in range(2)
        for dx in range(4)
        if dx or dc
    ]
    along_y = [along_yz(dy, 0) for dy in (1, 2, 3)]
    steps = [-2, -1, 1, 2]
    late_step = [
        jnp.logical_and(level + step >= EARLY, level + step < levels) for step in steps
    ]
    late_steps = sum(ok.astype(jnp.int32) for ok in late_step)
    has_across = jnp.where(core == 1, pz < nz - 1, pz > 0)
    across = place(z=lax.rem(pz + nz + 2 * core - 1, nz))

    def greet_late(sem):
        for step, ok in zip(steps, late_step):

            @pl.when(ok)
            def _():
                greet(sem, along_yz(0, step % 8))

    barrier = pltpu.get_barrier_semaphore()
    for peer in stage_a + along_y:
        greet(barrier, peer)

    @pl.when(has_across)
    def _():
        greet(barrier, across)

    @pl.when(early)
    def _():
        for dz in range(1, 8):

            @pl.when(level + dz < levels)
            def _():
                for dy in range(4):
                    greet(barrier, along_yz(dy, dz))

    @pl.when(jnp.logical_not(early))
    def _():
        greet_late(barrier)

    flag_copy.wait()
    wait_bytes(q.at[pl.ds(0, 2)], load_sem.at[1])
    disp_load.wait()

    flag_open = [flag[i].astype(jnp.float32) for i in range(6)]
    first = [px == 0, py == 0, pz == 0]
    final = [px == nx - 1, py == ny - 1, pz == nz - 1]
    low_scale = [jnp.where(first[a], flag_open[2 * a], 1.0) for a in range(3)]
    gain = [jnp.where(first[a], flag_open[2 * a] * STEP, 0.0) for a in range(3)]
    loss = [jnp.where(final[a], flag_open[2 * a + 1] * -STEP, 0.0) for a in range(3)]

    rows = lax.broadcasted_iota(jnp.int32, (64, 128), 0)
    lanes = lax.broadcasted_iota(jnp.int32, (64, 128), 1)
    weight_y = jnp.where(rows == 0, gain[1], jnp.where(rows == 63, loss[1], 0.0))
    weight_z = jnp.where(lanes == 0, gain[2], jnp.where(lanes == 127, loss[2], 0.0))

    def fold(block):
        return jnp.sum(block.reshape(8, 8, 128), axis=0)

    def plane_sum(x, sums):
        weight = (
            1.0
            + weight_y * disp[1, x].astype(jnp.float32)
            + weight_z * disp[2, x].astype(jnp.float32)
        )
        return (sums[0] + fold(q[0, x] * weight), sums[1] + fold(q[1, x] * weight))

    weight_low = gain[0] * disp[0, 0].astype(jnp.float32)
    weight_high = loss[0] * disp[0, 7].astype(jnp.float32)
    sums = tuple(fold(q[f, 0] * weight_low + q[f, 7] * weight_high) for f in (0, 1))
    sums = lax.fori_loop(0, 8, plane_sum, sums)
    lane1 = lax.broadcasted_iota(jnp.int32, (1, 128), 1)

    def halves(low, high):
        low = jnp.sum(low, axis=0, keepdims=True)
        high = jnp.sum(high, axis=0, keepdims=True)
        return jnp.where(lane1 < 64, low + pltpu.roll(low, 64, 1), high + pltpu.roll(high, 64, 1))

    part[0] = halves(*sums)
    momentum_load.wait()

    greeted = (
        len(stage_a)
        + len(along_y)
        + has_across.astype(jnp.int32)
        + jnp.where(early, 4 * level, 4 * EARLY + late_steps)
    )
    pl.semaphore_wait(barrier, greeted)

    offsets_b = sorted(
        [(dy, dz) for dy in range(4) for dz in range(8) if dy or dz],
        key=lambda o: -min(o[0], 4 - o[0]) - min(o[1], 8 - o[1]),
    )
    stage_b = [along_yz(dy, dz) for dy, dz in offsets_b]
    def total_copies(stage, peers, slots):
        return [
            pltpu.make_async_remote_copy(
                src_ref=part.at[stage],
                dst_ref=slots.at[i],
                send_sem=ts_sem.at[stage],
                recv_sem=tr_sem.at[stage],
                device_id=peer,
                device_id_type=MESH,
            )
            for i, peer in enumerate(peers)
        ]

    copies_a = total_copies(0, stage_a, slots_a)
    copies_b = total_copies(1, stage_b, slots_b)
    for copy in copies_a:
        copy.start()

    @pl.when(jnp.logical_not(early))
    def _():
        greet_late(round_sem.at[0])
        for peer in along_y:
            greet(round_sem.at[0], peer)

    def remote(src, dst, send_sem, recv_sem, peer):
        return pltpu.make_async_remote_copy(
            src_ref=src,
            dst_ref=dst,
            send_sem=send_sem,
            recv_sem=recv_sem,
            device_id=peer,
            device_id_type=MESH,
        )

    x_next = place(x=lax.rem(px + 1, nx))
    x_prev = place(x=lax.rem(px + nx - 1, nx))
    face_copy = remote(disp.at[0, 0], xface, xs_sem.at[2], xr_sem.at[5], x_prev)
    up_copies = [
        remote(q.at[f, pl.ds(6, 2)], xhalo.at[f, 0], xs_sem.at[0], xr_sem.at[f], x_next) for f in range(5)
    ]
    down_copies = [
        remote(q.at[f, pl.ds(0, 2)], xhalo.at[f, 1], xs_sem.at[1], xr_sem.at[f], x_prev)
        for f in range(5)
    ]

    @pl.when(jnp.logical_not(first[0]))
    def _():
        face_copy.start()

    for f in range(5):

        @pl.when(jnp.logical_not(final[0]))
        def _():
            up_copies[f].start()

        @pl.when(jnp.logical_not(first[0]))
        def _():
            down_copies[f].start()

    for f in range(5):
        for r in range(2):
            yup[2 * f + r] = q[f, :, 62 + r, :]
            ydown[2 * f + r] = q[f, :, r, :]
    ydown[10] = disp[1, :, 0, :].astype(jnp.float32) * STEP

    y_up = remote(yup, ylow, ys_sem.at[0], yr_sem.at[0], place(y=lax.rem(py + 1, ny)))
    y_down = remote(ydown, yhigh, ys_sem.at[1], yr_sem.at[1], place(y=lax.rem(py + ny - 1, ny)))

    @pl.when(jnp.logical_not(first[1]))
    def _():
        y_down.start()

    @pl.when(jnp.logical_not(jnp.logical_or(final[1], early)))
    def _():
        y_up.start()

    lane8 = lax.broadcasted_iota(jnp.int32, (8, 128), 1)
    slot_of = lane8 // 4
    place4 = lane8 % 4

    def pack(source, base, half):
        packed = jnp.zeros((8, 128), jnp.float32)
        for xx in range(4):
            plane = source[base, half * 4 + xx].astype(jnp.float32)
            for t in range(8):
                k = xx * 8 + t
                moved = pltpu.roll(plane[8 * t : 8 * t + 8], (4 * k + 2) % 128, 1)
                packed = jnp.where(slot_of == k, moved, packed)
        return packed

    for f in range(5):
        for half in range(2):
            zpack[2 * f + half] = pack(q, f, half)
    for half in range(2):
        zpack[10 + half] = pack(disp, 2, half) * STEP

    z_up = remote(zpack, zlow, zs_sem.at[0], zr_sem.at[0], place(z=lax.rem(pz + 1, nz)))
    z_down = remote(zpack, zhigh, zs_sem.at[1], zr_sem.at[1], place(z=lax.rem(pz + nz - 1, nz)))

    @pl.when(jnp.logical_not(final[2]))
    def _():
        z_up.start()

    @pl.when(jnp.logical_not(first[2]))
    def _():
        z_down.start()

    for back_step in (1, 2):

        @pl.when(jnp.logical_and(level - back_step >= 0, level - back_step < EARLY))
        def _():
            greet(reply_sem.at[0], along_yz(0, 8 - back_step))

    for target in range(EARLY):

        @pl.when(target < level)
        def _():
            for dy in range(4):
                greet(
                    reply_sem.at[jnp.where(early, 2, 1)],
                    along_yz(dy, lax.rem(levels + target - level, levels)),
                )

    scale_y = jnp.where(
        jnp.logical_or(rows < 2, rows == 63), 0.0, STEP
    )
    scale_z = jnp.where(lanes == 0, STEP * low_scale[2], STEP)

    def planes(x, carry):
        vy = disp[1, x].astype(jnp.float32) * scale_y
        gy = half_weight(vy)
        up_y = vy > 0
        vz = disp[2, x].astype(jnp.float32) * scale_z
        right = jnp.where(lanes == 127, 0.0, jnp.maximum(ahead(vz), 0.0))
        right_w = jnp.where(lanes == 0, 0.0, 0.5 * right * (1.0 - right))
        left = jnp.minimum(vz, 0.0)
        left_w = jnp.where(
            jnp.logical_or(lanes == 0, lanes == 127), 0.0, -0.5 * left * (1.0 + left)
        )
        for f in range(5):
            value = q[f, x]
            below = back(value)
            above = ahead(value)
            slope = minmod(value - below, above - value)
            out_right = right * value + right_w * slope
            out_left = left * value + left_w * slope
            change_z = (back(out_right) - out_right) + (out_left - ahead(out_left))

            below = pltpu.roll(value, 1, 0)
            diff = value - below
            slope = minmod(diff, pltpu.roll(diff, 63, 0))
            flux = vy * jnp.where(up_y, below, value) + gy * jnp.where(
                up_y, pltpu.roll(slope, 1, 0), slope
            )
            acc[f, x] = (value + (flux - pltpu.roll(flux, 63, 0))) + change_z
        return carry

    lax.fori_loop(0, 3, planes, 0)

    late = jnp.logical_not(early)

    @pl.when(late)
    def _():
        pl.semaphore_wait(round_sem.at[0], len(along_y) + late_steps)
        greet_late(round_sem.at[1])
        for peer in along_y:
            greet(round_sem.at[1], peer)

    wait_bytes(slots_a, tr_sem.at[0])
    part[1] = part[0] + jnp.sum(slots_a[...], axis=0)

    def far(dz):
        other = lax.rem(level + dz, levels)
        return jnp.logical_and(other >= EARLY, jnp.abs(other - level) > 2)

    @pl.when(late)
    def _():
        for (dy, dz), copy in zip(offsets_b, copies_b):
            if dz in (3, 4, 5):
                pl.when(jnp.logical_not(far(dz)))(copy.start)
            else:
                copy.start()

    @pl.when(early)
    def _():
        pl.semaphore_wait(reply_sem.at[0], 2)
        y_up.start()

        @pl.when(level < EARLY - 1)
        def _():
            pl.semaphore_wait(reply_sem.at[2], 4 * (EARLY - 1 - level))

        for (dy, dz), copy in zip(offsets_b, copies_b):
            if dz in (0, 1, 2, 6, 7):
                pl.when(lax.rem(level + dz, levels) < EARLY)(copy.start)

    lax.fori_loop(3, 8, planes, 0)

    @pl.when(late)
    def _():
        pl.semaphore_wait(round_sem.at[1], len(along_y) + late_steps)
        for (dy, dz), copy in zip(offsets_b, copies_b):
            if dz in (3, 4, 5):
                pl.when(far(dz))(copy.start)

    @pl.when(jnp.logical_not(first[1]))
    def _():
        y_up.wait_recv()

    @pl.when(jnp.logical_not(final[1]))
    def _():
        y_down.wait_recv()

    v0, v1, v63 = [disp[1, :, r, :].astype(jnp.float32) * STEP for r in (0, 1, 63)]
    v64 = jnp.where(final[1], v63 * flag_open[3], yhigh[10])
    v0 = v0 * low_scale[1]

    def flux_row(v, behind, at, slope_behind, slope_at):
        return v * jnp.where(v > 0, behind, at) + half_weight(v) * jnp.where(
            v > 0, slope_behind, slope_at
        )

    for f in range(5):
        q0, q1, q2, q61, q62, q63 = [q[f, :, r, :] for r in (0, 1, 2, 61, 62, 63)]
        lo1 = jnp.where(first[1], q0, ylow[2 * f + 1])
        lo2 = jnp.where(first[1], q0, ylow[2 * f])
        hi0 = jnp.where(final[1], q63, yhigh[2 * f])
        hi1 = jnp.where(final[1], q63, yhigh[2 * f + 1])
        s0 = minmod(q0 - lo1, q1 - q0)
        s63 = minmod(q63 - q62, hi0 - q63)
        flux_0 = flux_row(v0, lo1, q0, minmod(lo1 - lo2, q0 - lo1), s0)
        flux_1 = flux_row(v1, q0, q1, s0, minmod(q1 - q0, q2 - q1))
        flux_63 = flux_row(v63, q62, q63, minmod(q62 - q61, q63 - q62), s63)
        flux_64 = flux_row(v64, q63, hi0, s63, minmod(hi0 - q63, hi1 - hi0))
        acc[f, :, 0, :] += flux_0 - flux_1
        acc[f, :, 1, :] += flux_1
        acc[f, :, 62, :] -= flux_63
        acc[f, :, 63, :] += flux_63 - flux_64

    @pl.when(jnp.logical_not(first[2]))
    def _():
        z_up.wait_recv()

    @pl.when(jnp.logical_not(final[2]))
    def _():
        z_down.wait_recv()

    def face(four, v):
        behind = back(four)
        diff = four - behind
        slope = minmod(diff, ahead(diff))
        flux = v * jnp.where(v > 0, behind, four) + half_weight(v) * jnp.where(
            v > 0, back(slope), slope
        )
        return slope, flux

    for half in range(2):
        own_v = zpack[10 + half]
        v_low = jnp.where(place4 == 2, own_v * low_scale[2], own_v)
        v_high = jnp.where(final[2], back(own_v) * flag_open[5], zhigh[10 + half])
        left = jnp.minimum(v_low, 0.0)
        left_w = -0.5 * left * (1.0 + left)
        right = jnp.maximum(ahead(own_v), 0.0)
        right_w = 0.5 * right * (1.0 - right)
        for f in range(5):
            j = 2 * f + half
            own = zpack[j]
            ghost_low = jnp.where(place4 == 0, pltpu.roll(own, 126, 1), ahead(own))
            ghost_high = jnp.where(place4 == 2, back(own), pltpu.roll(own, 2, 1))
            low = jnp.where(place4 < 2, jnp.where(first[2], ghost_low, zlow[j]), own)
            high = jnp.where(place4 < 2, own, jnp.where(final[2], ghost_high, zhigh[j]))
            slope_low, flux_low = face(low, v_low)
            slope_high, flux_high = face(high, v_high)
            by_left = left_w * jnp.where(place4 == 1, slope_high, slope_low)
            by_right = right_w * slope_low
            entering = jnp.where(v_low > 0, flux_low, 0.0)
            zcorr[j] = jnp.where(
                place4 == 0,
                -ahead(by_left),
                jnp.where(
                    place4 == 1,
                    by_left - ahead(flux_high) + ahead(left * own),
                    jnp.where(place4 == 2, entering + by_left - by_right, back(by_right)),
                ),
            )

    @pl.when(early)
    def _():
        pl.semaphore_wait(reply_sem.at[1], 4 * (levels - EARLY))
        for (dy, dz), copy in zip(offsets_b, copies_b):
            if dz:
                pl.when(lax.rem(level + dz, levels) >= EARLY)(copy.start)

    @pl.when(jnp.logical_not(final[0]))
    def _():
        face_copy.wait_recv()

    for i in range(9):
        if i == 0:
            v = disp[0, 0].astype(jnp.float32) * (STEP * low_scale[0])
        elif i < 8:
            v = disp[0, i].astype(jnp.float32) * STEP
        else:
            v_last = disp[0, 7].astype(jnp.float32) * (STEP * flag_open[1])
            v = jnp.where(final[0], v_last, xface[...].astype(jnp.float32) * STEP)
        vx[i] = v
        gx_w[i] = half_weight(v)

    inner = jnp.logical_not(jnp.logical_or(first[0], final[0]))
    edge_lanes = jnp.logical_or(lane8 < 2, lane8 > 125)
    for f in range(5):

        @pl.when(inner)
        def _():
            wait_bytes(xhalo.at[f], xr_sem.at[f])

        @pl.when(jnp.logical_not(inner))
        def _():
            wait_bytes(xhalo.at[f, 0], xr_sem.at[f])

        def tile(t, carry):
            part_rows = pl.ds(pl.multiple_of(t * 8, 8), 8)
            own = [q[f, i, part_rows] for i in range(8)]
            cell = (
                [jnp.where(first[0], own[0], xhalo[f, 0, r, part_rows]) for r in range(2)]
                + own
                + [jnp.where(final[0], own[7], xhalo[f, 1, r, part_rows]) for r in range(2)]
            )
            diff = [cell[i + 1] - cell[i] for i in range(11)]
            slope = [minmod(diff[i], diff[i + 1]) for i in range(10)]
            flux = []
            for i in range(9):
                v = vx[i, part_rows]
                g = gx_w[i, part_rows]
                flux.append(
                    v * jnp.where(v > 0, cell[i + 1], cell[i + 2])
                    + g * jnp.where(v > 0, slope[i], slope[i + 1])
                )
            for i in range(8):
                move = lax.rem(254 - 4 * ((i % 4) * 8 + t), 128)
                corr = pltpu.roll(zcorr[2 * f + i // 4], move, 1)
                corr = jnp.where(edge_lanes, corr, 0.0)
                acc[f, i, part_rows] += (flux[i] - flux[i + 1]) + corr
            return carry

        lax.fori_loop(0, 8, tile, 0)

    wait_bytes(slots_a, ts_sem.at[0])

    @pl.when(jnp.logical_not(first[0]))
    def _():
        face_copy.wait_send()

    for copy, there in (
        (y_up, final[1]),
        (y_down, first[1]),
        (z_up, final[2]),
        (z_down, first[2]),
    ):

        @pl.when(jnp.logical_not(there))
        def _():
            copy.wait_send()

    @pl.when(jnp.logical_not(final[0]))
    def _():
        wait_bytes(xhalo.at[:, 0], xs_sem.at[0])

    @pl.when(jnp.logical_not(first[0]))
    def _():
        wait_bytes(xhalo.at[:, 1], xs_sem.at[1])

    wait_bytes(slots_b, ts_sem.at[1])
    wait_bytes(slots_b, tr_sem.at[1])
    grand[...] = part[1] + jnp.sum(slots_b[...], axis=0)


def write_out(cells, acc, grand, new_density, new_momentum, new_energy, totals, pair, sem):
    stores = [
        pltpu.make_async_copy(acc.at[0], new_density, sem.at[0]),
        pltpu.make_async_copy(acc.at[1], new_energy, sem.at[0]),
    ] + [pltpu.make_async_copy(acc.at[2 + c], new_momentum.at[c], sem.at[0]) for c in range(3)]
    for store in stores:
        store.start()
    lane1 = lax.broadcasted_iota(jnp.int32, (1, 128), 1)
    both = grand[...]
    pair[0] = jnp.sum(jnp.where(lane1 < 64, both, 0.0)) / cells
    pair[1] = jnp.sum(jnp.where(lane1 < 64, 0.0, both)) / cells
    last = pltpu.make_async_copy(pair, totals, sem.at[1])
    last.start()
    pltpu.make_async_copy(acc, acc, sem.at[0]).wait()
    last.wait()


def shards(cells, density, momentum, energy, displacement, flags):
    f32, i32 = jnp.float32, jnp.int32
    anywhere = pl.BlockSpec(memory_space=pltpu.HBM)
    local = pl.BlockSpec(memory_space=pltpu.VMEM)
    inputs = [
        pltpu.with_memory_space_constraint(a, pltpu.HBM)
        for a in (density, momentum, energy, displacement, flags)
    ]
    acc, grand = pl.pallas_call(
        kernel,
        out_shape=(
            jax.ShapeDtypeStruct((5, 8, 64, 128), f32),
            jax.ShapeDtypeStruct((1, 128), f32),
        ),
        in_specs=[anywhere] * 5,
        out_specs=(local, local),
        scratch_shapes=[
            pltpu.VMEM((5, 8, 64, 128), f32),
            pltpu.VMEM((3, 8, 64, 128), i32),
            pltpu.SMEM((6,), i32),
            pltpu.VMEM((9, 64, 128), f32),
            pltpu.VMEM((9, 64, 128), f32),
            pltpu.VMEM((5, 2, 2, 64, 128), f32),
            pltpu.VMEM((64, 128), i32),
            pltpu.VMEM((10, 8, 128), f32),
            pltpu.VMEM((11, 8, 128), f32),
            pltpu.VMEM((10, 8, 128), f32),
            pltpu.VMEM((11, 8, 128), f32),
            pltpu.VMEM((12, 8, 128), f32),
            pltpu.VMEM((12, 8, 128), f32),
            pltpu.VMEM((12, 8, 128), f32),
            pltpu.VMEM((10, 8, 128), f32),
            pltpu.VMEM((2, 1, 128), f32),
            pltpu.VMEM((7, 1, 128), f32),
            pltpu.VMEM((31, 1, 128), f32),
            pltpu.SemaphoreType.DMA((4,)),
            pltpu.SemaphoreType.DMA((3,)),
            pltpu.SemaphoreType.DMA((6,)),
            pltpu.SemaphoreType.DMA((2,)),
            pltpu.SemaphoreType.DMA((2,)),
            pltpu.SemaphoreType.DMA((2,)),
            pltpu.SemaphoreType.DMA((2,)),
            pltpu.SemaphoreType.DMA((2,)),
            pltpu.SemaphoreType.DMA((2,)),
            pltpu.SemaphoreType.REGULAR((2,)),
            pltpu.SemaphoreType.REGULAR((3,)),
        ],
        compiler_params=pltpu.CompilerParams(
            collective_id=0, has_side_effects=True, vmem_limit_bytes=16 * 2**20
        ),
        name="remap",
    )(*inputs)
    return pl.pallas_call(
        functools.partial(write_out, cells),
        out_shape=(
            jax.ShapeDtypeStruct(density.shape, f32),
            jax.ShapeDtypeStruct(momentum.shape, f32),
            jax.ShapeDtypeStruct(energy.shape, f32),
            jax.ShapeDtypeStruct((2,), f32),
        ),
        in_specs=[local, local],
        out_specs=[anywhere] * 4,
        scratch_shapes=[pltpu.SMEM((2,), f32), pltpu.SemaphoreType.DMA((2,))],
        compiler_params=pltpu.CompilerParams(vmem_limit_bytes=4 * 2**20),
        name="write_out",
    )(acc, grand)


def solution(mesh):
    cells = float(mesh.shape["gx"] * mesh.shape["gy"] * mesh.shape["gz"] * 8 * 64 * 128)
    block = P("gx", "gy", "gz")
    three = P(None, "gx", "gy", "gz")
    return jax.shard_map(
        functools.partial(shards, cells),
        mesh=mesh,
        in_specs=(block, three, block, three, P()),
        out_specs=(block, three, block, P()),
        check_vma=False,
    )
```

```python
import functools

import jax
import jax.numpy as jnp
from jax import lax
from jax.experimental import pallas as pl
from jax.experimental.pallas import tpu as pltpu
from jax.sharding import PartitionSpec as P

MESH = pl.DeviceIdType.MESH
STEP = 1.0 / 256.0
EARLY = 3


def minmod(left_diff, right_diff):
    least = jnp.minimum(left_diff, right_diff)
    most = jnp.maximum(left_diff, right_diff)
    return jnp.maximum(least, jnp.minimum(most, 0.0))


def half_weight(v):
    size = jnp.abs(v)
    return 0.5 * size * (1.0 - size)


def back(block):
    return pltpu.roll(block, 1, 1)


def ahead(block):
    return pltpu.roll(block, 127, 1)


def kernel(
    density,
    momentum,
    energy,
    displacement,
    flags,
    acc,
    grand,
    q,
    disp,
    flag,
    vx,
    gx_w,
    xhalo,
    xface,
    yup,
    ydown,
    ylow,
    yhigh,
    zpack,
    zlow,
    zhigh,
    zcorr,
    part,
    slots_a,
    slots_b,
    load_sem,
    xs_sem,
    xr_sem,
    ys_sem,
    yr_sem,
    zs_sem,
    zr_sem,
    ts_sem,
    tr_sem,
    round_sem,
    reply_sem,
):
    px, py, pz = lax.axis_index("gx"), lax.axis_index("gy"), lax.axis_index("gz")
    nx, ny, nz = lax.axis_size("gx"), lax.axis_size("gy"), lax.axis_size("gz")
    core = pz % 2
    zl = (pz // 2) % 2
    flag_copy = pltpu.make_async_copy(flags, flag, load_sem.at[0])
    flag_copy.start()
    pltpu.make_async_copy(density, q.at[0], load_sem.at[1]).start()
    pltpu.make_async_copy(energy, q.at[1], load_sem.at[1]).start()
    disp_load = pltpu.make_async_copy(displacement, disp, load_sem.at[2])
    disp_load.start()
    momentum_load = pltpu.make_async_copy(momentum, q.at[pl.ds(2, 3)], load_sem.at[3])
    momentum_load.start()

    def wait_bytes(of, sem):
        pltpu.make_async_copy(of, of, sem).wait()

    def place(x=None, y=None, z=None):
        target = {}
        if x is not None:
            target["gx"] = x
        if y is not None:
            target["gy"] = y
        if z is not None:
            target["gz"] = z
        return target

    level = py * 2 + zl
    levels = 2 * ny
    early = level < EARLY

    def along_yz(dy, dz):
        chip = lax.rem(level + dz, levels)
        return place(y=chip // 2, z=lax.rem(pz + 4 * dy, nz) + 2 * (chip % 2 - zl))

    def greet(sem, peer):
        pl.semaphore_signal(sem, inc=1, device_id=peer, device_id_type=MESH)

    stage_a = [
        place(x=lax.rem(px + dx, nx), z=pz + dc * (1 - 2 * core))
        for dc in range(2)
        for dx in range(4)
        if dx or dc
    ]
    along_y = [along_yz(dy, 0) for dy in (1, 2, 3)]
    steps = [-2, -1, 1, 2]
    late_step = [
        jnp.logical_and(level + step >= EARLY, level + step < levels) for step in steps
    ]
    late_steps = sum(ok.astype(jnp.int32) for ok in late_step)
    has_across = jnp.where(core == 1, pz < nz - 1, pz > 0)
    across = place(z=lax.rem(pz + nz + 2 * core - 1, nz))

    def greet_late(sem):
        for step, ok in zip(steps, late_step):

            @pl.when(ok)
            def _():
                greet(sem, along_yz(0, step % 8))

    barrier = pltpu.get_barrier_semaphore()
    for peer in stage_a + along_y:
        greet(barrier, peer)

    @pl.when(has_across)
    def _():
        greet(barrier, across)

    @pl.when(early)
    def _():
        for dz in range(1, 8):

            @pl.when(level + dz < levels)
            def _():
                for dy in range(4):
                    greet(barrier, along_yz(dy, dz))

    @pl.when(jnp.logical_not(early))
    def _():
        greet_late(barrier)

    flag_copy.wait()
    wait_bytes(q.at[pl.ds(0, 2)], load_sem.at[1])
    disp_load.wait()

    flag_open = [flag[i].astype(jnp.float32) for i in range(6)]
    first = [px == 0, py == 0, pz == 0]
    final = [px == nx - 1, py == ny - 1, pz == nz - 1]
    low_scale = [jnp.where(first[a], flag_open[2 * a], 1.0) for a in range(3)]
    gain = [jnp.where(first[a], flag_open[2 * a] * STEP, 0.0) for a in range(3)]
    loss = [jnp.where(final[a], flag_open[2 * a + 1] * -STEP, 0.0) for a in range(3)]

    rows = lax.broadcasted_iota(jnp.int32, (64, 128), 0)
    lanes = lax.broadcasted_iota(jnp.int32, (64, 128), 1)
    weight_y = jnp.where(rows == 0, gain[1], jnp.where(rows == 63, loss[1], 0.0))
    weight_z = jnp.where(lanes == 0, gain[2], jnp.where(lanes == 127, loss[2], 0.0))

    def fold(block):
        return jnp.sum(block.reshape(8, 8, 128), axis=0)

    def plane_sum(x, sums):
        weight = (
            1.0
            + weight_y * disp[1, x].astype(jnp.float32)
            + weight_z * disp[2, x].astype(jnp.float32)
        )
        return (sums[0] + fold(q[0, x] * weight), sums[1] + fold(q[1, x] * weight))

    weight_low = gain[0] * disp[0, 0].astype(jnp.float32)
    weight_high = loss[0] * disp[0, 7].astype(jnp.float32)
    sums = tuple(fold(q[f, 0] * weight_low + q[f, 7] * weight_high) for f in (0, 1))
    sums = lax.fori_loop(0, 8, plane_sum, sums)
    lane1 = lax.broadcasted_iota(jnp.int32, (1, 128), 1)

    def halves(low, high):
        low = jnp.sum(low, axis=0, keepdims=True)
        high = jnp.sum(high, axis=0, keepdims=True)
        return jnp.where(lane1 < 64, low + pltpu.roll(low, 64, 1), high + pltpu.roll(high, 64, 1))

    part[0] = halves(*sums)
    momentum_load.wait()

    greeted = (
        len(stage_a)
        + len(along_y)
        + has_across.astype(jnp.int32)
        + jnp.where(early, 4 * level, 4 * EARLY + late_steps)
    )
    pl.semaphore_wait(barrier, greeted)

    offsets_b = sorted(
        [(dy, dz) for dy in range(4) for dz in range(8) if dy or dz],
        key=lambda o: -min(o[0], 4 - o[0]) - min(o[1], 8 - o[1]),
    )
    stage_b = [along_yz(dy, dz) for dy, dz in offsets_b]
    def remote(src, dst, send_sem, recv_sem, peer):
        return pltpu.make_async_remote_copy(
            src_ref=src,
            dst_ref=dst,
            send_sem=send_sem,
            recv_sem=recv_sem,
            device_id=peer,
            device_id_type=MESH,
        )

    copies_a = [
        remote(part.at[0], slots_a.at[i], ts_sem.at[0], tr_sem.at[0], peer)
        for i, peer in enumerate(stage_a)
    ]
    slot = level * 4 + pz // 4
    arrival = tr_sem.at[jnp.where(early, 1, 2)]
    copies_b = [
        remote(part.at[1], slots_b.at[slot], ts_sem.at[1], arrival, peer) for peer in stage_b
    ]
    for copy in copies_a:
        copy.start()

    @pl.when(jnp.logical_not(early))
    def _():
        greet_late(round_sem.at[0])
        for peer in along_y:
            greet(round_sem.at[0], peer)

    for back_step in (1, 2):

        @pl.when(jnp.logical_and(level - back_step >= 0, level - back_step < EARLY))
        def _():
            greet(reply_sem.at[0], along_yz(0, 8 - back_step))

    @pl.when(early)
    def _():
        for target in range(EARLY - 1):

            @pl.when(target < level)
            def _():
                for dy in range(4):
                    greet(reply_sem.at[2], along_yz(dy, lax.rem(levels + target - level, levels)))

    @pl.when(jnp.logical_not(early))
    def _():
        greet(reply_sem.at[1], along_yz(0, lax.rem(levels + EARLY - 1 - level, levels)))

    x_next = place(x=lax.rem(px + 1, nx))
    x_prev = place(x=lax.rem(px + nx - 1, nx))
    face_copy = remote(disp.at[0, 0], xface, xs_sem.at[2], xr_sem.at[5], x_prev)
    up_copies = [
        remote(q.at[f, pl.ds(6, 2)], xhalo.at[f, 0], xs_sem.at[0], xr_sem.at[f], x_next) for f in range(5)
    ]
    down_copies = [
        remote(q.at[f, pl.ds(0, 2)], xhalo.at[f, 1], xs_sem.at[1], xr_sem.at[f], x_prev)
        for f in range(5)
    ]

    @pl.when(jnp.logical_not(first[0]))
    def _():
        face_copy.start()

    for f in range(5):

        @pl.when(jnp.logical_not(final[0]))
        def _():
            up_copies[f].start()

        @pl.when(jnp.logical_not(first[0]))
        def _():
            down_copies[f].start()

    for f in range(5):
        for r in range(2):
            yup[2 * f + r] = q[f, :, 62 + r, :]
            ydown[2 * f + r] = q[f, :, r, :]
    ydown[10] = disp[1, :, 0, :].astype(jnp.float32) * STEP

    y_up = remote(yup, ylow, ys_sem.at[0], yr_sem.at[0], place(y=lax.rem(py + 1, ny)))
    y_down = remote(ydown, yhigh, ys_sem.at[1], yr_sem.at[1], place(y=lax.rem(py + ny - 1, ny)))

    @pl.when(jnp.logical_not(first[1]))
    def _():
        y_down.start()

    @pl.when(jnp.logical_not(jnp.logical_or(final[1], early)))
    def _():
        y_up.start()

    lane8 = lax.broadcasted_iota(jnp.int32, (8, 128), 1)
    slot_of = lane8 // 4
    place4 = lane8 % 4

    def pack(source, base, half):
        packed = jnp.zeros((8, 128), jnp.float32)
        for xx in range(4):
            plane = source[base, half * 4 + xx].astype(jnp.float32)
            for t in range(8):
                k = xx * 8 + t
                moved = pltpu.roll(plane[8 * t : 8 * t + 8], (4 * k + 2) % 128, 1)
                packed = jnp.where(slot_of == k, moved, packed)
        return packed

    for f in range(5):
        for half in range(2):
            zpack[2 * f + half] = pack(q, f, half)
    for half in range(2):
        zpack[10 + half] = pack(disp, 2, half) * STEP

    z_up = remote(zpack, zlow, zs_sem.at[0], zr_sem.at[0], place(z=lax.rem(pz + 1, nz)))
    z_down = remote(zpack, zhigh, zs_sem.at[1], zr_sem.at[1], place(z=lax.rem(pz + nz - 1, nz)))

    @pl.when(jnp.logical_not(final[2]))
    def _():
        z_up.start()

    @pl.when(jnp.logical_not(first[2]))
    def _():
        z_down.start()

    scale_y = jnp.where(
        jnp.logical_or(rows < 2, rows == 63), 0.0, STEP
    )
    scale_z = jnp.where(lanes == 0, STEP * low_scale[2], STEP)

    def planes(x, carry):
        vy = disp[1, x].astype(jnp.float32) * scale_y
        gy = half_weight(vy)
        up_y = vy > 0
        vz = disp[2, x].astype(jnp.float32) * scale_z
        right = jnp.where(lanes == 127, 0.0, jnp.maximum(ahead(vz), 0.0))
        right_w = jnp.where(lanes == 0, 0.0, 0.5 * right * (1.0 - right))
        left = jnp.minimum(vz, 0.0)
        left_w = jnp.where(
            jnp.logical_or(lanes == 0, lanes == 127), 0.0, -0.5 * left * (1.0 + left)
        )
        for f in range(5):
            value = q[f, x]
            below = back(value)
            above = ahead(value)
            slope = minmod(value - below, above - value)
            out_right = right * value + right_w * slope
            out_left = left * value + left_w * slope
            change_z = (back(out_right) - out_right) + (out_left - ahead(out_left))

            below = pltpu.roll(value, 1, 0)
            diff = value - below
            slope = minmod(diff, pltpu.roll(diff, 63, 0))
            flux = vy * jnp.where(up_y, below, value) + gy * jnp.where(
                up_y, pltpu.roll(slope, 1, 0), slope
            )
            acc[f, x] = (value + (flux - pltpu.roll(flux, 63, 0))) + change_z
        return carry

    lax.fori_loop(0, 3, planes, 0)

    late = jnp.logical_not(early)

    @pl.when(late)
    def _():
        pl.semaphore_wait(round_sem.at[0], len(along_y) + late_steps)
        greet_late(round_sem.at[1])
        for peer in along_y:
            greet(round_sem.at[1], peer)

    wait_bytes(slots_a, tr_sem.at[0])
    group = part[0] + jnp.sum(slots_a[...], axis=0)
    part[1] = group
    slots_b[slot] = group

    def far(dz):
        other = lax.rem(level + dz, levels)
        return jnp.logical_and(other >= EARLY, jnp.abs(other - level) > 2)

    @pl.when(late)
    def _():
        for (dy, dz), copy in zip(offsets_b, copies_b):
            if dz in (3, 4, 5):
                pl.when(jnp.logical_not(far(dz)))(copy.start)
            else:
                copy.start()

    @pl.when(early)
    def _():
        for (dy, dz), copy in zip(offsets_b, copies_b):
            if dz in (0, 6, 7):
                pl.when(level + dz >= (levels if dz else 0))(copy.start)

        @pl.when(level < EARLY - 1)
        def _():
            pl.semaphore_wait(reply_sem.at[2], 4 * (EARLY - 1 - level))

        for (dy, dz), copy in zip(offsets_b, copies_b):
            if dz in (1, 2):
                pl.when(level + dz < EARLY)(copy.start)
        pl.semaphore_wait(reply_sem.at[0], 2)
        y_up.start()

    lax.fori_loop(3, 6, planes, 0)

    @pl.when(late)
    def _():
        pl.semaphore_wait(round_sem.at[1], len(along_y) + late_steps)
        for (dy, dz), copy in zip(offsets_b, copies_b):
            if dz in (3, 4, 5):
                pl.when(far(dz))(copy.start)

    lax.fori_loop(6, 8, planes, 0)

    @pl.when(jnp.logical_not(first[1]))
    def _():
        y_up.wait_recv()

    @pl.when(jnp.logical_not(final[1]))
    def _():
        y_down.wait_recv()

    v0, v1, v63 = [disp[1, :, r, :].astype(jnp.float32) * STEP for r in (0, 1, 63)]
    v64 = jnp.where(final[1], v63 * flag_open[3], yhigh[10])
    v0 = v0 * low_scale[1]

    def flux_row(v, behind, at, slope_behind, slope_at):
        return v * jnp.where(v > 0, behind, at) + half_weight(v) * jnp.where(
            v > 0, slope_behind, slope_at
        )

    for f in range(5):
        q0, q1, q2, q61, q62, q63 = [q[f, :, r, :] for r in (0, 1, 2, 61, 62, 63)]
        lo1 = jnp.where(first[1], q0, ylow[2 * f + 1])
        lo2 = jnp.where(first[1], q0, ylow[2 * f])
        hi0 = jnp.where(final[1], q63, yhigh[2 * f])
        hi1 = jnp.where(final[1], q63, yhigh[2 * f + 1])
        s0 = minmod(q0 - lo1, q1 - q0)
        s63 = minmod(q63 - q62, hi0 - q63)
        flux_0 = flux_row(v0, lo1, q0, minmod(lo1 - lo2, q0 - lo1), s0)
        flux_1 = flux_row(v1, q0, q1, s0, minmod(q1 - q0, q2 - q1))
        flux_63 = flux_row(v63, q62, q63, minmod(q62 - q61, q63 - q62), s63)
        flux_64 = flux_row(v64, q63, hi0, s63, minmod(hi0 - q63, hi1 - hi0))
        acc[f, :, 0, :] += flux_0 - flux_1
        acc[f, :, 1, :] += flux_1
        acc[f, :, 62, :] -= flux_63
        acc[f, :, 63, :] += flux_63 - flux_64

    @pl.when(jnp.logical_not(first[2]))
    def _():
        z_up.wait_recv()

    @pl.when(jnp.logical_not(final[2]))
    def _():
        z_down.wait_recv()

    def face(four, v):
        behind = back(four)
        diff = four - behind
        slope = minmod(diff, ahead(diff))
        flux = v * jnp.where(v > 0, behind, four) + half_weight(v) * jnp.where(
            v > 0, back(slope), slope
        )
        return slope, flux

    for half in range(2):
        own_v = zpack[10 + half]
        v_low = jnp.where(place4 == 2, own_v * low_scale[2], own_v)
        v_high = jnp.where(final[2], back(own_v) * flag_open[5], zhigh[10 + half])
        left = jnp.minimum(v_low, 0.0)
        left_w = -0.5 * left * (1.0 + left)
        right = jnp.maximum(ahead(own_v), 0.0)
        right_w = 0.5 * right * (1.0 - right)
        for f in range(5):
            j = 2 * f + half
            own = zpack[j]
            ghost_low = jnp.where(place4 == 0, pltpu.roll(own, 126, 1), ahead(own))
            ghost_high = jnp.where(place4 == 2, back(own), pltpu.roll(own, 2, 1))
            low = jnp.where(place4 < 2, jnp.where(first[2], ghost_low, zlow[j]), own)
            high = jnp.where(place4 < 2, own, jnp.where(final[2], ghost_high, zhigh[j]))
            slope_low, flux_low = face(low, v_low)
            slope_high, flux_high = face(high, v_high)
            by_left = left_w * jnp.where(place4 == 1, slope_high, slope_low)
            by_right = right_w * slope_low
            entering = jnp.where(v_low > 0, flux_low, 0.0)
            zcorr[j] = jnp.where(
                place4 == 0,
                -ahead(by_left),
                jnp.where(
                    place4 == 1,
                    by_left - ahead(flux_high) + ahead(left * own),
                    jnp.where(place4 == 2, entering + by_left - by_right, back(by_right)),
                ),
            )

    last_early = level == EARLY - 1
    copies_c = [
        remote(part.at[2], slots_b.at[0], ts_sem.at[2], tr_sem.at[1], along_yz(0, dz))
        for dz in range(1, 6)
    ]

    @pl.when(last_early)
    def _():
        wait_bytes(slots_b.at[pl.ds(0, 4 * EARLY - 1)], tr_sem.at[1])
        part[2] = jnp.sum(slots_b[: 4 * EARLY], axis=0)
        pl.semaphore_wait(reply_sem.at[1], levels - EARLY)
        for copy in copies_c:
            copy.start()

    @pl.when(jnp.logical_not(final[0]))
    def _():
        face_copy.wait_recv()

    for i in range(9):
        if i == 0:
            v = disp[0, 0].astype(jnp.float32) * (STEP * low_scale[0])
        elif i < 8:
            v = disp[0, i].astype(jnp.float32) * STEP
        else:
            v_last = disp[0, 7].astype(jnp.float32) * (STEP * flag_open[1])
            v = jnp.where(final[0], v_last, xface[...].astype(jnp.float32) * STEP)
        vx[i] = v
        gx_w[i] = half_weight(v)

    inner = jnp.logical_not(jnp.logical_or(first[0], final[0]))
    edge_lanes = jnp.logical_or(lane8 < 2, lane8 > 125)
    for f in range(5):

        @pl.when(inner)
        def _():
            wait_bytes(xhalo.at[f], xr_sem.at[f])

        @pl.when(jnp.logical_not(inner))
        def _():
            wait_bytes(xhalo.at[f, 0], xr_sem.at[f])

        def tile(t, carry):
            part_rows = pl.ds(pl.multiple_of(t * 8, 8), 8)
            own = [q[f, i, part_rows] for i in range(8)]
            cell = (
                [jnp.where(first[0], own[0], xhalo[f, 0, r, part_rows]) for r in range(2)]
                + own
                + [jnp.where(final[0], own[7], xhalo[f, 1, r, part_rows]) for r in range(2)]
            )
            diff = [cell[i + 1] - cell[i] for i in range(11)]
            slope = [minmod(diff[i], diff[i + 1]) for i in range(10)]
            flux = []
            for i in range(9):
                v = vx[i, part_rows]
                g = gx_w[i, part_rows]
                flux.append(
                    v * jnp.where(v > 0, cell[i + 1], cell[i + 2])
                    + g * jnp.where(v > 0, slope[i], slope[i + 1])
                )
            for i in range(8):
                move = lax.rem(254 - 4 * ((i % 4) * 8 + t), 128)
                corr = pltpu.roll(zcorr[2 * f + i // 4], move, 1)
                corr = jnp.where(edge_lanes, corr, 0.0)
                acc[f, i, part_rows] += (flux[i] - flux[i + 1]) + corr
            return carry

        lax.fori_loop(0, 8, tile, 0)

    wait_bytes(slots_a, ts_sem.at[0])

    @pl.when(jnp.logical_not(first[0]))
    def _():
        face_copy.wait_send()

    for copy, there in (
        (y_up, final[1]),
        (y_down, first[1]),
        (z_up, final[2]),
        (z_down, first[2]),
    ):

        @pl.when(jnp.logical_not(there))
        def _():
            copy.wait_send()

    @pl.when(jnp.logical_not(final[0]))
    def _():
        wait_bytes(xhalo.at[:, 0], xs_sem.at[0])

    @pl.when(jnp.logical_not(first[0]))
    def _():
        wait_bytes(xhalo.at[:, 1], xs_sem.at[1])

    @pl.when(early)
    def _():
        wait_bytes(slots_b.at[pl.ds(0, 4 * EARLY - 1)], ts_sem.at[1])
        wait_bytes(slots_b.at[pl.ds(0, 4 * (8 - EARLY))], tr_sem.at[2])

    @pl.when(level < EARLY - 1)
    def _():
        wait_bytes(slots_b.at[pl.ds(0, 4 * EARLY - 1)], tr_sem.at[1])

    @pl.when(last_early)
    def _():
        wait_bytes(slots_b.at[pl.ds(0, 5)], ts_sem.at[2])

    @pl.when(late)
    def _():
        wait_bytes(slots_b.at[pl.ds(0, 31)], ts_sem.at[1])
        wait_bytes(slots_b.at[pl.ds(0, 1)], tr_sem.at[1])
        wait_bytes(slots_b.at[pl.ds(0, 4 * (8 - EARLY) - 1)], tr_sem.at[2])

    others = jnp.sum(slots_b[1 : 4 * EARLY], axis=0)
    grand[...] = (
        slots_b[0]
        + jnp.where(early, others, 0.0)
        + jnp.sum(slots_b[4 * EARLY :], axis=0)
    )


def write_out(cells, acc, grand, new_density, new_momentum, new_energy, totals, pair, sem):
    stores = [
        pltpu.make_async_copy(acc.at[0], new_density, sem.at[0]),
        pltpu.make_async_copy(acc.at[1], new_energy, sem.at[0]),
    ] + [pltpu.make_async_copy(acc.at[2 + c], new_momentum.at[c], sem.at[0]) for c in range(3)]
    for store in stores:
        store.start()
    lane1 = lax.broadcasted_iota(jnp.int32, (1, 128), 1)
    both = grand[...]
    pair[0] = jnp.sum(jnp.where(lane1 < 64, both, 0.0)) / cells
    pair[1] = jnp.sum(jnp.where(lane1 < 64, 0.0, both)) / cells
    last = pltpu.make_async_copy(pair, totals, sem.at[1])
    last.start()
    pltpu.make_async_copy(acc, acc, sem.at[0]).wait()
    last.wait()


def shards(cells, density, momentum, energy, displacement, flags):
    f32, i32 = jnp.float32, jnp.int32
    anywhere = pl.BlockSpec(memory_space=pltpu.HBM)
    local = pl.BlockSpec(memory_space=pltpu.VMEM)
    inputs = [
        pltpu.with_memory_space_constraint(a, pltpu.HBM)
        for a in (density, momentum, energy, displacement, flags)
    ]
    acc, grand = pl.pallas_call(
        kernel,
        out_shape=(
            jax.ShapeDtypeStruct((5, 8, 64, 128), f32),
            jax.ShapeDtypeStruct((1, 128), f32),
        ),
        in_specs=[anywhere] * 5,
        out_specs=(local, local),
        scratch_shapes=[
            pltpu.VMEM((5, 8, 64, 128), f32),
            pltpu.VMEM((3, 8, 64, 128), i32),
            pltpu.SMEM((6,), i32),
            pltpu.VMEM((9, 64, 128), f32),
            pltpu.VMEM((9, 64, 128), f32),
            pltpu.VMEM((5, 2, 2, 64, 128), f32),
            pltpu.VMEM((64, 128), i32),
            pltpu.VMEM((10, 8, 128), f32),
            pltpu.VMEM((11, 8, 128), f32),
            pltpu.VMEM((10, 8, 128), f32),
            pltpu.VMEM((11, 8, 128), f32),
            pltpu.VMEM((12, 8, 128), f32),
            pltpu.VMEM((12, 8, 128), f32),
            pltpu.VMEM((12, 8, 128), f32),
            pltpu.VMEM((10, 8, 128), f32),
            pltpu.VMEM((3, 1, 128), f32),
            pltpu.VMEM((7, 1, 128), f32),
            pltpu.VMEM((32, 1, 128), f32),
            pltpu.SemaphoreType.DMA((4,)),
            pltpu.SemaphoreType.DMA((3,)),
            pltpu.SemaphoreType.DMA((6,)),
            pltpu.SemaphoreType.DMA((2,)),
            pltpu.SemaphoreType.DMA((2,)),
            pltpu.SemaphoreType.DMA((2,)),
            pltpu.SemaphoreType.DMA((2,)),
            pltpu.SemaphoreType.DMA((3,)),
            pltpu.SemaphoreType.DMA((3,)),
            pltpu.SemaphoreType.REGULAR((2,)),
            pltpu.SemaphoreType.REGULAR((3,)),
        ],
        compiler_params=pltpu.CompilerParams(
            collective_id=0, has_side_effects=True, vmem_limit_bytes=16 * 2**20
        ),
        name="remap",
    )(*inputs)
    return pl.pallas_call(
        functools.partial(write_out, cells),
        out_shape=(
            jax.ShapeDtypeStruct(density.shape, f32),
            jax.ShapeDtypeStruct(momentum.shape, f32),
            jax.ShapeDtypeStruct(energy.shape, f32),
            jax.ShapeDtypeStruct((2,), f32),
        ),
        in_specs=[local, local],
        out_specs=[anywhere] * 4,
        scratch_shapes=[pltpu.SMEM((2,), f32), pltpu.SemaphoreType.DMA((2,))],
        compiler_params=pltpu.CompilerParams(vmem_limit_bytes=4 * 2**20),
        name="write_out",
    )(acc, grand)


def solution(mesh):
    cells = float(mesh.shape["gx"] * mesh.shape["gy"] * mesh.shape["gz"] * 8 * 64 * 128)
    block = P("gx", "gy", "gz")
    three = P(None, "gx", "gy", "gz")
    return jax.shard_map(
        functools.partial(shards, cells),
        mesh=mesh,
        in_specs=(block, three, block, three, P()),
        out_specs=(block, three, block, P()),
        check_vma=False,
    )
```

```python
import functools

import jax
import jax.numpy as jnp
from jax import lax
from jax.experimental import pallas as pl
from jax.experimental.pallas import tpu as pltpu
from jax.sharding import PartitionSpec as P

MESH = pl.DeviceIdType.MESH
STEP = 1.0 / 256.0
EARLY = 3


def minmod(left_diff, right_diff):
    least = jnp.minimum(left_diff, right_diff)
    most = jnp.maximum(left_diff, right_diff)
    return jnp.maximum(least, jnp.minimum(most, 0.0))


def half_weight(v):
    size = jnp.abs(v)
    return 0.5 * size * (1.0 - size)


def back(block):
    return pltpu.roll(block, 1, 1)


def ahead(block):
    return pltpu.roll(block, 127, 1)


def kernel(
    density,
    momentum,
    energy,
    displacement,
    flags,
    acc,
    grand,
    q,
    disp,
    flag,
    vx,
    gx_w,
    xhalo,
    xface,
    yup,
    ydown,
    ylow,
    yhigh,
    zpack,
    zlow,
    zhigh,
    zcorr,
    part,
    slots_a,
    slots_b,
    slots_d,
    load_sem,
    xs_sem,
    xr_sem,
    ys_sem,
    yr_sem,
    zs_sem,
    zr_sem,
    ts_sem,
    tr_sem,
    round_sem,
    reply_sem,
):
    px, py, pz = lax.axis_index("gx"), lax.axis_index("gy"), lax.axis_index("gz")
    nx, ny, nz = lax.axis_size("gx"), lax.axis_size("gy"), lax.axis_size("gz")
    core = pz % 2
    zl = (pz // 2) % 2
    def wait_bytes(of, sem):
        pltpu.make_async_copy(of, of, sem).wait()

    def place(x=None, y=None, z=None):
        target = {}
        if x is not None:
            target["gx"] = x
        if y is not None:
            target["gy"] = y
        if z is not None:
            target["gz"] = z
        return target

    level = py * 2 + zl
    levels = 2 * ny
    early = level < EARLY

    def along_yz(dy, dz):
        chip = lax.rem(level + dz, levels)
        return place(y=chip // 2, z=lax.rem(pz + 4 * dy, nz) + 2 * (chip % 2 - zl))

    def greet(sem, peer):
        pl.semaphore_signal(sem, inc=1, device_id=peer, device_id_type=MESH)

    stage_a = [
        place(x=lax.rem(px + dx, nx), z=pz + dc * (1 - 2 * core))
        for dx in (2, 1, 3, 0)
        for dc in range(2)
        if dx or dc
    ]
    along_y = [along_yz(dy, 0) for dy in (1, 2, 3)]
    steps = [-2, -1, 1, 2]
    late_step = [
        jnp.logical_and(level + step >= EARLY, level + step < levels) for step in steps
    ]
    late_steps = sum(ok.astype(jnp.int32) for ok in late_step)
    has_across = jnp.where(core == 1, pz < nz - 1, pz > 0)
    across = place(z=lax.rem(pz + nz + 2 * core - 1, nz))

    def greet_late(sem):
        for step, ok in zip(steps, late_step):

            @pl.when(ok)
            def _():
                greet(sem, along_yz(0, step % 8))

    barrier = pltpu.get_barrier_semaphore()
    for peer in stage_a + along_y:
        greet(barrier, peer)

    flag_copy = pltpu.make_async_copy(flags, flag, load_sem.at[0])
    flag_copy.start()
    pltpu.make_async_copy(density, q.at[0], load_sem.at[1]).start()
    pltpu.make_async_copy(energy, q.at[1], load_sem.at[1]).start()
    disp_load = pltpu.make_async_copy(displacement, disp, load_sem.at[2])
    disp_load.start()
    momentum_load = pltpu.make_async_copy(momentum, q.at[pl.ds(2, 3)], load_sem.at[3])
    momentum_load.start()

    @pl.when(has_across)
    def _():
        greet(barrier, across)

    in_column = jnp.logical_and(px == 0, core == 1)
    root = jnp.logical_and(in_column, jnp.logical_and(level == 0, pz < 2))

    @pl.when(root)
    def _():
        def greet_group(k, carry):
            t = lax.rem(k // 4 + EARLY, 8)
            y = lax.rem(k, 4)
            z = 4 * y + 2 * lax.rem(t, 2)
            for x in range(4):
                for c in range(2):
                    peer = place(x=x, y=t // 2, z=z + c)
                    if x or not c:
                        greet(barrier, peer)
                    else:
                        pl.when(t + y > 0)(functools.partial(greet, barrier, peer))
            return carry

        lax.fori_loop(0, 32, greet_group, 0)

    @pl.when(early)
    def _():
        for dz in range(1, 8):

            @pl.when(level + dz < levels)
            def _():
                for dy in range(4):
                    greet(barrier, along_yz(dy, dz))

    @pl.when(jnp.logical_not(early))
    def _():
        greet_late(barrier)

    flag_copy.wait()
    wait_bytes(q.at[pl.ds(0, 2)], load_sem.at[1])
    disp_load.wait()

    flag_open = [flag[i].astype(jnp.float32) for i in range(6)]
    first = [px == 0, py == 0, pz == 0]
    final = [px == nx - 1, py == ny - 1, pz == nz - 1]
    low_scale = [jnp.where(first[a], flag_open[2 * a], 1.0) for a in range(3)]
    gain = [jnp.where(first[a], flag_open[2 * a] * STEP, 0.0) for a in range(3)]
    loss = [jnp.where(final[a], flag_open[2 * a + 1] * -STEP, 0.0) for a in range(3)]

    rows = lax.broadcasted_iota(jnp.int32, (64, 128), 0)
    lanes = lax.broadcasted_iota(jnp.int32, (64, 128), 1)
    weight_y = jnp.where(rows == 0, gain[1], jnp.where(rows == 63, loss[1], 0.0))
    weight_z = jnp.where(lanes == 0, gain[2], jnp.where(lanes == 127, loss[2], 0.0))

    def fold(block):
        return jnp.sum(block.reshape(8, 8, 128), axis=0)

    def plane_sum(x, sums):
        weight = (
            1.0
            + weight_y * disp[1, x].astype(jnp.float32)
            + weight_z * disp[2, x].astype(jnp.float32)
        )
        return (sums[0] + fold(q[0, x] * weight), sums[1] + fold(q[1, x] * weight))

    weight_low = gain[0] * disp[0, 0].astype(jnp.float32)
    weight_high = loss[0] * disp[0, 7].astype(jnp.float32)
    sums = tuple(fold(q[f, 0] * weight_low + q[f, 7] * weight_high) for f in (0, 1))
    sums = lax.fori_loop(0, 8, plane_sum, sums)
    lane1 = lax.broadcasted_iota(jnp.int32, (1, 128), 1)

    def halves(low, high):
        low = jnp.sum(low, axis=0, keepdims=True)
        high = jnp.sum(high, axis=0, keepdims=True)
        return jnp.where(lane1 < 64, low + pltpu.roll(low, 64, 1), high + pltpu.roll(high, 64, 1))

    part[0] = halves(*sums)
    momentum_load.wait()

    greeted = (
        len(stage_a)
        + len(along_y)
        + has_across.astype(jnp.int32)
        + 1
        - root.astype(jnp.int32)
        + jnp.where(early, 4 * level, 4 * EARLY + late_steps)
    )
    pl.semaphore_wait(barrier, greeted)

    def remote(src, dst, send_sem, recv_sem, peer):
        return pltpu.make_async_remote_copy(
            src_ref=src,
            dst_ref=dst,
            send_sem=send_sem,
            recv_sem=recv_sem,
            device_id=peer,
            device_id_type=MESH,
        )

    copies_a = [
        remote(part.at[0], slots_a.at[i], ts_sem.at[0], tr_sem.at[0], peer)
        for i, peer in enumerate(stage_a)
    ]
    slot = level * 4 + pz // 4
    arrival = tr_sem.at[jnp.where(early, 1, 2)]
    me_y = pz // 4
    base_z = pz - 4 * me_y - 2 * zl
    places = [(t, y) for t in range(8) for y in (0, 1, 3, 2)]
    copies_b = [
        remote(
            part.at[1],
            slots_b.at[slot],
            ts_sem.at[1],
            arrival,
            place(y=t // 2, z=base_z + 4 * y + 2 * (t % 2)),
        )
        for t, y in places
    ]

    def send_b(wanted):
        for (t, y), copy in zip(places, copies_b):
            ok = wanted(t)
            if ok is not None:
                other = jnp.logical_or(level != t, me_y != y)
                if not (t or y):
                    other = jnp.logical_and(other, jnp.logical_not(in_column))
                pl.when(jnp.logical_and(ok, other))(copy.start)
    index = (px * ny + py) * nz + pz
    to_root = remote(
        part.at[0], slots_d.at[index], ts_sem.at[3], tr_sem.at[3], place(x=0, y=0, z=1)
    )

    @pl.when(jnp.logical_not(root))
    def _():
        to_root.start()

    for copy in copies_a:
        copy.start()

    @pl.when(jnp.logical_not(early))
    def _():
        greet_late(round_sem.at[0])
        for peer in along_y:
            greet(round_sem.at[0], peer)

    for back_step in (1, 2):

        @pl.when(jnp.logical_and(level - back_step >= 0, level - back_step < EARLY))
        def _():
            greet(reply_sem.at[0], along_yz(0, 8 - back_step))

    @pl.when(early)
    def _():
        for target in range(EARLY - 1):

            @pl.when(target < level)
            def _():
                for dy in range(4):
                    greet(reply_sem.at[2], along_yz(dy, lax.rem(levels + target - level, levels)))

    @pl.when(jnp.logical_not(early))
    def _():
        greet(reply_sem.at[1], along_yz(0, lax.rem(levels + EARLY - 1 - level, levels)))

    x_next = place(x=lax.rem(px + 1, nx))
    x_prev = place(x=lax.rem(px + nx - 1, nx))
    face_copy = remote(disp.at[0, 0], xface, xs_sem.at[2], xr_sem.at[5], x_prev)
    up_copies = [
        remote(q.at[f, pl.ds(6, 2)], xhalo.at[f, 0], xs_sem.at[0], xr_sem.at[f], x_next) for f in range(5)
    ]
    down_copies = [
        remote(q.at[f, pl.ds(0, 2)], xhalo.at[f, 1], xs_sem.at[1], xr_sem.at[f], x_prev)
        for f in range(5)
    ]

    @pl.when(jnp.logical_not(first[0]))
    def _():
        face_copy.start()

    for f in range(5):

        @pl.when(jnp.logical_not(final[0]))
        def _():
            up_copies[f].start()

        @pl.when(jnp.logical_not(first[0]))
        def _():
            down_copies[f].start()

    for f in range(5):
        for r in range(2):
            yup[2 * f + r] = q[f, :, 62 + r, :]
            ydown[2 * f + r] = q[f, :, r, :]
    ydown[10] = disp[1, :, 0, :].astype(jnp.float32) * STEP

    y_up = remote(yup, ylow, ys_sem.at[0], yr_sem.at[0], place(y=lax.rem(py + 1, ny)))
    y_down = remote(ydown, yhigh, ys_sem.at[1], yr_sem.at[1], place(y=lax.rem(py + ny - 1, ny)))

    @pl.when(jnp.logical_not(first[1]))
    def _():
        y_down.start()

    @pl.when(jnp.logical_not(jnp.logical_or(final[1], early)))
    def _():
        y_up.start()

    lane8 = lax.broadcasted_iota(jnp.int32, (8, 128), 1)
    slot_of = lane8 // 4
    place4 = lane8 % 4

    def pack(source, base, half):
        packed = jnp.zeros((8, 128), jnp.float32)
        for xx in range(4):
            plane = source[base, half * 4 + xx].astype(jnp.float32)
            for t in range(8):
                k = xx * 8 + t
                moved = pltpu.roll(plane[8 * t : 8 * t + 8], (4 * k + 2) % 128, 1)
                packed = jnp.where(slot_of == k, moved, packed)
        return packed

    for f in range(5):
        for half in range(2):
            zpack[2 * f + half] = pack(q, f, half)
    for half in range(2):
        zpack[10 + half] = pack(disp, 2, half) * STEP

    z_up = remote(zpack, zlow, zs_sem.at[0], zr_sem.at[0], place(z=lax.rem(pz + 1, nz)))
    z_down = remote(zpack, zhigh, zs_sem.at[1], zr_sem.at[1], place(z=lax.rem(pz + nz - 1, nz)))

    @pl.when(jnp.logical_not(final[2]))
    def _():
        z_up.start()

    @pl.when(jnp.logical_not(first[2]))
    def _():
        z_down.start()

    scale_y = jnp.where(
        jnp.logical_or(rows < 2, rows == 63), 0.0, STEP
    )
    scale_z = jnp.where(lanes == 0, STEP * low_scale[2], STEP)

    def planes(x, carry):
        vy = disp[1, x].astype(jnp.float32) * scale_y
        gy = half_weight(vy)
        up_y = vy > 0
        vz = disp[2, x].astype(jnp.float32) * scale_z
        right = jnp.where(lanes == 127, 0.0, jnp.maximum(ahead(vz), 0.0))
        right_w = jnp.where(lanes == 0, 0.0, 0.5 * right * (1.0 - right))
        left = jnp.minimum(vz, 0.0)
        left_w = jnp.where(
            jnp.logical_or(lanes == 0, lanes == 127), 0.0, -0.5 * left * (1.0 + left)
        )
        for f in range(5):
            value = q[f, x]
            below = back(value)
            above = ahead(value)
            slope = minmod(value - below, above - value)
            out_right = right * value + right_w * slope
            out_left = left * value + left_w * slope
            change_z = (back(out_right) - out_right) + (out_left - ahead(out_left))

            below = pltpu.roll(value, 1, 0)
            diff = value - below
            slope = minmod(diff, pltpu.roll(diff, 63, 0))
            flux = vy * jnp.where(up_y, below, value) + gy * jnp.where(
                up_y, pltpu.roll(slope, 1, 0), slope
            )
            acc[f, x] = (value + (flux - pltpu.roll(flux, 63, 0))) + change_z
        return carry

    lax.fori_loop(0, 3, planes, 0)

    late = jnp.logical_not(early)

    @pl.when(late)
    def _():
        pl.semaphore_wait(round_sem.at[0], len(along_y) + late_steps)
        greet_late(round_sem.at[1])
        for peer in along_y:
            greet(round_sem.at[1], peer)

    wait_bytes(slots_a, tr_sem.at[0])
    group = part[0] + jnp.sum(slots_a[...], axis=0)
    part[1] = group
    slots_b[slot] = group

    @pl.when(late)
    def _():
        for (t, y), copy in zip(places, copies_b):
            if not (t or y):
                pl.when(jnp.logical_not(in_column))(copy.start)
            elif t < EARLY:
                copy.start()
        send_b(lambda t: jnp.abs(level - t) < 3 if t >= EARLY else None)

    @pl.when(early)
    def _():
        send_b(lambda t: level >= t if t < EARLY else None)

        @pl.when(level < EARLY - 1)
        def _():
            pl.semaphore_wait(reply_sem.at[2], 4 * (EARLY - 1 - level))
            send_b(lambda t: level < t if t < EARLY else None)

        pl.semaphore_wait(reply_sem.at[0], 2)
        y_up.start()

    lax.fori_loop(3, 6, planes, 0)

    @pl.when(late)
    def _():
        pl.semaphore_wait(round_sem.at[1], len(along_y) + late_steps)
        send_b(lambda t: jnp.abs(level - t) > 2 if t >= EARLY else None)

    lax.fori_loop(6, 8, planes, 0)

    @pl.when(jnp.logical_not(first[1]))
    def _():
        y_up.wait_recv()

    @pl.when(jnp.logical_not(final[1]))
    def _():
        y_down.wait_recv()

    v0, v1, v63 = [disp[1, :, r, :].astype(jnp.float32) * STEP for r in (0, 1, 63)]
    v64 = jnp.where(final[1], v63 * flag_open[3], yhigh[10])
    v0 = v0 * low_scale[1]

    def flux_row(v, behind, at, slope_behind, slope_at):
        return v * jnp.where(v > 0, behind, at) + half_weight(v) * jnp.where(
            v > 0, slope_behind, slope_at
        )

    for f in range(5):
        q0, q1, q2, q61, q62, q63 = [q[f, :, r, :] for r in (0, 1, 2, 61, 62, 63)]
        lo1 = jnp.where(first[1], q0, ylow[2 * f + 1])
        lo2 = jnp.where(first[1], q0, ylow[2 * f])
        hi0 = jnp.where(final[1], q63, yhigh[2 * f])
        hi1 = jnp.where(final[1], q63, yhigh[2 * f + 1])
        s0 = minmod(q0 - lo1, q1 - q0)
        s63 = minmod(q63 - q62, hi0 - q63)
        flux_0 = flux_row(v0, lo1, q0, minmod(lo1 - lo2, q0 - lo1), s0)
        flux_1 = flux_row(v1, q0, q1, s0, minmod(q1 - q0, q2 - q1))
        flux_63 = flux_row(v63, q62, q63, minmod(q62 - q61, q63 - q62), s63)
        flux_64 = flux_row(v64, q63, hi0, s63, minmod(hi0 - q63, hi1 - hi0))
        acc[f, :, 0, :] += flux_0 - flux_1
        acc[f, :, 1, :] += flux_1
        acc[f, :, 62, :] -= flux_63
        acc[f, :, 63, :] += flux_63 - flux_64

    @pl.when(jnp.logical_not(first[2]))
    def _():
        z_up.wait_recv()

    @pl.when(jnp.logical_not(final[2]))
    def _():
        z_down.wait_recv()

    def face(four, v):
        behind = back(four)
        diff = four - behind
        slope = minmod(diff, ahead(diff))
        flux = v * jnp.where(v > 0, behind, four) + half_weight(v) * jnp.where(
            v > 0, back(slope), slope
        )
        return slope, flux

    for half in range(2):
        own_v = zpack[10 + half]
        v_low = jnp.where(place4 == 2, own_v * low_scale[2], own_v)
        v_high = jnp.where(final[2], back(own_v) * flag_open[5], zhigh[10 + half])
        left = jnp.minimum(v_low, 0.0)
        left_w = -0.5 * left * (1.0 + left)
        right = jnp.maximum(ahead(own_v), 0.0)
        right_w = 0.5 * right * (1.0 - right)
        for f in range(5):
            j = 2 * f + half
            own = zpack[j]
            ghost_low = jnp.where(place4 == 0, pltpu.roll(own, 126, 1), ahead(own))
            ghost_high = jnp.where(place4 == 2, back(own), pltpu.roll(own, 2, 1))
            low = jnp.where(place4 < 2, jnp.where(first[2], ghost_low, zlow[j]), own)
            high = jnp.where(place4 < 2, own, jnp.where(final[2], ghost_high, zhigh[j]))
            slope_low, flux_low = face(low, v_low)
            slope_high, flux_high = face(high, v_high)
            by_left = left_w * jnp.where(place4 == 1, slope_high, slope_low)
            by_right = right_w * slope_low
            entering = jnp.where(v_low > 0, flux_low, 0.0)
            zcorr[j] = jnp.where(
                place4 == 0,
                -ahead(by_left),
                jnp.where(
                    place4 == 1,
                    by_left - ahead(flux_high) + ahead(left * own),
                    jnp.where(place4 == 2, entering + by_left - by_right, back(by_right)),
                ),
            )

    last_early = level == EARLY - 1
    copies_c = [
        remote(part.at[2], slots_b.at[0], ts_sem.at[2], tr_sem.at[1], along_yz(0, dz))
        for dz in range(1, 6)
    ]

    @pl.when(last_early)
    def _():
        wait_bytes(slots_b.at[pl.ds(0, 4 * EARLY - 1)], tr_sem.at[1])
        part[2] = jnp.sum(slots_b[: 4 * EARLY], axis=0)
        pl.semaphore_wait(reply_sem.at[1], levels - EARLY)
        for copy in copies_c:
            copy.start()

    @pl.when(jnp.logical_not(final[0]))
    def _():
        face_copy.wait_recv()

    for i in range(9):
        if i == 0:
            v = disp[0, 0].astype(jnp.float32) * (STEP * low_scale[0])
        elif i < 8:
            v = disp[0, i].astype(jnp.float32) * STEP
        else:
            v_last = disp[0, 7].astype(jnp.float32) * (STEP * flag_open[1])
            v = jnp.where(final[0], v_last, xface[...].astype(jnp.float32) * STEP)
        vx[i] = v
        gx_w[i] = half_weight(v)

    inner = jnp.logical_not(jnp.logical_or(first[0], final[0]))
    edge_lanes = jnp.logical_or(lane8 < 2, lane8 > 125)
    for f in range(5):

        @pl.when(inner)
        def _():
            wait_bytes(xhalo.at[f], xr_sem.at[f])

        @pl.when(jnp.logical_not(inner))
        def _():
            wait_bytes(xhalo.at[f, 0], xr_sem.at[f])

        def tile(t, carry):
            part_rows = pl.ds(pl.multiple_of(t * 8, 8), 8)
            own = [q[f, i, part_rows] for i in range(8)]
            cell = (
                [jnp.where(first[0], own[0], xhalo[f, 0, r, part_rows]) for r in range(2)]
                + own
                + [jnp.where(final[0], own[7], xhalo[f, 1, r, part_rows]) for r in range(2)]
            )
            diff = [cell[i + 1] - cell[i] for i in range(11)]
            slope = [minmod(diff[i], diff[i + 1]) for i in range(10)]
            flux = []
            for i in range(9):
                v = vx[i, part_rows]
                g = gx_w[i, part_rows]
                flux.append(
                    v * jnp.where(v > 0, cell[i + 1], cell[i + 2])
                    + g * jnp.where(v > 0, slope[i], slope[i + 1])
                )
            for i in range(8):
                move = lax.rem(254 - 4 * ((i % 4) * 8 + t), 128)
                corr = pltpu.roll(zcorr[2 * f + i // 4], move, 1)
                corr = jnp.where(edge_lanes, corr, 0.0)
                acc[f, i, part_rows] += (flux[i] - flux[i + 1]) + corr
            return carry

        lax.fori_loop(0, 8, tile, 0)

    wait_bytes(slots_a, ts_sem.at[0])

    @pl.when(jnp.logical_not(first[0]))
    def _():
        face_copy.wait_send()

    for copy, there in (
        (y_up, final[1]),
        (y_down, first[1]),
        (z_up, final[2]),
        (z_down, first[2]),
    ):

        @pl.when(jnp.logical_not(there))
        def _():
            copy.wait_send()

    @pl.when(jnp.logical_not(final[0]))
    def _():
        wait_bytes(xhalo.at[:, 0], xs_sem.at[0])

    @pl.when(jnp.logical_not(first[0]))
    def _():
        wait_bytes(xhalo.at[:, 1], xs_sem.at[1])

    not_root = jnp.logical_not(root)
    skips = jnp.logical_and(in_column, not_root)

    def wait_rows(when, count, sem):
        @pl.when(when)
        def _():
            wait_bytes(slots_b.at[pl.ds(0, count)], sem)

    both = jnp.logical_and
    sent = jnp.logical_not(skips)
    wait_rows(both(early, sent), 4 * EARLY - 1, ts_sem.at[1])
    wait_rows(both(early, skips), 4 * EARLY - 2, ts_sem.at[1])
    wait_rows(both(late, sent), 31, ts_sem.at[1])
    wait_rows(both(late, skips), 30, ts_sem.at[1])
    wait_rows(last_early, 5, ts_sem.at[2])

    @pl.when(not_root)
    def _():
        to_root.wait_send()

    wait_rows(both(level < EARLY - 1, not_root), 4 * EARLY - 1, tr_sem.at[1])
    wait_rows(both(early, not_root), 4 * (8 - EARLY), tr_sem.at[2])
    wait_rows(late, 1, tr_sem.at[1])
    wait_rows(late, 4 * (8 - EARLY) - 1, tr_sem.at[2])

    @pl.when(root)
    def _():
        slots_d[index] = part[0]
        wait_bytes(slots_d.at[pl.ds(0, 255)], tr_sem.at[3])
        grand[...] = jnp.sum(slots_d[...], axis=0)

    @pl.when(not_root)
    def _():
        others = jnp.sum(slots_b[1 : 4 * EARLY], axis=0)
        grand[...] = (
            slots_b[0]
            + jnp.where(early, others, 0.0)
            + jnp.sum(slots_b[4 * EARLY :], axis=0)
        )


def write_out(cells, acc, grand, new_density, new_momentum, new_energy, totals, pair, sem):
    stores = [
        pltpu.make_async_copy(acc.at[0], new_density, sem.at[0]),
        pltpu.make_async_copy(acc.at[1], new_energy, sem.at[0]),
    ] + [pltpu.make_async_copy(acc.at[2 + c], new_momentum.at[c], sem.at[0]) for c in range(3)]
    for store in stores:
        store.start()
    lane1 = lax.broadcasted_iota(jnp.int32, (1, 128), 1)
    both = grand[...]
    pair[0] = jnp.sum(jnp.where(lane1 < 64, both, 0.0)) / cells
    pair[1] = jnp.sum(jnp.where(lane1 < 64, 0.0, both)) / cells
    last = pltpu.make_async_copy(pair, totals, sem.at[1])
    last.start()
    pltpu.make_async_copy(acc, acc, sem.at[0]).wait()
    last.wait()


def shards(cells, density, momentum, energy, displacement, flags):
    f32, i32 = jnp.float32, jnp.int32
    anywhere = pl.BlockSpec(memory_space=pltpu.HBM)
    local = pl.BlockSpec(memory_space=pltpu.VMEM)
    inputs = [
        pltpu.with_memory_space_constraint(a, pltpu.HBM)
        for a in (density, momentum, energy, displacement, flags)
    ]
    acc, grand = pl.pallas_call(
        kernel,
        out_shape=(
            jax.ShapeDtypeStruct((5, 8, 64, 128), f32),
            jax.ShapeDtypeStruct((1, 128), f32),
        ),
        in_specs=[anywhere] * 5,
        out_specs=(local, local),
        scratch_shapes=[
            pltpu.VMEM((5, 8, 64, 128), f32),
            pltpu.VMEM((3, 8, 64, 128), i32),
            pltpu.SMEM((6,), i32),
            pltpu.VMEM((9, 64, 128), f32),
            pltpu.VMEM((9, 64, 128), f32),
            pltpu.VMEM((5, 2, 2, 64, 128), f32),
            pltpu.VMEM((64, 128), i32),
            pltpu.VMEM((10, 8, 128), f32),
            pltpu.VMEM((11, 8, 128), f32),
            pltpu.VMEM((10, 8, 128), f32),
            pltpu.VMEM((11, 8, 128), f32),
            pltpu.VMEM((12, 8, 128), f32),
            pltpu.VMEM((12, 8, 128), f32),
            pltpu.VMEM((12, 8, 128), f32),
            pltpu.VMEM((10, 8, 128), f32),
            pltpu.VMEM((3, 1, 128), f32),
            pltpu.VMEM((7, 1, 128), f32),
            pltpu.VMEM((32, 1, 128), f32),
            pltpu.VMEM((256, 1, 128), f32),
            pltpu.SemaphoreType.DMA((4,)),
            pltpu.SemaphoreType.DMA((3,)),
            pltpu.SemaphoreType.DMA((6,)),
            pltpu.SemaphoreType.DMA((2,)),
            pltpu.SemaphoreType.DMA((2,)),
            pltpu.SemaphoreType.DMA((2,)),
            pltpu.SemaphoreType.DMA((2,)),
            pltpu.SemaphoreType.DMA((4,)),
            pltpu.SemaphoreType.DMA((4,)),
            pltpu.SemaphoreType.REGULAR((2,)),
            pltpu.SemaphoreType.REGULAR((3,)),
        ],
        compiler_params=pltpu.CompilerParams(
            collective_id=0, has_side_effects=True, vmem_limit_bytes=16 * 2**20
        ),
        name="remap",
    )(*inputs)
    return pl.pallas_call(
        functools.partial(write_out, cells),
        out_shape=(
            jax.ShapeDtypeStruct(density.shape, f32),
            jax.ShapeDtypeStruct(momentum.shape, f32),
            jax.ShapeDtypeStruct(energy.shape, f32),
            jax.ShapeDtypeStruct((2,), f32),
        ),
        in_specs=[local, local],
        out_specs=[anywhere] * 4,
        scratch_shapes=[pltpu.SMEM((2,), f32), pltpu.SemaphoreType.DMA((2,))],
        compiler_params=pltpu.CompilerParams(vmem_limit_bytes=4 * 2**20),
        name="write_out",
    )(acc, grand)


def solution(mesh):
    cells = float(mesh.shape["gx"] * mesh.shape["gy"] * mesh.shape["gz"] * 8 * 64 * 128)
    block = P("gx", "gy", "gz")
    three = P(None, "gx", "gy", "gz")
    return jax.shard_map(
        functools.partial(shards, cells),
        mesh=mesh,
        in_specs=(block, three, block, three, P()),
        out_specs=(block, three, block, P()),
        check_vma=False,
    )
```

```python
import functools

import jax
import jax.numpy as jnp
from jax import lax
from jax.experimental import pallas as pl
from jax.experimental.pallas import tpu as pltpu
from jax.sharding import PartitionSpec as P

MESH = pl.DeviceIdType.MESH
STEP = 1.0 / 256.0
EARLY = 3
ROOTS = (
    (0, 0, 0, 1),
    (0, 1, 0, 0),
    (0, 0, 1, 0),
    (0, 2, 0, 0),
    (0, 3, 0, 0),
    (0, 0, 2, 0),
    (0, 0, 3, 0),
    (0, 0, 0, 0),
    (0, 1, 0, 1),
    (0, 2, 0, 1),
    (0, 1, 1, 0),
    (0, 0, 1, 1),
    (1, 0, 0, 0),
    (1, 0, 0, 1),
    (1, 1, 0, 0),
    (1, 0, 1, 0),
)


def minmod(left_diff, right_diff):
    least = jnp.minimum(left_diff, right_diff)
    most = jnp.maximum(left_diff, right_diff)
    return jnp.maximum(least, jnp.minimum(most, 0.0))


def half_weight(v):
    size = jnp.abs(v)
    return 0.5 * size * (1.0 - size)


def back(block):
    return pltpu.roll(block, 1, 1)


def ahead(block):
    return pltpu.roll(block, 127, 1)


def kernel(
    density,
    momentum,
    energy,
    displacement,
    flags,
    acc,
    grand,
    q,
    disp,
    flag,
    vx,
    gx_w,
    xhalo,
    xface,
    yup,
    ydown,
    ylow,
    yhigh,
    zpack,
    zlow,
    zhigh,
    zcorr,
    part,
    slots_a,
    slots_b,
    slots_d,
    load_sem,
    xs_sem,
    xr_sem,
    ys_sem,
    yr_sem,
    zs_sem,
    zr_sem,
    ts_sem,
    tr_sem,
    round_sem,
    reply_sem,
):
    px, py, pz = lax.axis_index("gx"), lax.axis_index("gy"), lax.axis_index("gz")
    nx, ny, nz = lax.axis_size("gx"), lax.axis_size("gy"), lax.axis_size("gz")
    core = pz % 2
    zl = (pz // 2) % 2
    def wait_bytes(of, sem):
        pltpu.make_async_copy(of, of, sem).wait()

    def place(x=None, y=None, z=None):
        target = {}
        if x is not None:
            target["gx"] = x
        if y is not None:
            target["gy"] = y
        if z is not None:
            target["gz"] = z
        return target

    level = py * 2 + zl
    levels = 2 * ny
    early = level < EARLY
    both = jnp.logical_and
    late = jnp.logical_not(early)

    def along_yz(dy, dz):
        chip = lax.rem(level + dz, levels)
        return place(y=chip // 2, z=lax.rem(pz + 4 * dy, nz) + 2 * (chip % 2 - zl))

    def greet(sem, peer):
        pl.semaphore_signal(sem, inc=1, device_id=peer, device_id_type=MESH)

    stage_a = [
        place(x=lax.rem(px + dx, nx), z=pz + dc * (1 - 2 * core))
        for dx in (2, 1, 3, 0)
        for dc in range(2)
        if dx or dc
    ]
    along_y = [along_yz(dy, 0) for dy in (2, 1, 3)]
    steps = [-2, 2, -1, 1]
    late_step = [
        jnp.logical_and(level + step >= EARLY, level + step < levels) for step in steps
    ]
    late_steps = sum(ok.astype(jnp.int32) for ok in late_step)
    has_across = jnp.where(core == 1, pz < nz - 1, pz > 0)
    across = place(z=lax.rem(pz + nz + 2 * core - 1, nz))

    def greet_late(sem):
        for step, ok in zip(steps, late_step):

            @pl.when(ok)
            def _():
                greet(sem, along_yz(0, step % 8))

    barrier = pltpu.get_barrier_semaphore()

    @pl.when(late)
    def _():
        greet_late(barrier)

    for peer in stage_a + along_y:
        greet(barrier, peer)

    flag_copy = pltpu.make_async_copy(flags, flag, load_sem.at[0])
    flag_copy.start()
    pltpu.make_async_copy(density, q.at[0], load_sem.at[1]).start()
    pltpu.make_async_copy(energy, q.at[1], load_sem.at[1]).start()
    disp_load = pltpu.make_async_copy(displacement, disp, load_sem.at[2])
    disp_load.start()
    momentum_load = pltpu.make_async_copy(momentum, q.at[pl.ds(2, 3)], load_sem.at[3])
    momentum_load.start()

    @pl.when(has_across)
    def _():
        greet(barrier, across)

    me_y = pz // 4
    in_column = [both(px == x, core == c) for _, x, _, c in ROOTS]
    skipped = sum(ok.astype(jnp.int32) for ok in in_column)
    at_root = [
        both(ok, both(level == t, me_y == y)) for ok, (t, _, y, _) in zip(in_column, ROOTS)
    ]
    root = functools.reduce(jnp.logical_or, at_root)

    @pl.when(root)
    def _():
        def greet_group(k, carry):
            t = 7 - k // 4
            z = 4 * lax.rem(k, 4) + 2 * lax.rem(t, 2)
            for x in range(4):
                for c in range(2):
                    greet(barrier, place(x=x, y=t // 2, z=z + c))
            return carry

        lax.fori_loop(0, 4 * (8 - EARLY), greet_group, 0)

    @pl.when(early)
    def _():
        for dz in range(1, 8):

            @pl.when(level + dz < levels)
            def _():
                for dy in range(4):
                    greet(barrier, along_yz(dy, dz))


    flag_copy.wait()
    wait_bytes(q.at[pl.ds(0, 2)], load_sem.at[1])
    disp_load.wait()

    flag_open = [flag[i].astype(jnp.float32) for i in range(6)]
    first = [px == 0, py == 0, pz == 0]
    final = [px == nx - 1, py == ny - 1, pz == nz - 1]
    low_scale = [jnp.where(first[a], flag_open[2 * a], 1.0) for a in range(3)]
    gain = [jnp.where(first[a], flag_open[2 * a] * STEP, 0.0) for a in range(3)]
    loss = [jnp.where(final[a], flag_open[2 * a + 1] * -STEP, 0.0) for a in range(3)]

    rows = lax.broadcasted_iota(jnp.int32, (64, 128), 0)
    lanes = lax.broadcasted_iota(jnp.int32, (64, 128), 1)
    weight_y = jnp.where(rows == 0, gain[1], jnp.where(rows == 63, loss[1], 0.0))
    weight_z = jnp.where(lanes == 0, gain[2], jnp.where(lanes == 127, loss[2], 0.0))

    def fold(block):
        return jnp.sum(block.reshape(8, 8, 128), axis=0)

    def plane_sum(x, sums):
        weight = (
            1.0
            + weight_y * disp[1, x].astype(jnp.float32)
            + weight_z * disp[2, x].astype(jnp.float32)
        )
        return (sums[0] + fold(q[0, x] * weight), sums[1] + fold(q[1, x] * weight))

    weight_low = gain[0] * disp[0, 0].astype(jnp.float32)
    weight_high = loss[0] * disp[0, 7].astype(jnp.float32)
    sums = tuple(fold(q[f, 0] * weight_low + q[f, 7] * weight_high) for f in (0, 1))
    sums = lax.fori_loop(0, 8, plane_sum, sums)
    lane1 = lax.broadcasted_iota(jnp.int32, (1, 128), 1)

    def halves(low, high):
        low = jnp.sum(low, axis=0, keepdims=True)
        high = jnp.sum(high, axis=0, keepdims=True)
        return jnp.where(lane1 < 64, low + pltpu.roll(low, 64, 1), high + pltpu.roll(high, 64, 1))

    part[0] = halves(*sums)
    momentum_load.wait()

    greeted = (
        len(stage_a)
        + len(along_y)
        + has_across.astype(jnp.int32)
        + jnp.where(early, 0, len(ROOTS))
        + jnp.where(early, 4 * level, 4 * EARLY + late_steps)
    )
    pl.semaphore_wait(barrier, greeted)

    def remote(src, dst, send_sem, recv_sem, peer):
        return pltpu.make_async_remote_copy(
            src_ref=src,
            dst_ref=dst,
            send_sem=send_sem,
            recv_sem=recv_sem,
            device_id=peer,
            device_id_type=MESH,
        )

    copies_a = [
        remote(part.at[0], slots_a.at[i], ts_sem.at[0], tr_sem.at[0], peer)
        for i, peer in enumerate(stage_a)
    ]
    slot = level * 4 + pz // 4
    arrival = tr_sem.at[jnp.where(early, 1, 2)]
    base_z = pz - 4 * me_y - 2 * zl
    places = [(t, y) for t in range(8) for y in (0, 1, 3, 2)]
    copies_b = [
        remote(
            part.at[1],
            slots_b.at[slot],
            ts_sem.at[1],
            arrival,
            place(y=t // 2, z=base_z + 4 * y + 2 * (t % 2)),
        )
        for t, y in places
    ]

    def send_b(wanted):
        for (t, y), copy in zip(places, copies_b):
            ok = wanted(t)
            if ok is not None:
                other = jnp.logical_or(level != t, me_y != y)
                pl.when(jnp.logical_and(ok, other))(copy.start)
    index = (level - EARLY) * 32 + me_y * 8 + px * 2 + core
    to_roots = [
        remote(
            part.at[0],
            slots_d.at[index],
            ts_sem.at[3],
            tr_sem.at[3],
            place(x=x, y=t // 2, z=4 * y + 2 * (t % 2) + c),
        )
        for t, x, y, c in ROOTS
    ]

    @pl.when(late)
    def _():
        to_roots[0].start()

    for copy in copies_a:
        copy.start()

    @pl.when(late)
    def _():
        for copy in to_roots[1:]:
            copy.start()
        greet_late(round_sem.at[0])
        for peer in along_y:
            greet(round_sem.at[0], peer)

    for back_step in (1, 2):

        @pl.when(jnp.logical_and(level - back_step >= 0, level - back_step < EARLY))
        def _():
            greet(reply_sem.at[0], along_yz(0, 8 - back_step))

    @pl.when(early)
    def _():
        for target in range(EARLY - 1):

            @pl.when(target < level)
            def _():
                for dy in range(4):
                    greet(reply_sem.at[2], along_yz(dy, lax.rem(levels + target - level, levels)))

    @pl.when(jnp.logical_not(early))
    def _():
        greet(reply_sem.at[1], along_yz(0, lax.rem(levels + EARLY - 1 - level, levels)))

    x_next = place(x=lax.rem(px + 1, nx))
    x_prev = place(x=lax.rem(px + nx - 1, nx))
    face_copy = remote(disp.at[0, 0], xface, xs_sem.at[2], xr_sem.at[5], x_prev)
    up_copies = [
        remote(q.at[f, pl.ds(6, 2)], xhalo.at[f, 0], xs_sem.at[0], xr_sem.at[f], x_next) for f in range(5)
    ]
    down_copies = [
        remote(q.at[f, pl.ds(0, 2)], xhalo.at[f, 1], xs_sem.at[1], xr_sem.at[f], x_prev)
        for f in range(5)
    ]

    @pl.when(jnp.logical_not(first[0]))
    def _():
        face_copy.start()

    for f in range(5):

        @pl.when(jnp.logical_not(final[0]))
        def _():
            up_copies[f].start()

        @pl.when(jnp.logical_not(first[0]))
        def _():
            down_copies[f].start()

    for f in range(5):
        for r in range(2):
            yup[2 * f + r] = q[f, :, 62 + r, :]
            ydown[2 * f + r] = q[f, :, r, :]
    ydown[10] = disp[1, :, 0, :].astype(jnp.float32) * STEP

    y_up = remote(yup, ylow, ys_sem.at[0], yr_sem.at[0], place(y=lax.rem(py + 1, ny)))
    y_down = remote(ydown, yhigh, ys_sem.at[1], yr_sem.at[1], place(y=lax.rem(py + ny - 1, ny)))

    @pl.when(jnp.logical_not(first[1]))
    def _():
        y_down.start()

    @pl.when(jnp.logical_not(jnp.logical_or(final[1], early)))
    def _():
        y_up.start()

    lane8 = lax.broadcasted_iota(jnp.int32, (8, 128), 1)
    slot_of = lane8 // 4
    place4 = lane8 % 4

    def pack(source, base, half):
        packed = jnp.zeros((8, 128), jnp.float32)
        for xx in range(4):
            plane = source[base, half * 4 + xx].astype(jnp.float32)
            for t in range(8):
                k = xx * 8 + t
                moved = pltpu.roll(plane[8 * t : 8 * t + 8], (4 * k + 2) % 128, 1)
                packed = jnp.where(slot_of == k, moved, packed)
        return packed

    for f in range(5):
        for half in range(2):
            zpack[2 * f + half] = pack(q, f, half)
    for half in range(2):
        zpack[10 + half] = pack(disp, 2, half) * STEP

    z_up = remote(zpack, zlow, zs_sem.at[0], zr_sem.at[0], place(z=lax.rem(pz + 1, nz)))
    z_down = remote(zpack, zhigh, zs_sem.at[1], zr_sem.at[1], place(z=lax.rem(pz + nz - 1, nz)))

    @pl.when(jnp.logical_not(final[2]))
    def _():
        z_up.start()

    @pl.when(jnp.logical_not(first[2]))
    def _():
        z_down.start()

    scale_y = jnp.where(
        jnp.logical_or(rows < 2, rows == 63), 0.0, STEP
    )
    scale_z = jnp.where(lanes == 0, STEP * low_scale[2], STEP)

    def planes(x, carry):
        vy = disp[1, x].astype(jnp.float32) * scale_y
        gy = half_weight(vy)
        up_y = vy > 0
        vz = disp[2, x].astype(jnp.float32) * scale_z
        right = jnp.where(lanes == 127, 0.0, jnp.maximum(ahead(vz), 0.0))
        right_w = jnp.where(lanes == 0, 0.0, 0.5 * right * (1.0 - right))
        left = jnp.minimum(vz, 0.0)
        left_w = jnp.where(
            jnp.logical_or(lanes == 0, lanes == 127), 0.0, -0.5 * left * (1.0 + left)
        )
        for f in range(5):
            value = q[f, x]
            below = back(value)
            above = ahead(value)
            slope = minmod(value - below, above - value)
            out_right = right * value + right_w * slope
            out_left = left * value + left_w * slope
            change_z = (back(out_right) - out_right) + (out_left - ahead(out_left))

            below = pltpu.roll(value, 1, 0)
            diff = value - below
            slope = minmod(diff, pltpu.roll(diff, 63, 0))
            flux = vy * jnp.where(up_y, below, value) + gy * jnp.where(
                up_y, pltpu.roll(slope, 1, 0), slope
            )
            acc[f, x] = (value + (flux - pltpu.roll(flux, 63, 0))) + change_z
        return carry

    lax.fori_loop(0, 2, planes, 0)

    @pl.when(late)
    def _():
        pl.semaphore_wait(round_sem.at[0], len(along_y) + late_steps)
        greet_late(round_sem.at[1])
        for peer in along_y:
            greet(round_sem.at[1], peer)

    lax.fori_loop(2, 3, planes, 0)

    wait_bytes(slots_a, tr_sem.at[0])
    group = part[0] + jnp.sum(slots_a[...], axis=0)
    part[1] = group
    slots_b[slot] = group

    @pl.when(late)
    def _():
        for (t, y), copy in zip(places, copies_b):
            skip = [ok for ok, spot in zip(in_column, ROOTS) if spot[0] == t and spot[2] == y]
            if skip:
                pl.when(jnp.logical_not(functools.reduce(jnp.logical_or, skip)))(copy.start)
            elif t < EARLY:
                copy.start()
        send_b(lambda t: jnp.abs(level - t) < 3 if t >= EARLY else None)

    @pl.when(early)
    def _():
        send_b(lambda t: level >= t if t < EARLY else None)

    lax.fori_loop(3, 5, planes, 0)

    @pl.when(early)
    def _():
        pl.semaphore_wait(reply_sem.at[0], 2)
        y_up.start()

    @pl.when(late)
    def _():
        pl.semaphore_wait(round_sem.at[1], len(along_y) + late_steps)
        send_b(lambda t: jnp.abs(level - t) > 2 if t >= EARLY else None)

    lax.fori_loop(5, 8, planes, 0)

    @pl.when(level < EARLY - 1)
    def _():
        pl.semaphore_wait(reply_sem.at[2], 4 * (EARLY - 1 - level))
        send_b(lambda t: level < t if t < EARLY else None)

    @pl.when(jnp.logical_not(first[1]))
    def _():
        y_up.wait_recv()

    @pl.when(jnp.logical_not(final[1]))
    def _():
        y_down.wait_recv()

    v0, v1, v63 = [disp[1, :, r, :].astype(jnp.float32) * STEP for r in (0, 1, 63)]
    v64 = jnp.where(final[1], v63 * flag_open[3], yhigh[10])
    v0 = v0 * low_scale[1]

    def flux_row(v, behind, at, slope_behind, slope_at):
        return v * jnp.where(v > 0, behind, at) + half_weight(v) * jnp.where(
            v > 0, slope_behind, slope_at
        )

    for f in range(5):
        q0, q1, q2, q61, q62, q63 = [q[f, :, r, :] for r in (0, 1, 2, 61, 62, 63)]
        lo1 = jnp.where(first[1], q0, ylow[2 * f + 1])
        lo2 = jnp.where(first[1], q0, ylow[2 * f])
        hi0 = jnp.where(final[1], q63, yhigh[2 * f])
        hi1 = jnp.where(final[1], q63, yhigh[2 * f + 1])
        s0 = minmod(q0 - lo1, q1 - q0)
        s63 = minmod(q63 - q62, hi0 - q63)
        flux_0 = flux_row(v0, lo1, q0, minmod(lo1 - lo2, q0 - lo1), s0)
        flux_1 = flux_row(v1, q0, q1, s0, minmod(q1 - q0, q2 - q1))
        flux_63 = flux_row(v63, q62, q63, minmod(q62 - q61, q63 - q62), s63)
        flux_64 = flux_row(v64, q63, hi0, s63, minmod(hi0 - q63, hi1 - hi0))
        acc[f, :, 0, :] += flux_0 - flux_1
        acc[f, :, 1, :] += flux_1
        acc[f, :, 62, :] -= flux_63
        acc[f, :, 63, :] += flux_63 - flux_64

    @pl.when(jnp.logical_not(first[2]))
    def _():
        z_up.wait_recv()

    @pl.when(jnp.logical_not(final[2]))
    def _():
        z_down.wait_recv()

    def face(four, v):
        behind = back(four)
        diff = four - behind
        slope = minmod(diff, ahead(diff))
        flux = v * jnp.where(v > 0, behind, four) + half_weight(v) * jnp.where(
            v > 0, back(slope), slope
        )
        return slope, flux

    for half in range(2):
        own_v = zpack[10 + half]
        v_low = jnp.where(place4 == 2, own_v * low_scale[2], own_v)
        v_high = jnp.where(final[2], back(own_v) * flag_open[5], zhigh[10 + half])
        left = jnp.minimum(v_low, 0.0)
        left_w = -0.5 * left * (1.0 + left)
        right = jnp.maximum(ahead(own_v), 0.0)
        right_w = 0.5 * right * (1.0 - right)
        for f in range(5):
            j = 2 * f + half
            own = zpack[j]
            ghost_low = jnp.where(place4 == 0, pltpu.roll(own, 126, 1), ahead(own))
            ghost_high = jnp.where(place4 == 2, back(own), pltpu.roll(own, 2, 1))
            low = jnp.where(place4 < 2, jnp.where(first[2], ghost_low, zlow[j]), own)
            high = jnp.where(place4 < 2, own, jnp.where(final[2], ghost_high, zhigh[j]))
            slope_low, flux_low = face(low, v_low)
            slope_high, flux_high = face(high, v_high)
            by_left = left_w * jnp.where(place4 == 1, slope_high, slope_low)
            by_right = right_w * slope_low
            entering = jnp.where(v_low > 0, flux_low, 0.0)
            zcorr[j] = jnp.where(
                place4 == 0,
                -ahead(by_left),
                jnp.where(
                    place4 == 1,
                    by_left - ahead(flux_high) + ahead(left * own),
                    jnp.where(place4 == 2, entering + by_left - by_right, back(by_right)),
                ),
            )

    last_early = level == EARLY - 1
    copies_c = [
        remote(part.at[2], slots_b.at[0], ts_sem.at[2], tr_sem.at[1], along_yz(0, dz))
        for dz in range(1, 6)
    ]

    @pl.when(last_early)
    def _():
        wait_bytes(slots_b.at[pl.ds(0, 4 * EARLY - 1)], tr_sem.at[1])
        part[2] = jnp.sum(slots_b[: 4 * EARLY], axis=0)
        pl.semaphore_wait(reply_sem.at[1], levels - EARLY)
        for copy in copies_c:
            copy.start()

    @pl.when(jnp.logical_not(final[0]))
    def _():
        face_copy.wait_recv()

    for i in range(9):
        if i == 0:
            v = disp[0, 0].astype(jnp.float32) * (STEP * low_scale[0])
        elif i < 8:
            v = disp[0, i].astype(jnp.float32) * STEP
        else:
            v_last = disp[0, 7].astype(jnp.float32) * (STEP * flag_open[1])
            v = jnp.where(final[0], v_last, xface[...].astype(jnp.float32) * STEP)
        vx[i] = v
        gx_w[i] = half_weight(v)

    inner = jnp.logical_not(jnp.logical_or(first[0], final[0]))
    edge_lanes = jnp.logical_or(lane8 < 2, lane8 > 125)
    for f in range(5):

        @pl.when(inner)
        def _():
            wait_bytes(xhalo.at[f], xr_sem.at[f])

        @pl.when(jnp.logical_not(inner))
        def _():
            wait_bytes(xhalo.at[f, 0], xr_sem.at[f])

        def tile(t, carry):
            part_rows = pl.ds(pl.multiple_of(t * 8, 8), 8)
            own = [q[f, i, part_rows] for i in range(8)]
            cell = (
                [jnp.where(first[0], own[0], xhalo[f, 0, r, part_rows]) for r in range(2)]
                + own
                + [jnp.where(final[0], own[7], xhalo[f, 1, r, part_rows]) for r in range(2)]
            )
            diff = [cell[i + 1] - cell[i] for i in range(11)]
            slope = [minmod(diff[i], diff[i + 1]) for i in range(10)]
            flux = []
            for i in range(9):
                v = vx[i, part_rows]
                g = gx_w[i, part_rows]
                flux.append(
                    v * jnp.where(v > 0, cell[i + 1], cell[i + 2])
                    + g * jnp.where(v > 0, slope[i], slope[i + 1])
                )
            for i in range(8):
                move = lax.rem(254 - 4 * ((i % 4) * 8 + t), 128)
                corr = pltpu.roll(zcorr[2 * f + i // 4], move, 1)
                corr = jnp.where(edge_lanes, corr, 0.0)
                acc[f, i, part_rows] += (flux[i] - flux[i + 1]) + corr
            return carry

        lax.fori_loop(0, 8, tile, 0)

    wait_bytes(slots_a, ts_sem.at[0])

    @pl.when(jnp.logical_not(first[0]))
    def _():
        face_copy.wait_send()

    for copy, there in (
        (y_up, final[1]),
        (y_down, first[1]),
        (z_up, final[2]),
        (z_down, first[2]),
    ):

        @pl.when(jnp.logical_not(there))
        def _():
            copy.wait_send()

    @pl.when(jnp.logical_not(final[0]))
    def _():
        wait_bytes(xhalo.at[:, 0], xs_sem.at[0])

    @pl.when(jnp.logical_not(first[0]))
    def _():
        wait_bytes(xhalo.at[:, 1], xs_sem.at[1])

    not_root = jnp.logical_not(root)

    def wait_rows(when, count, sem):
        @pl.when(when)
        def _():
            wait_bytes(slots_b.at[pl.ds(0, count)], sem)

    wait_rows(early, 4 * EARLY - 1, ts_sem.at[1])
    columns = [(x, c) for _, x, _, c in ROOTS]
    for skip in sorted({columns.count((x, c)) for x in range(4) for c in range(2)}):
        wait_rows(both(late, skipped == skip), 31 - skip, ts_sem.at[1])
    wait_rows(last_early, 5, ts_sem.at[2])
    wait_rows(late, len(ROOTS), ts_sem.at[3])
    wait_rows(level < EARLY - 1, 4 * EARLY - 1, tr_sem.at[1])
    wait_rows(both(early, not_root), 4 * (8 - EARLY), tr_sem.at[2])
    wait_rows(late, 1, tr_sem.at[1])
    wait_rows(late, 4 * (8 - EARLY) - 1, tr_sem.at[2])
    others = jnp.sum(slots_b[1 : 4 * EARLY], axis=0)
    near_sum = slots_b[0] + jnp.where(early, others, 0.0)

    @pl.when(root)
    def _():
        wait_bytes(slots_d, tr_sem.at[3])
        grand[...] = near_sum + jnp.sum(slots_d[...], axis=0)

    @pl.when(not_root)
    def _():
        grand[...] = near_sum + jnp.sum(slots_b[4 * EARLY :], axis=0)


def write_out(cells, acc, grand, new_density, new_momentum, new_energy, totals, pair, sem):
    stores = [
        pltpu.make_async_copy(acc.at[0], new_density, sem.at[0]),
        pltpu.make_async_copy(acc.at[1], new_energy, sem.at[0]),
    ] + [pltpu.make_async_copy(acc.at[2 + c], new_momentum.at[c], sem.at[0]) for c in range(3)]
    for store in stores:
        store.start()
    lane1 = lax.broadcasted_iota(jnp.int32, (1, 128), 1)
    both = grand[...]
    pair[0] = jnp.sum(jnp.where(lane1 < 64, both, 0.0)) / cells
    pair[1] = jnp.sum(jnp.where(lane1 < 64, 0.0, both)) / cells
    last = pltpu.make_async_copy(pair, totals, sem.at[1])
    last.start()
    pltpu.make_async_copy(acc, acc, sem.at[0]).wait()
    last.wait()


def shards(cells, density, momentum, energy, displacement, flags):
    f32, i32 = jnp.float32, jnp.int32
    anywhere = pl.BlockSpec(memory_space=pltpu.HBM)
    local = pl.BlockSpec(memory_space=pltpu.VMEM)
    inputs = [
        pltpu.with_memory_space_constraint(a, pltpu.HBM)
        for a in (density, momentum, energy, displacement, flags)
    ]
    acc, grand = pl.pallas_call(
        kernel,
        out_shape=(
            jax.ShapeDtypeStruct((5, 8, 64, 128), f32),
            jax.ShapeDtypeStruct((1, 128), f32),
        ),
        in_specs=[anywhere] * 5,
        out_specs=(local, local),
        scratch_shapes=[
            pltpu.VMEM((5, 8, 64, 128), f32),
            pltpu.VMEM((3, 8, 64, 128), i32),
            pltpu.SMEM((6,), i32),
            pltpu.VMEM((9, 64, 128), f32),
            pltpu.VMEM((9, 64, 128), f32),
            pltpu.VMEM((5, 2, 2, 64, 128), f32),
            pltpu.VMEM((64, 128), i32),
            pltpu.VMEM((10, 8, 128), f32),
            pltpu.VMEM((11, 8, 128), f32),
            pltpu.VMEM((10, 8, 128), f32),
            pltpu.VMEM((11, 8, 128), f32),
            pltpu.VMEM((12, 8, 128), f32),
            pltpu.VMEM((12, 8, 128), f32),
            pltpu.VMEM((12, 8, 128), f32),
            pltpu.VMEM((10, 8, 128), f32),
            pltpu.VMEM((3, 1, 128), f32),
            pltpu.VMEM((7, 1, 128), f32),
            pltpu.VMEM((32, 1, 128), f32),
            pltpu.VMEM((160, 1, 128), f32),
            pltpu.SemaphoreType.DMA((4,)),
            pltpu.SemaphoreType.DMA((3,)),
            pltpu.SemaphoreType.DMA((6,)),
            pltpu.SemaphoreType.DMA((2,)),
            pltpu.SemaphoreType.DMA((2,)),
            pltpu.SemaphoreType.DMA((2,)),
            pltpu.SemaphoreType.DMA((2,)),
            pltpu.SemaphoreType.DMA((4,)),
            pltpu.SemaphoreType.DMA((4,)),
            pltpu.SemaphoreType.REGULAR((2,)),
            pltpu.SemaphoreType.REGULAR((3,)),
        ],
        compiler_params=pltpu.CompilerParams(
            collective_id=0, has_side_effects=True, vmem_limit_bytes=16 * 2**20
        ),
        name="remap",
    )(*inputs)
    return pl.pallas_call(
        functools.partial(write_out, cells),
        out_shape=(
            jax.ShapeDtypeStruct(density.shape, f32),
            jax.ShapeDtypeStruct(momentum.shape, f32),
            jax.ShapeDtypeStruct(energy.shape, f32),
            jax.ShapeDtypeStruct((2,), f32),
        ),
        in_specs=[local, local],
        out_specs=[anywhere] * 4,
        scratch_shapes=[pltpu.SMEM((2,), f32), pltpu.SemaphoreType.DMA((2,))],
        compiler_params=pltpu.CompilerParams(vmem_limit_bytes=4 * 2**20),
        name="write_out",
    )(acc, grand)


def solution(mesh):
    cells = float(mesh.shape["gx"] * mesh.shape["gy"] * mesh.shape["gz"] * 8 * 64 * 128)
    block = P("gx", "gy", "gz")
    three = P(None, "gx", "gy", "gz")
    return jax.shard_map(
        functools.partial(shards, cells),
        mesh=mesh,
        in_specs=(block, three, block, three, P()),
        out_specs=(block, three, block, P()),
        check_vma=False,
    )
```

```python
import functools

import jax
import jax.numpy as jnp
from jax import lax
from jax.experimental import pallas as pl
from jax.experimental.pallas import tpu as pltpu
from jax.sharding import PartitionSpec as P

MESH = pl.DeviceIdType.MESH
STEP = 1.0 / 256.0
EARLY = 3
ROOTS = (
    (0, 0, 0, 1),
    (0, 1, 0, 0),
    (0, 0, 1, 0),
    (0, 2, 0, 0),
    (0, 3, 0, 0),
    (0, 0, 2, 0),
    (0, 0, 3, 0),
    (0, 0, 0, 0),
    (0, 1, 0, 1),
    (0, 2, 0, 1),
    (0, 1, 1, 0),
    (0, 0, 1, 1),
    (1, 0, 0, 0),
    (1, 0, 0, 1),
    (1, 1, 0, 0),
    (1, 0, 1, 0),
)


def minmod(left_diff, right_diff):
    least = jnp.minimum(left_diff, right_diff)
    most = jnp.maximum(left_diff, right_diff)
    return jnp.maximum(least, jnp.minimum(most, 0.0))


def half_weight(v):
    size = jnp.abs(v)
    return 0.5 * size * (1.0 - size)


def back(block):
    return pltpu.roll(block, 1, 1)


def ahead(block):
    return pltpu.roll(block, 127, 1)


def kernel(
    density,
    momentum,
    energy,
    displacement,
    flags,
    acc,
    grand,
    q,
    disp,
    flag,
    vx,
    gx_w,
    xhalo,
    xface,
    yup,
    ydown,
    yin,
    zpack,
    zin,
    zcorr,
    part,
    slots_a,
    slots_b,
    slots_d,
    load_sem,
    xs_sem,
    xr_sem,
    ys_sem,
    yr_sem,
    zs_sem,
    zr_sem,
    ts_sem,
    tr_sem,
    round_sem,
):
    px, py, pz = lax.axis_index("gx"), lax.axis_index("gy"), lax.axis_index("gz")
    nx, ny, nz = lax.axis_size("gx"), lax.axis_size("gy"), lax.axis_size("gz")
    core = pz % 2
    zl = (pz // 2) % 2
    def wait_bytes(of, sem):
        pltpu.make_async_copy(of, of, sem).wait()

    def place(x=None, y=None, z=None):
        target = {}
        if x is not None:
            target["gx"] = x
        if y is not None:
            target["gy"] = y
        if z is not None:
            target["gz"] = z
        return target

    level = py * 2 + zl
    levels = 2 * ny
    early = level < EARLY
    both = jnp.logical_and
    late = jnp.logical_not(early)

    def along_yz(dy, dz):
        chip = lax.rem(level + dz, levels)
        return place(y=chip // 2, z=lax.rem(pz + 4 * dy, nz) + 2 * (chip % 2 - zl))

    def greet(sem, peer):
        pl.semaphore_signal(sem, inc=1, device_id=peer, device_id_type=MESH)

    stage_a = [
        place(x=lax.rem(px + dx, nx), z=pz + dc * (1 - 2 * core))
        for dx in (2, 1, 3, 0)
        for dc in range(2)
        if dx or dc
    ]
    along_y = [along_yz(dy, 0) for dy in (2, 1, 3)]
    steps = [-2, 2, -1, 1]
    late_step = [
        jnp.logical_and(level + step >= EARLY, level + step < levels) for step in steps
    ]
    late_steps = sum(ok.astype(jnp.int32) for ok in late_step)
    has_across = jnp.where(core == 1, pz < nz - 1, pz > 0)
    across = place(z=lax.rem(pz + nz + 2 * core - 1, nz))

    def greet_late(sem):
        for step, ok in zip(steps, late_step):

            @pl.when(ok)
            def _():
                greet(sem, along_yz(0, step % 8))

    barrier = pltpu.get_barrier_semaphore()

    @pl.when(late)
    def _():
        greet_late(barrier)

    for peer in stage_a + along_y:
        greet(barrier, peer)

    flag_copy = pltpu.make_async_copy(flags, flag, load_sem.at[0])
    flag_copy.start()
    pltpu.make_async_copy(density, q.at[0], load_sem.at[1]).start()
    pltpu.make_async_copy(energy, q.at[1], load_sem.at[1]).start()
    pltpu.make_async_copy(displacement, disp, load_sem.at[1]).start()
    momentum_load = pltpu.make_async_copy(momentum, q.at[pl.ds(2, 3)], load_sem.at[2])
    momentum_load.start()

    @pl.when(has_across)
    def _():
        greet(barrier, across)

    me_y = pz // 4
    in_column = [both(px == x, core == c) for _, x, _, c in ROOTS]
    skipped = sum(ok.astype(jnp.int32) for ok in in_column)
    at_root = [
        both(ok, both(level == t, me_y == y)) for ok, (t, _, y, _) in zip(in_column, ROOTS)
    ]
    root = functools.reduce(jnp.logical_or, at_root)

    @pl.when(root)
    def _():
        def greet_group(k, carry):
            t = 7 - k // 4
            z = 4 * lax.rem(k, 4) + 2 * lax.rem(t, 2)
            for x in range(4):
                for c in range(2):
                    greet(barrier, place(x=x, y=t // 2, z=z + c))
            return carry

        lax.fori_loop(0, 4 * (8 - EARLY), greet_group, 0)

    @pl.when(early)
    def _():
        for dz in range(1, 8):

            @pl.when(level + dz < levels)
            def _():
                for dy in range(4):
                    greet(barrier, along_yz(dy, dz))


    flag_copy.wait()
    wait_bytes(q, load_sem.at[1])

    def wait_pair(buffer, axis, sem):
        one = jnp.logical_or(first[axis], final[axis])

        @pl.when(one)
        def _():
            wait_bytes(buffer.at[0], sem)

        @pl.when(jnp.logical_not(one))
        def _():
            wait_bytes(buffer, sem)

    flag_open = [flag[i].astype(jnp.float32) for i in range(6)]
    first = [px == 0, py == 0, pz == 0]
    final = [px == nx - 1, py == ny - 1, pz == nz - 1]
    low_scale = [jnp.where(first[a], flag_open[2 * a], 1.0) for a in range(3)]
    gain = [jnp.where(first[a], flag_open[2 * a] * STEP, 0.0) for a in range(3)]
    loss = [jnp.where(final[a], flag_open[2 * a + 1] * -STEP, 0.0) for a in range(3)]

    rows = lax.broadcasted_iota(jnp.int32, (64, 128), 0)
    lanes = lax.broadcasted_iota(jnp.int32, (64, 128), 1)
    weight_y = jnp.where(rows == 0, gain[1], jnp.where(rows == 63, loss[1], 0.0))
    weight_z = jnp.where(lanes == 0, gain[2], jnp.where(lanes == 127, loss[2], 0.0))

    def fold(block):
        return jnp.sum(block.reshape(8, 8, 128), axis=0)

    def plane_sum(x, sums):
        weight = (
            1.0
            + weight_y * disp[1, x].astype(jnp.float32)
            + weight_z * disp[2, x].astype(jnp.float32)
        )
        return (sums[0] + fold(q[0, x] * weight), sums[1] + fold(q[1, x] * weight))

    weight_low = gain[0] * disp[0, 0].astype(jnp.float32)
    weight_high = loss[0] * disp[0, 7].astype(jnp.float32)
    sums = tuple(fold(q[f, 0] * weight_low + q[f, 7] * weight_high) for f in (0, 1))
    sums = lax.fori_loop(0, 8, plane_sum, sums)
    lane1 = lax.broadcasted_iota(jnp.int32, (1, 128), 1)

    def halves(low, high):
        low = jnp.sum(low, axis=0, keepdims=True)
        high = jnp.sum(high, axis=0, keepdims=True)
        return jnp.where(lane1 < 64, low + pltpu.roll(low, 64, 1), high + pltpu.roll(high, 64, 1))

    part[0] = halves(*sums)
    momentum_load.wait()

    greeted = (
        len(stage_a)
        + len(along_y)
        + has_across.astype(jnp.int32)
        + jnp.where(early, 0, len(ROOTS))
        + jnp.where(early, 4 * level, 4 * EARLY + late_steps)
    )
    pl.semaphore_wait(barrier, greeted)

    def remote(src, dst, send_sem, recv_sem, peer):
        return pltpu.make_async_remote_copy(
            src_ref=src,
            dst_ref=dst,
            send_sem=send_sem,
            recv_sem=recv_sem,
            device_id=peer,
            device_id_type=MESH,
        )

    copies_a = [
        remote(part.at[0], slots_a.at[i], ts_sem.at[0], tr_sem.at[0], peer)
        for i, peer in enumerate(stage_a)
    ]
    slot = level * 4 + pz // 4
    arrival = tr_sem.at[jnp.where(early, 1, 2)]
    base_z = pz - 4 * me_y - 2 * zl
    places = [(t, y) for t in range(8) for y in (0, 1, 3, 2)]
    copies_b = [
        remote(
            part.at[1],
            slots_b.at[slot],
            ts_sem.at[1],
            arrival,
            place(y=t // 2, z=base_z + 4 * y + 2 * (t % 2)),
        )
        for t, y in places
    ]

    def send_b(wanted):
        for (t, y), copy in zip(places, copies_b):
            ok = wanted(t)
            if ok is not None:
                other = jnp.logical_or(level != t, me_y != y)
                pl.when(jnp.logical_and(ok, other))(copy.start)
    index = (level - EARLY) * 32 + me_y * 8 + px * 2 + core
    to_roots = [
        remote(
            part.at[0],
            slots_d.at[index],
            ts_sem.at[1],
            tr_sem.at[2],
            place(x=x, y=t // 2, z=4 * y + 2 * (t % 2) + c),
        )
        for t, x, y, c in ROOTS
    ]

    @pl.when(late)
    def _():
        to_roots[0].start()

    for copy in copies_a:
        copy.start()

    @pl.when(late)
    def _():
        for copy in to_roots[1:]:
            copy.start()
        greet_late(round_sem.at[0])
        for peer in along_y:
            greet(round_sem.at[0], peer)

    for back_step in (1, 2):

        @pl.when(jnp.logical_and(level - back_step >= 0, level - back_step < EARLY))
        def _():
            greet(round_sem.at[0], along_yz(0, 8 - back_step))

    @pl.when(early)
    def _():
        for target in range(EARLY - 1):

            @pl.when(target < level)
            def _():
                for dy in range(4):
                    greet(round_sem.at[2], along_yz(dy, lax.rem(levels + target - level, levels)))

    @pl.when(jnp.logical_not(early))
    def _():
        greet(round_sem.at[1], along_yz(0, lax.rem(levels + EARLY - 1 - level, levels)))

    x_next = place(x=lax.rem(px + 1, nx))
    x_prev = place(x=lax.rem(px + nx - 1, nx))
    face_copy = remote(disp.at[0, 0], xface, xs_sem.at[1], xr_sem.at[2], x_prev)
    up_copies = [
        remote(q.at[f, pl.ds(6, 2)], xhalo.at[f, 0], xs_sem.at[0], xr_sem.at[f // 3], x_next) for f in range(5)
    ]
    down_copies = [
        remote(q.at[f, pl.ds(0, 2)], xhalo.at[f, 1], xs_sem.at[0], xr_sem.at[f // 3], x_prev)
        for f in range(5)
    ]

    @pl.when(jnp.logical_not(first[0]))
    def _():
        face_copy.start()

    for f in range(5):

        @pl.when(jnp.logical_not(final[0]))
        def _():
            up_copies[f].start()

        @pl.when(jnp.logical_not(first[0]))
        def _():
            down_copies[f].start()

    for f in range(5):
        for r in range(2):
            yup[2 * f + r] = q[f, :, 62 + r, :]
            ydown[2 * f + r] = q[f, :, r, :]
    yup[10] = jnp.zeros((8, 128), jnp.float32)
    ydown[10] = disp[1, :, 0, :].astype(jnp.float32) * STEP

    y_up = remote(yup, yin.at[0], ys_sem.at[0], yr_sem.at[0], place(y=lax.rem(py + 1, ny)))
    y_down = remote(ydown, yin.at[1], ys_sem.at[0], yr_sem.at[0], place(y=lax.rem(py + ny - 1, ny)))

    @pl.when(jnp.logical_not(first[1]))
    def _():
        y_down.start()

    @pl.when(jnp.logical_not(jnp.logical_or(final[1], early)))
    def _():
        y_up.start()

    lane8 = lax.broadcasted_iota(jnp.int32, (8, 128), 1)
    slot_of = lane8 // 4
    place4 = lane8 % 4

    def pack(source, base, half):
        packed = jnp.zeros((8, 128), jnp.float32)
        for xx in range(4):
            plane = source[base, half * 4 + xx].astype(jnp.float32)
            for t in range(8):
                k = xx * 8 + t
                moved = pltpu.roll(plane[8 * t : 8 * t + 8], (4 * k + 2) % 128, 1)
                packed = jnp.where(slot_of == k, moved, packed)
        return packed

    for f in range(5):
        for half in range(2):
            zpack[2 * f + half] = pack(q, f, half)
    for half in range(2):
        zpack[10 + half] = pack(disp, 2, half) * STEP

    z_up = remote(zpack, zin.at[0], zs_sem.at[0], zr_sem.at[0], place(z=lax.rem(pz + 1, nz)))
    z_down = remote(zpack, zin.at[1], zs_sem.at[0], zr_sem.at[0], place(z=lax.rem(pz + nz - 1, nz)))

    @pl.when(jnp.logical_not(final[2]))
    def _():
        z_up.start()

    @pl.when(jnp.logical_not(first[2]))
    def _():
        z_down.start()

    scale_y = jnp.where(
        jnp.logical_or(rows < 2, rows == 63), 0.0, STEP
    )
    scale_z = jnp.where(lanes == 0, STEP * low_scale[2], STEP)

    def planes(x, carry):
        vy = disp[1, x].astype(jnp.float32) * scale_y
        gy = half_weight(vy)
        up_y = vy > 0
        vz = disp[2, x].astype(jnp.float32) * scale_z
        right = jnp.where(lanes == 127, 0.0, jnp.maximum(ahead(vz), 0.0))
        right_w = jnp.where(lanes == 0, 0.0, 0.5 * right * (1.0 - right))
        left = jnp.minimum(vz, 0.0)
        left_w = jnp.where(
            jnp.logical_or(lanes == 0, lanes == 127), 0.0, -0.5 * left * (1.0 + left)
        )
        for f in range(5):
            value = q[f, x]
            below = back(value)
            above = ahead(value)
            slope = minmod(value - below, above - value)
            out_right = right * value + right_w * slope
            out_left = left * value + left_w * slope
            change_z = (back(out_right) - out_right) + (out_left - ahead(out_left))

            below = pltpu.roll(value, 1, 0)
            diff = value - below
            slope = minmod(diff, pltpu.roll(diff, 63, 0))
            flux = vy * jnp.where(up_y, below, value) + gy * jnp.where(
                up_y, pltpu.roll(slope, 1, 0), slope
            )
            acc[f, x] = (value + (flux - pltpu.roll(flux, 63, 0))) + change_z
        return carry

    lax.fori_loop(0, 2, planes, 0)

    @pl.when(late)
    def _():
        pl.semaphore_wait(round_sem.at[0], len(along_y) + late_steps)
        greet_late(round_sem.at[1])
        for peer in along_y:
            greet(round_sem.at[1], peer)

    lax.fori_loop(2, 3, planes, 0)

    wait_bytes(slots_a, tr_sem.at[0])
    group = part[0] + jnp.sum(slots_a[...], axis=0)
    part[1] = group
    slots_b[slot] = group

    @pl.when(late)
    def _():
        for (t, y), copy in zip(places, copies_b):
            skip = [ok for ok, spot in zip(in_column, ROOTS) if spot[0] == t and spot[2] == y]
            if skip:
                pl.when(jnp.logical_not(functools.reduce(jnp.logical_or, skip)))(copy.start)
            elif t < EARLY:
                copy.start()
        send_b(lambda t: jnp.abs(level - t) < 3 if t >= EARLY else None)

    @pl.when(early)
    def _():
        send_b(lambda t: level >= t if t < EARLY else None)

    lax.fori_loop(3, 5, planes, 0)

    @pl.when(early)
    def _():
        pl.semaphore_wait(round_sem.at[0], 2)
        y_up.start()

    @pl.when(late)
    def _():
        pl.semaphore_wait(round_sem.at[1], len(along_y) + late_steps)
        send_b(lambda t: jnp.abs(level - t) > 2 if t >= EARLY else None)

    lax.fori_loop(5, 8, planes, 0)

    @pl.when(level < EARLY - 1)
    def _():
        pl.semaphore_wait(round_sem.at[2], 4 * (EARLY - 1 - level))
        send_b(lambda t: level < t if t < EARLY else None)

    wait_pair(yin, 1, yr_sem.at[0])

    v0, v1, v63 = [disp[1, :, r, :].astype(jnp.float32) * STEP for r in (0, 1, 63)]
    v64 = jnp.where(final[1], v63 * flag_open[3], yin[1, 10])
    v0 = v0 * low_scale[1]

    def flux_row(v, behind, at, slope_behind, slope_at):
        return v * jnp.where(v > 0, behind, at) + half_weight(v) * jnp.where(
            v > 0, slope_behind, slope_at
        )

    for f in range(5):
        q0, q1, q2, q61, q62, q63 = [q[f, :, r, :] for r in (0, 1, 2, 61, 62, 63)]
        lo1 = jnp.where(first[1], q0, yin[0, 2 * f + 1])
        lo2 = jnp.where(first[1], q0, yin[0, 2 * f])
        hi0 = jnp.where(final[1], q63, yin[1, 2 * f])
        hi1 = jnp.where(final[1], q63, yin[1, 2 * f + 1])
        s0 = minmod(q0 - lo1, q1 - q0)
        s63 = minmod(q63 - q62, hi0 - q63)
        flux_0 = flux_row(v0, lo1, q0, minmod(lo1 - lo2, q0 - lo1), s0)
        flux_1 = flux_row(v1, q0, q1, s0, minmod(q1 - q0, q2 - q1))
        flux_63 = flux_row(v63, q62, q63, minmod(q62 - q61, q63 - q62), s63)
        flux_64 = flux_row(v64, q63, hi0, s63, minmod(hi0 - q63, hi1 - hi0))
        acc[f, :, 0, :] += flux_0 - flux_1
        acc[f, :, 1, :] += flux_1
        acc[f, :, 62, :] -= flux_63
        acc[f, :, 63, :] += flux_63 - flux_64

    wait_pair(zin, 2, zr_sem.at[0])

    def face(four, v):
        behind = back(four)
        diff = four - behind
        slope = minmod(diff, ahead(diff))
        flux = v * jnp.where(v > 0, behind, four) + half_weight(v) * jnp.where(
            v > 0, back(slope), slope
        )
        return slope, flux

    for half in range(2):
        own_v = zpack[10 + half]
        v_low = jnp.where(place4 == 2, own_v * low_scale[2], own_v)
        v_high = jnp.where(final[2], back(own_v) * flag_open[5], zin[1, 10 + half])
        left = jnp.minimum(v_low, 0.0)
        left_w = -0.5 * left * (1.0 + left)
        right = jnp.maximum(ahead(own_v), 0.0)
        right_w = 0.5 * right * (1.0 - right)
        for f in range(5):
            j = 2 * f + half
            own = zpack[j]
            ghost_low = jnp.where(place4 == 0, pltpu.roll(own, 126, 1), ahead(own))
            ghost_high = jnp.where(place4 == 2, back(own), pltpu.roll(own, 2, 1))
            low = jnp.where(place4 < 2, jnp.where(first[2], ghost_low, zin[0, j]), own)
            high = jnp.where(place4 < 2, own, jnp.where(final[2], ghost_high, zin[1, j]))
            slope_low, flux_low = face(low, v_low)
            slope_high, flux_high = face(high, v_high)
            by_left = left_w * jnp.where(place4 == 1, slope_high, slope_low)
            by_right = right_w * slope_low
            entering = jnp.where(v_low > 0, flux_low, 0.0)
            zcorr[j] = jnp.where(
                place4 == 0,
                -ahead(by_left),
                jnp.where(
                    place4 == 1,
                    by_left - ahead(flux_high) + ahead(left * own),
                    jnp.where(place4 == 2, entering + by_left - by_right, back(by_right)),
                ),
            )

    last_early = level == EARLY - 1
    copies_c = [
        remote(part.at[2], slots_b.at[0], ts_sem.at[1], tr_sem.at[1], along_yz(0, dz))
        for dz in range(1, 6)
    ]

    @pl.when(last_early)
    def _():
        wait_bytes(slots_b.at[pl.ds(0, 4 * EARLY - 1)], tr_sem.at[1])
        part[2] = jnp.sum(slots_b[: 4 * EARLY], axis=0)
        pl.semaphore_wait(round_sem.at[1], levels - EARLY)
        for copy in copies_c:
            copy.start()

    @pl.when(jnp.logical_not(final[0]))
    def _():
        face_copy.wait_recv()

    for i in range(9):
        if i == 0:
            v = disp[0, 0].astype(jnp.float32) * (STEP * low_scale[0])
        elif i < 8:
            v = disp[0, i].astype(jnp.float32) * STEP
        else:
            v_last = disp[0, 7].astype(jnp.float32) * (STEP * flag_open[1])
            v = jnp.where(final[0], v_last, xface[...].astype(jnp.float32) * STEP)
        vx[i] = v
        gx_w[i] = half_weight(v)

    inner = jnp.logical_not(jnp.logical_or(first[0], final[0]))
    edge_lanes = jnp.logical_or(lane8 < 2, lane8 > 125)
    for f in range(5):

        if f in (0, 3):
            group = pl.ds(f, 3 - f // 3)

            @pl.when(inner)
            def _():
                wait_bytes(xhalo.at[group], xr_sem.at[f // 3])

            @pl.when(jnp.logical_not(inner))
            def _():
                wait_bytes(xhalo.at[group, 0], xr_sem.at[f // 3])

        def tile(t, carry):
            part_rows = pl.ds(pl.multiple_of(t * 8, 8), 8)
            own = [q[f, i, part_rows] for i in range(8)]
            cell = (
                [jnp.where(first[0], own[0], xhalo[f, 0, r, part_rows]) for r in range(2)]
                + own
                + [jnp.where(final[0], own[7], xhalo[f, 1, r, part_rows]) for r in range(2)]
            )
            diff = [cell[i + 1] - cell[i] for i in range(11)]
            slope = [minmod(diff[i], diff[i + 1]) for i in range(10)]
            flux = []
            for i in range(9):
                v = vx[i, part_rows]
                g = gx_w[i, part_rows]
                flux.append(
                    v * jnp.where(v > 0, cell[i + 1], cell[i + 2])
                    + g * jnp.where(v > 0, slope[i], slope[i + 1])
                )
            for i in range(8):
                move = lax.rem(254 - 4 * ((i % 4) * 8 + t), 128)
                corr = pltpu.roll(zcorr[2 * f + i // 4], move, 1)
                corr = jnp.where(edge_lanes, corr, 0.0)
                acc[f, i, part_rows] += (flux[i] - flux[i + 1]) + corr
            return carry

        lax.fori_loop(0, 8, tile, 0)

    wait_bytes(slots_a, ts_sem.at[0])

    @pl.when(jnp.logical_not(first[0]))
    def _():
        face_copy.wait_send()

    wait_pair(yin, 1, ys_sem.at[0])
    wait_pair(zin, 2, zs_sem.at[0])

    @pl.when(inner)
    def _():
        wait_bytes(xhalo, xs_sem.at[0])

    @pl.when(jnp.logical_not(inner))
    def _():
        wait_bytes(xhalo.at[:, 0], xs_sem.at[0])

    not_root = jnp.logical_not(root)

    def wait_rows(when, count, sem):
        @pl.when(when)
        def _():
            wait_bytes(slots_d.at[pl.ds(0, count)], sem)

    wait_rows(level < EARLY - 1, 4 * EARLY - 1, ts_sem.at[1])
    wait_rows(last_early, 4 * EARLY + 4, ts_sem.at[1])
    columns = [(x, c) for _, x, _, c in ROOTS]
    for skip in sorted({columns.count((x, c)) for x in range(4) for c in range(2)}):
        wait_rows(both(late, skipped == skip), 31 - skip + len(ROOTS), ts_sem.at[1])
    wait_rows(level < EARLY - 1, 4 * EARLY - 1, tr_sem.at[1])
    wait_rows(both(early, not_root), 4 * (8 - EARLY), tr_sem.at[2])
    wait_rows(late, 1, tr_sem.at[1])
    wait_rows(late, 4 * (8 - EARLY) - 1, tr_sem.at[2])
    others = jnp.sum(slots_b[1 : 4 * EARLY], axis=0)
    near_sum = slots_b[0] + jnp.where(early, others, 0.0)

    @pl.when(root)
    def _():
        wait_bytes(slots_d, tr_sem.at[2])
        grand[...] = near_sum + jnp.sum(slots_d[...], axis=0)

    @pl.when(not_root)
    def _():
        grand[...] = near_sum + jnp.sum(slots_b[4 * EARLY :], axis=0)


def write_out(cells, acc, grand, new_density, new_momentum, new_energy, totals, pair, sem):
    stores = [
        pltpu.make_async_copy(acc.at[0], new_density, sem.at[0]),
        pltpu.make_async_copy(acc.at[1], new_energy, sem.at[0]),
    ] + [pltpu.make_async_copy(acc.at[2 + c], new_momentum.at[c], sem.at[0]) for c in range(3)]
    for store in stores:
        store.start()
    lane1 = lax.broadcasted_iota(jnp.int32, (1, 128), 1)
    both = grand[...]
    pair[0] = jnp.sum(jnp.where(lane1 < 64, both, 0.0)) / cells
    pair[1] = jnp.sum(jnp.where(lane1 < 64, 0.0, both)) / cells
    last = pltpu.make_async_copy(pair, totals, sem.at[1])
    last.start()
    pltpu.make_async_copy(acc, acc, sem.at[0]).wait()
    last.wait()


def shards(cells, density, momentum, energy, displacement, flags):
    f32, i32 = jnp.float32, jnp.int32
    anywhere = pl.BlockSpec(memory_space=pltpu.HBM)
    local = pl.BlockSpec(memory_space=pltpu.VMEM)
    inputs = [
        pltpu.with_memory_space_constraint(a, pltpu.HBM)
        for a in (density, momentum, energy, displacement, flags)
    ]
    acc, grand = pl.pallas_call(
        kernel,
        out_shape=(
            jax.ShapeDtypeStruct((5, 8, 64, 128), f32),
            jax.ShapeDtypeStruct((1, 128), f32),
        ),
        in_specs=[anywhere] * 5,
        out_specs=(local, local),
        scratch_shapes=[
            pltpu.VMEM((5, 8, 64, 128), f32),
            pltpu.VMEM((3, 8, 64, 128), i32),
            pltpu.SMEM((6,), i32),
            pltpu.VMEM((9, 64, 128), f32),
            pltpu.VMEM((9, 64, 128), f32),
            pltpu.VMEM((5, 2, 2, 64, 128), f32),
            pltpu.VMEM((64, 128), i32),
            pltpu.VMEM((11, 8, 128), f32),
            pltpu.VMEM((11, 8, 128), f32),
            pltpu.VMEM((2, 11, 8, 128), f32),
            pltpu.VMEM((12, 8, 128), f32),
            pltpu.VMEM((2, 12, 8, 128), f32),
            pltpu.VMEM((10, 8, 128), f32),
            pltpu.VMEM((3, 1, 128), f32),
            pltpu.VMEM((7, 1, 128), f32),
            pltpu.VMEM((32, 1, 128), f32),
            pltpu.VMEM((160, 1, 128), f32),
            pltpu.SemaphoreType.DMA((3,)),
            pltpu.SemaphoreType.DMA((2,)),
            pltpu.SemaphoreType.DMA((3,)),
            pltpu.SemaphoreType.DMA((1,)),
            pltpu.SemaphoreType.DMA((1,)),
            pltpu.SemaphoreType.DMA((1,)),
            pltpu.SemaphoreType.DMA((1,)),
            pltpu.SemaphoreType.DMA((2,)),
            pltpu.SemaphoreType.DMA((3,)),
            pltpu.SemaphoreType.REGULAR((3,)),
        ],
        compiler_params=pltpu.CompilerParams(
            collective_id=0, has_side_effects=True, vmem_limit_bytes=16 * 2**20
        ),
        name="remap",
    )(*inputs)
    return pl.pallas_call(
        functools.partial(write_out, cells),
        out_shape=(
            jax.ShapeDtypeStruct(density.shape, f32),
            jax.ShapeDtypeStruct(momentum.shape, f32),
            jax.ShapeDtypeStruct(energy.shape, f32),
            jax.ShapeDtypeStruct((2,), f32),
        ),
        in_specs=[local, local],
        out_specs=[anywhere] * 4,
        scratch_shapes=[pltpu.SMEM((2,), f32), pltpu.SemaphoreType.DMA((2,))],
        compiler_params=pltpu.CompilerParams(vmem_limit_bytes=4 * 2**20),
        name="write_out",
    )(acc, grand)


def solution(mesh):
    cells = float(mesh.shape["gx"] * mesh.shape["gy"] * mesh.shape["gz"] * 8 * 64 * 128)
    block = P("gx", "gy", "gz")
    three = P(None, "gx", "gy", "gz")
    return jax.shard_map(
        functools.partial(shards, cells),
        mesh=mesh,
        in_specs=(block, three, block, three, P()),
        out_specs=(block, three, block, P()),
        check_vma=False,
    )
```

```python
import functools

import jax
import jax.numpy as jnp
from jax import lax
from jax.experimental import pallas as pl
from jax.experimental.pallas import tpu as pltpu
from jax.sharding import PartitionSpec as P

MESH = pl.DeviceIdType.MESH
STEP = 1.0 / 256.0
EARLY = 3
ROOTS = (
    (0, 0, 0, 1),
    (0, 1, 0, 0),
    (0, 0, 1, 0),
    (0, 2, 0, 0),
    (0, 3, 0, 0),
    (0, 0, 2, 0),
    (0, 0, 3, 0),
    (0, 0, 0, 0),
    (0, 1, 0, 1),
    (0, 2, 0, 1),
    (0, 1, 1, 0),
    (0, 0, 1, 1),
    (1, 0, 0, 0),
    (1, 0, 0, 1),
    (1, 1, 0, 0),
    (1, 0, 1, 0),
)


def minmod(left_diff, right_diff):
    least = jnp.minimum(left_diff, right_diff)
    most = jnp.maximum(left_diff, right_diff)
    return jnp.maximum(least, jnp.minimum(most, 0.0))


def half_weight(v):
    size = jnp.abs(v)
    return 0.5 * size * (1.0 - size)


def row_sum(rows, start, count):
    sums = [rows[start + i] for i in range(10)]
    for i in range(10, count):
        sums[i % 10] = sums[i % 10] + rows[start + i]
    while len(sums) > 1:
        paired = [sums[i] + sums[i + 1] for i in range(0, len(sums) - 1, 2)]
        sums = paired + sums[len(paired) * 2 :]
    return sums[0]


def back(block):
    return pltpu.roll(block, 1, 1)


def ahead(block):
    return pltpu.roll(block, 127, 1)


def kernel(
    density,
    momentum,
    energy,
    displacement,
    flags,
    acc,
    grand,
    q,
    disp,
    flag,
    vx,
    gx_w,
    xhalo,
    xface,
    yup,
    ydown,
    yin,
    zpack,
    zin,
    zcorr,
    part,
    slots_a,
    slots_b,
    slots_d,
    load_sem,
    xs_sem,
    xr_sem,
    ys_sem,
    yr_sem,
    zs_sem,
    zr_sem,
    ts_sem,
    tr_sem,
    round_sem,
):
    px, py, pz = lax.axis_index("gx"), lax.axis_index("gy"), lax.axis_index("gz")
    nx, ny, nz = lax.axis_size("gx"), lax.axis_size("gy"), lax.axis_size("gz")
    core = pz % 2
    zl = (pz // 2) % 2
    def wait_bytes(of, sem):
        pltpu.make_async_copy(of, of, sem).wait()

    def place(x=None, y=None, z=None):
        target = {}
        if x is not None:
            target["gx"] = x
        if y is not None:
            target["gy"] = y
        if z is not None:
            target["gz"] = z
        return target

    level = py * 2 + zl
    levels = 2 * ny
    early = level < EARLY
    both = jnp.logical_and
    late = jnp.logical_not(early)

    def along_yz(dy, dz):
        chip = lax.rem(level + dz, levels)
        return place(y=chip // 2, z=lax.rem(pz + 4 * dy, nz) + 2 * (chip % 2 - zl))

    def greet(sem, peer):
        pl.semaphore_signal(sem, inc=1, device_id=peer, device_id_type=MESH)

    stage_a = [
        place(x=lax.rem(px + dx, nx), z=pz + dc * (1 - 2 * core))
        for dx in (2, 1, 3, 0)
        for dc in range(2)
        if dx or dc
    ]
    along_y = [along_yz(dy, 0) for dy in (2, 1, 3)]
    steps = [-2, 2, -1, 1]
    late_step = [
        jnp.logical_and(level + step >= EARLY, level + step < levels) for step in steps
    ]
    late_steps = sum(ok.astype(jnp.int32) for ok in late_step)
    has_across = jnp.where(core == 1, pz < nz - 1, pz > 0)
    across = place(z=lax.rem(pz + nz + 2 * core - 1, nz))

    def greet_late(sem):
        for step, ok in zip(steps, late_step):

            @pl.when(ok)
            def _():
                greet(sem, along_yz(0, step % 8))

    flag_copy = pltpu.make_async_copy(flags, flag, load_sem.at[0])
    flag_copy.start()
    pltpu.make_async_copy(density, q.at[0], load_sem.at[1]).start()
    pltpu.make_async_copy(energy, q.at[1], load_sem.at[1]).start()
    pltpu.make_async_copy(displacement, disp, load_sem.at[1]).start()
    momentum_load = pltpu.make_async_copy(momentum, q.at[pl.ds(2, 3)], load_sem.at[2])
    momentum_load.start()

    barrier = pltpu.get_barrier_semaphore()

    @pl.when(late)
    def _():
        greet_late(barrier)

    for peer in stage_a + along_y:
        greet(barrier, peer)

    @pl.when(has_across)
    def _():
        greet(barrier, across)

    me_y = pz // 4
    in_column = [both(px == x, core == c) for _, x, _, c in ROOTS]
    skipped = sum(ok.astype(jnp.int32) for ok in in_column)
    at_root = [
        both(ok, both(level == t, me_y == y)) for ok, (t, _, y, _) in zip(in_column, ROOTS)
    ]
    root = functools.reduce(jnp.logical_or, at_root)

    @pl.when(root)
    def _():
        def greet_group(k, carry):
            t = 7 - k // 4
            z = 4 * lax.rem(k, 4) + 2 * lax.rem(t, 2)
            for x in range(4):
                for c in range(2):
                    greet(barrier, place(x=x, y=t // 2, z=z + c))
            return carry

        lax.fori_loop(0, 4 * (8 - EARLY), greet_group, 0)

    @pl.when(early)
    def _():
        for dz in range(1, 8):

            @pl.when(level + dz < levels)
            def _():
                for dy in range(4):
                    greet(barrier, along_yz(dy, dz))


    flag_copy.wait()
    wait_bytes(q, load_sem.at[1])

    def wait_pair(buffer, axis, sem):
        one = jnp.logical_or(first[axis], final[axis])

        @pl.when(one)
        def _():
            wait_bytes(buffer.at[0], sem)

        @pl.when(jnp.logical_not(one))
        def _():
            wait_bytes(buffer, sem)

    flag_open = [flag[i].astype(jnp.float32) for i in range(6)]
    first = [px == 0, py == 0, pz == 0]
    final = [px == nx - 1, py == ny - 1, pz == nz - 1]
    low_scale = [jnp.where(first[a], flag_open[2 * a], 1.0) for a in range(3)]
    gain = [jnp.where(first[a], flag_open[2 * a] * STEP, 0.0) for a in range(3)]
    loss = [jnp.where(final[a], flag_open[2 * a + 1] * -STEP, 0.0) for a in range(3)]

    rows = lax.broadcasted_iota(jnp.int32, (64, 128), 0)
    lanes = lax.broadcasted_iota(jnp.int32, (64, 128), 1)
    weight_y = jnp.where(rows == 0, gain[1], jnp.where(rows == 63, loss[1], 0.0))
    weight_z = jnp.where(lanes == 0, gain[2], jnp.where(lanes == 127, loss[2], 0.0))

    def fold(block):
        return jnp.sum(block.reshape(8, 8, 128), axis=0)

    def plane_sum(x, sums):
        weight = (
            1.0
            + weight_y * disp[1, x].astype(jnp.float32)
            + weight_z * disp[2, x].astype(jnp.float32)
        )
        return (sums[0] + fold(q[0, x] * weight), sums[1] + fold(q[1, x] * weight))

    weight_low = gain[0] * disp[0, 0].astype(jnp.float32)
    weight_high = loss[0] * disp[0, 7].astype(jnp.float32)
    sums = tuple(fold(q[f, 0] * weight_low + q[f, 7] * weight_high) for f in (0, 1))
    sums = lax.fori_loop(0, 8, plane_sum, sums)
    lane1 = lax.broadcasted_iota(jnp.int32, (1, 128), 1)

    def halves(low, high):
        low = jnp.sum(low, axis=0, keepdims=True)
        high = jnp.sum(high, axis=0, keepdims=True)
        return jnp.where(lane1 < 64, low + pltpu.roll(low, 64, 1), high + pltpu.roll(high, 64, 1))

    part[0] = halves(*sums)

    greeted = (
        len(stage_a)
        + len(along_y)
        + has_across.astype(jnp.int32)
        + jnp.where(early, 0, len(ROOTS))
        + jnp.where(early, 4 * level, 4 * EARLY + late_steps)
    )
    pl.semaphore_wait(barrier, greeted)

    def remote(src, dst, send_sem, recv_sem, peer):
        return pltpu.make_async_remote_copy(
            src_ref=src,
            dst_ref=dst,
            send_sem=send_sem,
            recv_sem=recv_sem,
            device_id=peer,
            device_id_type=MESH,
        )

    copies_a = [
        remote(part.at[0], slots_a.at[i], ts_sem.at[0], tr_sem.at[0], peer)
        for i, peer in enumerate(stage_a)
    ]
    slot = level * 4 + pz // 4
    arrival = tr_sem.at[jnp.where(early, 1, 2)]
    base_z = pz - 4 * me_y - 2 * zl
    places = [(t, y) for t in range(8) for y in (0, 1, 3, 2)]
    copies_b = [
        remote(
            part.at[1],
            slots_b.at[slot],
            ts_sem.at[1],
            arrival,
            place(y=t // 2, z=base_z + 4 * y + 2 * (t % 2)),
        )
        for t, y in places
    ]

    def send_b(wanted):
        for (t, y), copy in zip(places, copies_b):
            ok = wanted(t)
            if ok is not None:
                other = jnp.logical_or(level != t, me_y != y)
                pl.when(jnp.logical_and(ok, other))(copy.start)
    index = (level - EARLY) * 32 + me_y * 8 + px * 2 + core
    to_roots = [
        remote(
            part.at[0],
            slots_d.at[index],
            ts_sem.at[1],
            tr_sem.at[2],
            place(x=x, y=t // 2, z=4 * y + 2 * (t % 2) + c),
        )
        for t, x, y, c in ROOTS
    ]

    @pl.when(late)
    def _():
        to_roots[0].start()

    for copy in copies_a:
        copy.start()

    @pl.when(late)
    def _():
        for copy in to_roots[1:]:
            copy.start()
        greet_late(round_sem.at[0])
        for peer in along_y:
            greet(round_sem.at[0], peer)

    for back_step in (1, 2):

        @pl.when(jnp.logical_and(level - back_step >= 0, level - back_step < EARLY))
        def _():
            greet(round_sem.at[0], along_yz(0, 8 - back_step))

    @pl.when(early)
    def _():
        for target in range(EARLY - 1):

            @pl.when(target < level)
            def _():
                for dy in range(4):
                    greet(round_sem.at[2], along_yz(dy, lax.rem(levels + target - level, levels)))

    @pl.when(jnp.logical_not(early))
    def _():
        greet(round_sem.at[1], along_yz(0, lax.rem(levels + EARLY - 1 - level, levels)))

    momentum_load.wait()
    x_next = place(x=lax.rem(px + 1, nx))
    x_prev = place(x=lax.rem(px + nx - 1, nx))
    face_copy = remote(disp.at[0, 0], xface, xs_sem.at[1], xr_sem.at[2], x_prev)
    up_copies = [
        remote(q.at[f, pl.ds(6, 2)], xhalo.at[f, 0], xs_sem.at[0], xr_sem.at[f // 3], x_next) for f in range(5)
    ]
    down_copies = [
        remote(q.at[f, pl.ds(0, 2)], xhalo.at[f, 1], xs_sem.at[0], xr_sem.at[f // 3], x_prev)
        for f in range(5)
    ]

    @pl.when(jnp.logical_not(first[0]))
    def _():
        face_copy.start()

    for f in range(5):

        @pl.when(jnp.logical_not(final[0]))
        def _():
            up_copies[f].start()

        @pl.when(jnp.logical_not(first[0]))
        def _():
            down_copies[f].start()

    for f in range(5):
        for r in range(2):
            yup[2 * f + r] = q[f, :, 62 + r, :]
            ydown[2 * f + r] = q[f, :, r, :]
    yup[10] = jnp.zeros((8, 128), jnp.float32)
    ydown[10] = disp[1, :, 0, :].astype(jnp.float32) * STEP

    y_up = remote(yup, yin.at[0], ys_sem.at[0], yr_sem.at[0], place(y=lax.rem(py + 1, ny)))
    y_down = remote(ydown, yin.at[1], ys_sem.at[0], yr_sem.at[0], place(y=lax.rem(py + ny - 1, ny)))

    @pl.when(jnp.logical_not(first[1]))
    def _():
        y_down.start()

    @pl.when(jnp.logical_not(jnp.logical_or(final[1], early)))
    def _():
        y_up.start()

    lane8 = lax.broadcasted_iota(jnp.int32, (8, 128), 1)
    slot_of = lane8 // 4
    place4 = lane8 % 4

    def pack(source, base, half):
        packed = jnp.zeros((8, 128), jnp.float32)
        for xx in range(4):
            plane = source[base, half * 4 + xx].astype(jnp.float32)
            for t in range(8):
                k = xx * 8 + t
                moved = pltpu.roll(plane[8 * t : 8 * t + 8], (4 * k + 2) % 128, 1)
                packed = jnp.where(slot_of == k, moved, packed)
        return packed

    for f in range(5):
        for half in range(2):
            zpack[2 * f + half] = pack(q, f, half)
    for half in range(2):
        zpack[10 + half] = pack(disp, 2, half) * STEP

    z_up = remote(zpack, zin.at[0], zs_sem.at[0], zr_sem.at[0], place(z=lax.rem(pz + 1, nz)))
    z_down = remote(zpack, zin.at[1], zs_sem.at[0], zr_sem.at[0], place(z=lax.rem(pz + nz - 1, nz)))

    @pl.when(jnp.logical_not(final[2]))
    def _():
        z_up.start()

    @pl.when(jnp.logical_not(first[2]))
    def _():
        z_down.start()

    scale_y = jnp.where(
        jnp.logical_or(rows < 2, rows == 63), 0.0, STEP
    )
    scale_z = jnp.where(lanes == 0, STEP * low_scale[2], STEP)

    def planes(x, carry):
        vy = disp[1, x].astype(jnp.float32) * scale_y
        gy = half_weight(vy)
        up_y = vy > 0
        vz = disp[2, x].astype(jnp.float32) * scale_z
        right = jnp.where(lanes == 127, 0.0, jnp.maximum(ahead(vz), 0.0))
        right_w = jnp.where(lanes == 0, 0.0, 0.5 * right * (1.0 - right))
        left = jnp.minimum(vz, 0.0)
        left_w = jnp.where(
            jnp.logical_or(lanes == 0, lanes == 127), 0.0, -0.5 * left * (1.0 + left)
        )
        for f in range(5):
            value = q[f, x]
            below = back(value)
            above = ahead(value)
            slope = minmod(value - below, above - value)
            out_right = right * value + right_w * slope
            out_left = left * value + left_w * slope
            change_z = (back(out_right) - out_right) + (out_left - ahead(out_left))

            below = pltpu.roll(value, 1, 0)
            diff = value - below
            slope = minmod(diff, pltpu.roll(diff, 63, 0))
            flux = vy * jnp.where(up_y, below, value) + gy * jnp.where(
                up_y, pltpu.roll(slope, 1, 0), slope
            )
            acc[f, x] = (value + (flux - pltpu.roll(flux, 63, 0))) + change_z
        return carry

    lax.fori_loop(0, 2, planes, 0)

    @pl.when(late)
    def _():
        pl.semaphore_wait(round_sem.at[0], len(along_y) + late_steps)
        greet_late(round_sem.at[1])
        for peer in along_y:
            greet(round_sem.at[1], peer)

    lax.fori_loop(2, 3, planes, 0)

    wait_bytes(slots_a, tr_sem.at[0])
    group = part[0] + jnp.sum(slots_a[...], axis=0)
    part[1] = group
    slots_b[slot] = group

    @pl.when(late)
    def _():
        for (t, y), copy in zip(places, copies_b):
            skip = [ok for ok, spot in zip(in_column, ROOTS) if spot[0] == t and spot[2] == y]
            if skip:
                pl.when(jnp.logical_not(functools.reduce(jnp.logical_or, skip)))(copy.start)
            elif t < EARLY:
                copy.start()
        send_b(lambda t: jnp.abs(level - t) < 3 if t >= EARLY else None)

    @pl.when(early)
    def _():
        send_b(lambda t: level >= t if t < EARLY else None)

    lax.fori_loop(3, 5, planes, 0)

    @pl.when(early)
    def _():
        pl.semaphore_wait(round_sem.at[0], 2)
        y_up.start()

    @pl.when(late)
    def _():
        pl.semaphore_wait(round_sem.at[1], len(along_y) + late_steps)
        send_b(lambda t: jnp.abs(level - t) > 2 if t >= EARLY else None)

    lax.fori_loop(5, 8, planes, 0)

    @pl.when(level < EARLY - 1)
    def _():
        pl.semaphore_wait(round_sem.at[2], 4 * (EARLY - 1 - level))
        send_b(lambda t: level < t if t < EARLY else None)

    wait_pair(yin, 1, yr_sem.at[0])

    v0, v1, v63 = [disp[1, :, r, :].astype(jnp.float32) * STEP for r in (0, 1, 63)]
    v64 = jnp.where(final[1], v63 * flag_open[3], yin[1, 10])
    v0 = v0 * low_scale[1]

    def flux_row(v, behind, at, slope_behind, slope_at):
        return v * jnp.where(v > 0, behind, at) + half_weight(v) * jnp.where(
            v > 0, slope_behind, slope_at
        )

    for f in range(5):
        q0, q1, q2, q61, q62, q63 = [q[f, :, r, :] for r in (0, 1, 2, 61, 62, 63)]
        lo1 = jnp.where(first[1], q0, yin[0, 2 * f + 1])
        lo2 = jnp.where(first[1], q0, yin[0, 2 * f])
        hi0 = jnp.where(final[1], q63, yin[1, 2 * f])
        hi1 = jnp.where(final[1], q63, yin[1, 2 * f + 1])
        s0 = minmod(q0 - lo1, q1 - q0)
        s63 = minmod(q63 - q62, hi0 - q63)
        flux_0 = flux_row(v0, lo1, q0, minmod(lo1 - lo2, q0 - lo1), s0)
        flux_1 = flux_row(v1, q0, q1, s0, minmod(q1 - q0, q2 - q1))
        flux_63 = flux_row(v63, q62, q63, minmod(q62 - q61, q63 - q62), s63)
        flux_64 = flux_row(v64, q63, hi0, s63, minmod(hi0 - q63, hi1 - hi0))
        acc[f, :, 0, :] += flux_0 - flux_1
        acc[f, :, 1, :] += flux_1
        acc[f, :, 62, :] -= flux_63
        acc[f, :, 63, :] += flux_63 - flux_64

    wait_pair(zin, 2, zr_sem.at[0])

    def face(four, v):
        behind = back(four)
        diff = four - behind
        slope = minmod(diff, ahead(diff))
        flux = v * jnp.where(v > 0, behind, four) + half_weight(v) * jnp.where(
            v > 0, back(slope), slope
        )
        return slope, flux

    for half in range(2):
        own_v = zpack[10 + half]
        v_low = jnp.where(place4 == 2, own_v * low_scale[2], own_v)
        v_high = jnp.where(final[2], back(own_v) * flag_open[5], zin[1, 10 + half])
        left = jnp.minimum(v_low, 0.0)
        left_w = -0.5 * left * (1.0 + left)
        right = jnp.maximum(ahead(own_v), 0.0)
        right_w = 0.5 * right * (1.0 - right)
        for f in range(5):
            j = 2 * f + half
            own = zpack[j]
            ghost_low = jnp.where(place4 == 0, pltpu.roll(own, 126, 1), ahead(own))
            ghost_high = jnp.where(place4 == 2, back(own), pltpu.roll(own, 2, 1))
            low = jnp.where(place4 < 2, jnp.where(first[2], ghost_low, zin[0, j]), own)
            high = jnp.where(place4 < 2, own, jnp.where(final[2], ghost_high, zin[1, j]))
            slope_low, flux_low = face(low, v_low)
            slope_high, flux_high = face(high, v_high)
            by_left = left_w * jnp.where(place4 == 1, slope_high, slope_low)
            by_right = right_w * slope_low
            entering = jnp.where(v_low > 0, flux_low, 0.0)
            zcorr[j] = jnp.where(
                place4 == 0,
                -ahead(by_left),
                jnp.where(
                    place4 == 1,
                    by_left - ahead(flux_high) + ahead(left * own),
                    jnp.where(place4 == 2, entering + by_left - by_right, back(by_right)),
                ),
            )

    last_early = level == EARLY - 1
    copies_c = [
        remote(part.at[2], slots_b.at[0], ts_sem.at[1], tr_sem.at[1], along_yz(0, dz))
        for dz in range(1, 6)
    ]

    @pl.when(last_early)
    def _():
        wait_bytes(slots_b.at[pl.ds(0, 4 * EARLY - 1)], tr_sem.at[1])
        part[2] = jnp.sum(slots_b[: 4 * EARLY], axis=0)
        pl.semaphore_wait(round_sem.at[1], levels - EARLY)
        for copy in copies_c:
            copy.start()

    @pl.when(jnp.logical_not(final[0]))
    def _():
        face_copy.wait_recv()

    for i in range(9):
        if i == 0:
            v = disp[0, 0].astype(jnp.float32) * (STEP * low_scale[0])
        elif i < 8:
            v = disp[0, i].astype(jnp.float32) * STEP
        else:
            v_last = disp[0, 7].astype(jnp.float32) * (STEP * flag_open[1])
            v = jnp.where(final[0], v_last, xface[...].astype(jnp.float32) * STEP)
        vx[i] = v
        gx_w[i] = half_weight(v)

    inner = jnp.logical_not(jnp.logical_or(first[0], final[0]))
    edge_lanes = jnp.logical_or(lane8 < 2, lane8 > 125)
    for f in range(5):

        if f in (0, 3):
            group = pl.ds(f, 3 - f // 3)

            @pl.when(inner)
            def _():
                wait_bytes(xhalo.at[group], xr_sem.at[f // 3])

            @pl.when(jnp.logical_not(inner))
            def _():
                wait_bytes(xhalo.at[group, 0], xr_sem.at[f // 3])

        def tile(t, carry):
            part_rows = pl.ds(pl.multiple_of(t * 8, 8), 8)
            own = [q[f, i, part_rows] for i in range(8)]
            cell = (
                [jnp.where(first[0], own[0], xhalo[f, 0, r, part_rows]) for r in range(2)]
                + own
                + [jnp.where(final[0], own[7], xhalo[f, 1, r, part_rows]) for r in range(2)]
            )
            diff = [cell[i + 1] - cell[i] for i in range(11)]
            slope = [minmod(diff[i], diff[i + 1]) for i in range(10)]
            flux = []
            for i in range(9):
                v = vx[i, part_rows]
                g = gx_w[i, part_rows]
                flux.append(
                    v * jnp.where(v > 0, cell[i + 1], cell[i + 2])
                    + g * jnp.where(v > 0, slope[i], slope[i + 1])
                )
            for i in range(8):
                move = lax.rem(254 - 4 * ((i % 4) * 8 + t), 128)
                corr = pltpu.roll(zcorr[2 * f + i // 4], move, 1)
                corr = jnp.where(edge_lanes, corr, 0.0)
                acc[f, i, part_rows] += (flux[i] - flux[i + 1]) + corr
            return carry

        lax.fori_loop(0, 8, tile, 0)

    wait_bytes(slots_a, ts_sem.at[0])

    @pl.when(jnp.logical_not(first[0]))
    def _():
        face_copy.wait_send()

    wait_pair(yin, 1, ys_sem.at[0])
    wait_pair(zin, 2, zs_sem.at[0])

    @pl.when(inner)
    def _():
        wait_bytes(xhalo, xs_sem.at[0])

    @pl.when(jnp.logical_not(inner))
    def _():
        wait_bytes(xhalo.at[:, 0], xs_sem.at[0])

    not_root = jnp.logical_not(root)

    def wait_rows(when, count, sem):
        @pl.when(when)
        def _():
            wait_bytes(slots_d.at[pl.ds(0, count)], sem)

    wait_rows(level < EARLY - 1, 4 * EARLY - 1, ts_sem.at[1])
    wait_rows(last_early, 4 * EARLY + 4, ts_sem.at[1])
    columns = [(x, c) for _, x, _, c in ROOTS]
    for skip in sorted({columns.count((x, c)) for x in range(4) for c in range(2)}):
        wait_rows(both(late, skipped == skip), 31 - skip + len(ROOTS), ts_sem.at[1])
    wait_rows(level < EARLY - 1, 4 * EARLY - 1, tr_sem.at[1])
    wait_rows(both(early, not_root), 4 * (8 - EARLY), tr_sem.at[2])
    wait_rows(late, 1, tr_sem.at[1])
    wait_rows(late, 4 * (8 - EARLY) - 1, tr_sem.at[2])
    others = jnp.sum(slots_b[1 : 4 * EARLY], axis=0)
    near_sum = slots_b[0] + jnp.where(early, others, 0.0)

    @pl.when(root)
    def _():
        wait_bytes(slots_d, tr_sem.at[2])
        grand[...] = near_sum + row_sum(slots_d, 0, 160)

    @pl.when(not_root)
    def _():
        grand[...] = near_sum + row_sum(slots_b, 4 * EARLY, 4 * (8 - EARLY))


def write_out(cells, acc, grand, new_density, new_momentum, new_energy, totals, pair, sem):
    stores = [
        pltpu.make_async_copy(acc.at[0], new_density, sem.at[0]),
        pltpu.make_async_copy(acc.at[1], new_energy, sem.at[0]),
    ] + [pltpu.make_async_copy(acc.at[2 + c], new_momentum.at[c], sem.at[0]) for c in range(3)]
    for store in stores:
        store.start()
    lane1 = lax.broadcasted_iota(jnp.int32, (1, 128), 1)
    both = grand[...]
    pair[0] = jnp.sum(jnp.where(lane1 < 64, both, 0.0)) / cells
    pair[1] = jnp.sum(jnp.where(lane1 < 64, 0.0, both)) / cells
    last = pltpu.make_async_copy(pair, totals, sem.at[1])
    last.start()
    pltpu.make_async_copy(acc, acc, sem.at[0]).wait()
    last.wait()


def shards(cells, density, momentum, energy, displacement, flags):
    f32, i32 = jnp.float32, jnp.int32
    anywhere = pl.BlockSpec(memory_space=pltpu.HBM)
    local = pl.BlockSpec(memory_space=pltpu.VMEM)
    inputs = [
        pltpu.with_memory_space_constraint(a, pltpu.HBM)
        for a in (density, momentum, energy, displacement, flags)
    ]
    acc, grand = pl.pallas_call(
        kernel,
        out_shape=(
            jax.ShapeDtypeStruct((5, 8, 64, 128), f32),
            jax.ShapeDtypeStruct((1, 128), f32),
        ),
        in_specs=[anywhere] * 5,
        out_specs=(local, local),
        scratch_shapes=[
            pltpu.VMEM((5, 8, 64, 128), f32),
            pltpu.VMEM((3, 8, 64, 128), i32),
            pltpu.SMEM((6,), i32),
            pltpu.VMEM((9, 64, 128), f32),
            pltpu.VMEM((9, 64, 128), f32),
            pltpu.VMEM((5, 2, 2, 64, 128), f32),
            pltpu.VMEM((64, 128), i32),
            pltpu.VMEM((11, 8, 128), f32),
            pltpu.VMEM((11, 8, 128), f32),
            pltpu.VMEM((2, 11, 8, 128), f32),
            pltpu.VMEM((12, 8, 128), f32),
            pltpu.VMEM((2, 12, 8, 128), f32),
            pltpu.VMEM((10, 8, 128), f32),
            pltpu.VMEM((3, 1, 128), f32),
            pltpu.VMEM((7, 1, 128), f32),
            pltpu.VMEM((32, 1, 128), f32),
            pltpu.VMEM((160, 1, 128), f32),
            pltpu.SemaphoreType.DMA((3,)),
            pltpu.SemaphoreType.DMA((2,)),
            pltpu.SemaphoreType.DMA((3,)),
            pltpu.SemaphoreType.DMA((1,)),
            pltpu.SemaphoreType.DMA((1,)),
            pltpu.SemaphoreType.DMA((1,)),
            pltpu.SemaphoreType.DMA((1,)),
            pltpu.SemaphoreType.DMA((2,)),
            pltpu.SemaphoreType.DMA((3,)),
            pltpu.SemaphoreType.REGULAR((3,)),
        ],
        compiler_params=pltpu.CompilerParams(
            collective_id=0, has_side_effects=True, vmem_limit_bytes=16 * 2**20
        ),
        name="remap",
    )(*inputs)
    return pl.pallas_call(
        functools.partial(write_out, cells),
        out_shape=(
            jax.ShapeDtypeStruct(density.shape, f32),
            jax.ShapeDtypeStruct(momentum.shape, f32),
            jax.ShapeDtypeStruct(energy.shape, f32),
            jax.ShapeDtypeStruct((2,), f32),
        ),
        in_specs=[local, local],
        out_specs=[anywhere] * 4,
        scratch_shapes=[pltpu.SMEM((2,), f32), pltpu.SemaphoreType.DMA((2,))],
        compiler_params=pltpu.CompilerParams(vmem_limit_bytes=4 * 2**20),
        name="write_out",
    )(acc, grand)


def solution(mesh):
    cells = float(mesh.shape["gx"] * mesh.shape["gy"] * mesh.shape["gz"] * 8 * 64 * 128)
    block = P("gx", "gy", "gz")
    three = P(None, "gx", "gy", "gz")
    return jax.shard_map(
        functools.partial(shards, cells),
        mesh=mesh,
        in_specs=(block, three, block, three, P()),
        out_specs=(block, three, block, P()),
        check_vma=False,
    )
```

```python
import functools

import jax
import jax.numpy as jnp
from jax import lax
from jax.experimental import pallas as pl
from jax.experimental.pallas import tpu as pltpu
from jax.sharding import PartitionSpec as P

MESH = pl.DeviceIdType.MESH
STEP = 1.0 / 256.0
EARLY = 3
ROOTS = (
    (0, 0, 0, 1),
    (0, 1, 0, 0),
    (0, 0, 1, 0),
    (0, 2, 0, 0),
    (0, 3, 0, 0),
    (0, 0, 2, 0),
    (0, 0, 3, 0),
    (0, 0, 0, 0),
    (0, 1, 0, 1),
    (0, 2, 0, 1),
    (0, 1, 1, 0),
    (0, 0, 1, 1),
    (1, 0, 0, 0),
    (1, 0, 0, 1),
    (1, 1, 0, 0),
    (1, 0, 1, 0),
)


def minmod(left_diff, right_diff):
    least = jnp.minimum(left_diff, right_diff)
    most = jnp.maximum(left_diff, right_diff)
    return jnp.maximum(least, jnp.minimum(most, 0.0))


def half_weight(v):
    size = jnp.abs(v)
    return 0.5 * size * (1.0 - size)


def row_sum(rows, start, count):
    sums = [rows[start + i] for i in range(10)]
    for i in range(10, count):
        sums[i % 10] = sums[i % 10] + rows[start + i]
    while len(sums) > 1:
        paired = [sums[i] + sums[i + 1] for i in range(0, len(sums) - 1, 2)]
        sums = paired + sums[len(paired) * 2 :]
    return sums[0]


def back(block):
    return pltpu.roll(block, 1, 1)


def ahead(block):
    return pltpu.roll(block, 127, 1)


def kernel(
    density,
    momentum,
    energy,
    displacement,
    flags,
    acc,
    grand,
    q,
    disp,
    flag,
    vx,
    gx_w,
    xhalo,
    xface,
    yup,
    ydown,
    yin,
    zpack,
    zin,
    zcorr,
    part,
    slots_a,
    slots_b,
    slots_d,
    load_sem,
    xs_sem,
    xr_sem,
    ys_sem,
    yr_sem,
    zs_sem,
    zr_sem,
    ts_sem,
    tr_sem,
    round_sem,
):
    px, py, pz = lax.axis_index("gx"), lax.axis_index("gy"), lax.axis_index("gz")
    nx, ny, nz = lax.axis_size("gx"), lax.axis_size("gy"), lax.axis_size("gz")
    core = pz % 2
    zl = (pz // 2) % 2
    def wait_bytes(of, sem):
        pltpu.make_async_copy(of, of, sem).wait()

    def place(x=None, y=None, z=None):
        target = {}
        if x is not None:
            target["gx"] = x
        if y is not None:
            target["gy"] = y
        if z is not None:
            target["gz"] = z
        return target

    level = py * 2 + zl
    levels = 2 * ny
    early = level < EARLY
    both = jnp.logical_and
    late = jnp.logical_not(early)

    def along_yz(dy, dz):
        chip = lax.rem(level + dz, levels)
        return place(y=chip // 2, z=lax.rem(pz + 4 * dy, nz) + 2 * (chip % 2 - zl))

    def greet(sem, peer):
        pl.semaphore_signal(sem, inc=1, device_id=peer, device_id_type=MESH)

    stage_a = [
        place(x=lax.rem(px + dx, nx), z=pz + dc * (1 - 2 * core))
        for dx in (2, 1, 3, 0)
        for dc in range(2)
        if dx or dc
    ]
    along_y = [along_yz(dy, 0) for dy in (2, 1, 3)]
    steps = [-2, 2, -1, 1]
    late_step = [
        jnp.logical_and(level + step >= EARLY, level + step < levels) for step in steps
    ]
    late_steps = sum(ok.astype(jnp.int32) for ok in late_step)
    has_across = jnp.where(core == 1, pz < nz - 1, pz > 0)
    across = place(z=lax.rem(pz + nz + 2 * core - 1, nz))

    def greet_late(sem):
        for step, ok in zip(steps, late_step):

            @pl.when(ok)
            def _():
                greet(sem, along_yz(0, step % 8))

    flag_copy = pltpu.make_async_copy(flags, flag, load_sem.at[0])
    flag_copy.start()
    pltpu.make_async_copy(density, q.at[0], load_sem.at[1]).start()
    pltpu.make_async_copy(energy, q.at[1], load_sem.at[1]).start()
    for a in range(3):
        pltpu.make_async_copy(displacement.at[a], disp.at[a], load_sem.at[1]).start()
    momentum_load = pltpu.make_async_copy(momentum, q.at[pl.ds(2, 3)], load_sem.at[2])
    momentum_load.start()

    barrier = pltpu.get_barrier_semaphore()

    @pl.when(late)
    def _():
        greet_late(barrier)

    for peer in stage_a + along_y:
        greet(barrier, peer)

    @pl.when(has_across)
    def _():
        greet(barrier, across)

    me_y = pz // 4
    in_column = [both(px == x, core == c) for _, x, _, c in ROOTS]
    skipped = sum(ok.astype(jnp.int32) for ok in in_column)
    at_root = [
        both(ok, both(level == t, me_y == y)) for ok, (t, _, y, _) in zip(in_column, ROOTS)
    ]
    root = functools.reduce(jnp.logical_or, at_root)

    @pl.when(root)
    def _():
        def greet_group(k, carry):
            t = 7 - k // 4
            z = 4 * lax.rem(k, 4) + 2 * lax.rem(t, 2)
            for x in range(4):
                for c in range(2):
                    greet(barrier, place(x=x, y=t // 2, z=z + c))
            return carry

        lax.fori_loop(0, 4 * (8 - EARLY), greet_group, 0)

    @pl.when(early)
    def _():
        for dz in range(1, 8):

            @pl.when(level + dz < levels)
            def _():
                for dy in range(4):
                    greet(barrier, along_yz(dy, dz))


    flag_copy.wait()
    wait_bytes(q, load_sem.at[1])

    def wait_pair(buffer, axis, sem):
        one = jnp.logical_or(first[axis], final[axis])

        @pl.when(one)
        def _():
            wait_bytes(buffer.at[0], sem)

        @pl.when(jnp.logical_not(one))
        def _():
            wait_bytes(buffer, sem)

    flag_open = [flag[i].astype(jnp.float32) for i in range(6)]
    first = [px == 0, py == 0, pz == 0]
    final = [px == nx - 1, py == ny - 1, pz == nz - 1]
    low_scale = [jnp.where(first[a], flag_open[2 * a], 1.0) for a in range(3)]
    gain = [jnp.where(first[a], flag_open[2 * a] * STEP, 0.0) for a in range(3)]
    loss = [jnp.where(final[a], flag_open[2 * a + 1] * -STEP, 0.0) for a in range(3)]

    rows = lax.broadcasted_iota(jnp.int32, (64, 128), 0)
    lanes = lax.broadcasted_iota(jnp.int32, (64, 128), 1)
    weight_y = jnp.where(rows == 0, gain[1], jnp.where(rows == 63, loss[1], 0.0))
    weight_z = jnp.where(lanes == 0, gain[2], jnp.where(lanes == 127, loss[2], 0.0))

    def fold(block):
        return jnp.sum(block.reshape(8, 8, 128), axis=0)

    def plane_sum(x, sums):
        weight = (
            1.0
            + weight_y * disp[1, x].astype(jnp.float32)
            + weight_z * disp[2, x].astype(jnp.float32)
        )
        return (sums[0] + fold(q[0, x] * weight), sums[1] + fold(q[1, x] * weight))

    weight_low = gain[0] * disp[0, 0].astype(jnp.float32)
    weight_high = loss[0] * disp[0, 7].astype(jnp.float32)
    sums = tuple(fold(q[f, 0] * weight_low + q[f, 7] * weight_high) for f in (0, 1))
    sums = lax.fori_loop(0, 8, plane_sum, sums)
    lane1 = lax.broadcasted_iota(jnp.int32, (1, 128), 1)

    def halves(low, high):
        low = jnp.sum(low, axis=0, keepdims=True)
        high = jnp.sum(high, axis=0, keepdims=True)
        return jnp.where(lane1 < 64, low + pltpu.roll(low, 64, 1), high + pltpu.roll(high, 64, 1))

    part[0] = halves(*sums)

    greeted = (
        len(stage_a)
        + len(along_y)
        + has_across.astype(jnp.int32)
        + jnp.where(early, 0, len(ROOTS))
        + jnp.where(early, 4 * level, 4 * EARLY + late_steps)
    )
    pl.semaphore_wait(barrier, greeted)

    def remote(src, dst, send_sem, recv_sem, peer):
        return pltpu.make_async_remote_copy(
            src_ref=src,
            dst_ref=dst,
            send_sem=send_sem,
            recv_sem=recv_sem,
            device_id=peer,
            device_id_type=MESH,
        )

    copies_a = [
        remote(part.at[0], slots_a.at[i], ts_sem.at[0], tr_sem.at[0], peer)
        for i, peer in enumerate(stage_a)
    ]
    slot = level * 4 + pz // 4
    arrival = tr_sem.at[jnp.where(early, 1, 2)]
    base_z = pz - 4 * me_y - 2 * zl
    places = [(t, y) for t in range(8) for y in (0, 1, 3, 2)]
    copies_b = [
        remote(
            part.at[1],
            slots_b.at[slot],
            ts_sem.at[1],
            arrival,
            place(y=t // 2, z=base_z + 4 * y + 2 * (t % 2)),
        )
        for t, y in places
    ]

    def send_b(wanted):
        for (t, y), copy in zip(places, copies_b):
            ok = wanted(t)
            if ok is not None:
                other = jnp.logical_or(level != t, me_y != y)
                pl.when(jnp.logical_and(ok, other))(copy.start)
    index = (level - EARLY) * 32 + me_y * 8 + px * 2 + core
    to_roots = [
        remote(
            part.at[0],
            slots_d.at[index],
            ts_sem.at[1],
            tr_sem.at[2],
            place(x=x, y=t // 2, z=4 * y + 2 * (t % 2) + c),
        )
        for t, x, y, c in ROOTS
    ]

    @pl.when(late)
    def _():
        to_roots[0].start()

    for copy in copies_a:
        copy.start()

    @pl.when(late)
    def _():
        for copy in to_roots[1:]:
            copy.start()
        greet_late(round_sem.at[0])
        for peer in along_y:
            greet(round_sem.at[0], peer)

    for back_step in (1, 2):

        @pl.when(jnp.logical_and(level - back_step >= 0, level - back_step < EARLY))
        def _():
            greet(round_sem.at[0], along_yz(0, 8 - back_step))

    @pl.when(early)
    def _():
        for target in range(EARLY - 1):

            @pl.when(target < level)
            def _():
                for dy in range(4):
                    greet(round_sem.at[2], along_yz(dy, lax.rem(levels + target - level, levels)))

    @pl.when(jnp.logical_not(early))
    def _():
        greet(round_sem.at[1], along_yz(0, lax.rem(levels + EARLY - 1 - level, levels)))

    momentum_load.wait()
    x_next = place(x=lax.rem(px + 1, nx))
    x_prev = place(x=lax.rem(px + nx - 1, nx))
    face_copy = remote(disp.at[0, 0], xface, xs_sem.at[1], xr_sem.at[2], x_prev)
    up_copies = [
        remote(q.at[f, pl.ds(6, 2)], xhalo.at[f, 0], xs_sem.at[0], xr_sem.at[f // 3], x_next) for f in range(5)
    ]
    down_copies = [
        remote(q.at[f, pl.ds(0, 2)], xhalo.at[f, 1], xs_sem.at[0], xr_sem.at[f // 3], x_prev)
        for f in range(5)
    ]

    @pl.when(jnp.logical_not(first[0]))
    def _():
        face_copy.start()

    for f in range(5):

        @pl.when(jnp.logical_not(final[0]))
        def _():
            up_copies[f].start()

        @pl.when(jnp.logical_not(first[0]))
        def _():
            down_copies[f].start()

    for f in range(5):
        for r in range(2):
            yup[2 * f + r] = q[f, :, 62 + r, :]
            ydown[2 * f + r] = q[f, :, r, :]
    yup[10] = jnp.zeros((8, 128), jnp.float32)
    ydown[10] = disp[1, :, 0, :].astype(jnp.float32) * STEP

    y_up = remote(yup, yin.at[0], ys_sem.at[0], yr_sem.at[0], place(y=lax.rem(py + 1, ny)))
    y_down = remote(ydown, yin.at[1], ys_sem.at[0], yr_sem.at[0], place(y=lax.rem(py + ny - 1, ny)))

    @pl.when(jnp.logical_not(first[1]))
    def _():
        y_down.start()

    @pl.when(jnp.logical_not(jnp.logical_or(final[1], early)))
    def _():
        y_up.start()

    lane8 = lax.broadcasted_iota(jnp.int32, (8, 128), 1)
    slot_of = lane8 // 4
    place4 = lane8 % 4

    def pack(source, base, half):
        packed = jnp.zeros((8, 128), jnp.float32)
        for xx in range(4):
            plane = source[base, half * 4 + xx].astype(jnp.float32)
            for t in range(8):
                k = xx * 8 + t
                moved = pltpu.roll(plane[8 * t : 8 * t + 8], (4 * k + 2) % 128, 1)
                packed = jnp.where(slot_of == k, moved, packed)
        return packed

    for f in range(5):
        for half in range(2):
            zpack[2 * f + half] = pack(q, f, half)
    for half in range(2):
        zpack[10 + half] = pack(disp, 2, half) * STEP

    z_up = remote(zpack, zin.at[0], zs_sem.at[0], zr_sem.at[0], place(z=lax.rem(pz + 1, nz)))
    z_down = remote(zpack, zin.at[1], zs_sem.at[0], zr_sem.at[0], place(z=lax.rem(pz + nz - 1, nz)))

    @pl.when(jnp.logical_not(final[2]))
    def _():
        z_up.start()

    @pl.when(jnp.logical_not(first[2]))
    def _():
        z_down.start()

    scale_y = jnp.where(
        jnp.logical_or(rows < 2, rows == 63), 0.0, STEP
    )
    scale_z = jnp.where(lanes == 0, STEP * low_scale[2], STEP)

    def planes(x, carry):
        vy = disp[1, x].astype(jnp.float32) * scale_y
        gy = half_weight(vy)
        up_y = vy > 0
        vz = disp[2, x].astype(jnp.float32) * scale_z
        right = jnp.where(lanes == 127, 0.0, jnp.maximum(ahead(vz), 0.0))
        right_w = jnp.where(lanes == 0, 0.0, 0.5 * right * (1.0 - right))
        left = jnp.minimum(vz, 0.0)
        left_w = jnp.where(
            jnp.logical_or(lanes == 0, lanes == 127), 0.0, -0.5 * left * (1.0 + left)
        )
        for f in range(5):
            value = q[f, x]
            below = back(value)
            above = ahead(value)
            slope = minmod(value - below, above - value)
            out_right = right * value + right_w * slope
            out_left = left * value + left_w * slope
            change_z = (back(out_right) - out_right) + (out_left - ahead(out_left))

            below = pltpu.roll(value, 1, 0)
            diff = value - below
            slope = minmod(diff, pltpu.roll(diff, 63, 0))
            flux = vy * jnp.where(up_y, below, value) + gy * jnp.where(
                up_y, pltpu.roll(slope, 1, 0), slope
            )
            acc[f, x] = (value + (flux - pltpu.roll(flux, 63, 0))) + change_z
        return carry

    lax.fori_loop(0, 2, planes, 0)

    @pl.when(late)
    def _():
        pl.semaphore_wait(round_sem.at[0], len(along_y) + late_steps)
        greet_late(round_sem.at[1])
        for peer in along_y:
            greet(round_sem.at[1], peer)

    lax.fori_loop(2, 3, planes, 0)

    wait_bytes(slots_a, tr_sem.at[0])
    group = part[0] + jnp.sum(slots_a[...], axis=0)
    part[1] = group
    slots_b[slot] = group

    @pl.when(late)
    def _():
        for (t, y), copy in zip(places, copies_b):
            skip = [ok for ok, spot in zip(in_column, ROOTS) if spot[0] == t and spot[2] == y]
            if skip:
                pl.when(jnp.logical_not(functools.reduce(jnp.logical_or, skip)))(copy.start)
            elif t < EARLY:
                copy.start()
        send_b(lambda t: jnp.abs(level - t) < 3 if t >= EARLY else None)

    @pl.when(early)
    def _():
        send_b(lambda t: level >= t if t < EARLY else None)

    lax.fori_loop(3, 5, planes, 0)

    @pl.when(early)
    def _():
        pl.semaphore_wait(round_sem.at[0], 2)
        y_up.start()

    @pl.when(late)
    def _():
        pl.semaphore_wait(round_sem.at[1], len(along_y) + late_steps)
        send_b(lambda t: jnp.abs(level - t) > 2 if t >= EARLY else None)

    lax.fori_loop(5, 8, planes, 0)

    @pl.when(level < EARLY - 1)
    def _():
        pl.semaphore_wait(round_sem.at[2], 4 * (EARLY - 1 - level))
        send_b(lambda t: level < t if t < EARLY else None)

    wait_pair(yin, 1, yr_sem.at[0])

    v0, v1, v63 = [disp[1, :, r, :].astype(jnp.float32) * STEP for r in (0, 1, 63)]
    v64 = jnp.where(final[1], v63 * flag_open[3], yin[1, 10])
    v0 = v0 * low_scale[1]

    def flux_row(v, behind, at, slope_behind, slope_at):
        return v * jnp.where(v > 0, behind, at) + half_weight(v) * jnp.where(
            v > 0, slope_behind, slope_at
        )

    for f in range(5):
        q0, q1, q2, q61, q62, q63 = [q[f, :, r, :] for r in (0, 1, 2, 61, 62, 63)]
        lo1 = jnp.where(first[1], q0, yin[0, 2 * f + 1])
        lo2 = jnp.where(first[1], q0, yin[0, 2 * f])
        hi0 = jnp.where(final[1], q63, yin[1, 2 * f])
        hi1 = jnp.where(final[1], q63, yin[1, 2 * f + 1])
        s0 = minmod(q0 - lo1, q1 - q0)
        s63 = minmod(q63 - q62, hi0 - q63)
        flux_0 = flux_row(v0, lo1, q0, minmod(lo1 - lo2, q0 - lo1), s0)
        flux_1 = flux_row(v1, q0, q1, s0, minmod(q1 - q0, q2 - q1))
        flux_63 = flux_row(v63, q62, q63, minmod(q62 - q61, q63 - q62), s63)
        flux_64 = flux_row(v64, q63, hi0, s63, minmod(hi0 - q63, hi1 - hi0))
        acc[f, :, 0, :] += flux_0 - flux_1
        acc[f, :, 1, :] += flux_1
        acc[f, :, 62, :] -= flux_63
        acc[f, :, 63, :] += flux_63 - flux_64

    wait_pair(zin, 2, zr_sem.at[0])

    def face(four, v):
        behind = back(four)
        diff = four - behind
        slope = minmod(diff, ahead(diff))
        flux = v * jnp.where(v > 0, behind, four) + half_weight(v) * jnp.where(
            v > 0, back(slope), slope
        )
        return slope, flux

    for half in range(2):
        own_v = zpack[10 + half]
        v_low = jnp.where(place4 == 2, own_v * low_scale[2], own_v)
        v_high = jnp.where(final[2], back(own_v) * flag_open[5], zin[1, 10 + half])
        left = jnp.minimum(v_low, 0.0)
        left_w = -0.5 * left * (1.0 + left)
        right = jnp.maximum(ahead(own_v), 0.0)
        right_w = 0.5 * right * (1.0 - right)
        for f in range(5):
            j = 2 * f + half
            own = zpack[j]
            ghost_low = jnp.where(place4 == 0, pltpu.roll(own, 126, 1), ahead(own))
            ghost_high = jnp.where(place4 == 2, back(own), pltpu.roll(own, 2, 1))
            low = jnp.where(place4 < 2, jnp.where(first[2], ghost_low, zin[0, j]), own)
            high = jnp.where(place4 < 2, own, jnp.where(final[2], ghost_high, zin[1, j]))
            slope_low, flux_low = face(low, v_low)
            slope_high, flux_high = face(high, v_high)
            by_left = left_w * jnp.where(place4 == 1, slope_high, slope_low)
            by_right = right_w * slope_low
            entering = jnp.where(v_low > 0, flux_low, 0.0)
            zcorr[j] = jnp.where(
                place4 == 0,
                -ahead(by_left),
                jnp.where(
                    place4 == 1,
                    by_left - ahead(flux_high) + ahead(left * own),
                    jnp.where(place4 == 2, entering + by_left - by_right, back(by_right)),
                ),
            )

    last_early = level == EARLY - 1
    copies_c = [
        remote(part.at[2], slots_b.at[0], ts_sem.at[1], tr_sem.at[1], along_yz(0, dz))
        for dz in range(1, 6)
    ]

    @pl.when(last_early)
    def _():
        wait_bytes(slots_b.at[pl.ds(0, 4 * EARLY - 1)], tr_sem.at[1])
        part[2] = jnp.sum(slots_b[: 4 * EARLY], axis=0)
        pl.semaphore_wait(round_sem.at[1], levels - EARLY)
        for copy in copies_c:
            copy.start()

    @pl.when(jnp.logical_not(final[0]))
    def _():
        face_copy.wait_recv()

    for i in range(9):
        if i == 0:
            v = disp[0, 0].astype(jnp.float32) * (STEP * low_scale[0])
        elif i < 8:
            v = disp[0, i].astype(jnp.float32) * STEP
        else:
            v_last = disp[0, 7].astype(jnp.float32) * (STEP * flag_open[1])
            v = jnp.where(final[0], v_last, xface[...].astype(jnp.float32) * STEP)
        vx[i] = v
        gx_w[i] = half_weight(v)

    inner = jnp.logical_not(jnp.logical_or(first[0], final[0]))
    edge_lanes = jnp.logical_or(lane8 < 2, lane8 > 125)
    for f in range(5):

        if f in (0, 3):
            group = pl.ds(f, 3 - f // 3)

            @pl.when(inner)
            def _():
                wait_bytes(xhalo.at[group], xr_sem.at[f // 3])

            @pl.when(jnp.logical_not(inner))
            def _():
                wait_bytes(xhalo.at[group, 0], xr_sem.at[f // 3])

        def tile(t, carry):
            part_rows = pl.ds(pl.multiple_of(t * 8, 8), 8)
            own = [q[f, i, part_rows] for i in range(8)]
            cell = (
                [jnp.where(first[0], own[0], xhalo[f, 0, r, part_rows]) for r in range(2)]
                + own
                + [jnp.where(final[0], own[7], xhalo[f, 1, r, part_rows]) for r in range(2)]
            )
            diff = [cell[i + 1] - cell[i] for i in range(11)]
            slope = [minmod(diff[i], diff[i + 1]) for i in range(10)]
            flux = []
            for i in range(9):
                v = vx[i, part_rows]
                g = gx_w[i, part_rows]
                flux.append(
                    v * jnp.where(v > 0, cell[i + 1], cell[i + 2])
                    + g * jnp.where(v > 0, slope[i], slope[i + 1])
                )
            for i in range(8):
                move = lax.rem(254 - 4 * ((i % 4) * 8 + t), 128)
                corr = pltpu.roll(zcorr[2 * f + i // 4], move, 1)
                corr = jnp.where(edge_lanes, corr, 0.0)
                acc[f, i, part_rows] += (flux[i] - flux[i + 1]) + corr
            return carry

        lax.fori_loop(0, 8, tile, 0)

    wait_bytes(slots_a, ts_sem.at[0])

    @pl.when(jnp.logical_not(first[0]))
    def _():
        face_copy.wait_send()

    wait_pair(yin, 1, ys_sem.at[0])
    wait_pair(zin, 2, zs_sem.at[0])

    @pl.when(inner)
    def _():
        wait_bytes(xhalo, xs_sem.at[0])

    @pl.when(jnp.logical_not(inner))
    def _():
        wait_bytes(xhalo.at[:, 0], xs_sem.at[0])

    not_root = jnp.logical_not(root)

    def wait_rows(when, count, sem):
        @pl.when(when)
        def _():
            wait_bytes(slots_d.at[pl.ds(0, count)], sem)

    wait_rows(level < EARLY - 1, 4 * EARLY - 1, ts_sem.at[1])
    wait_rows(last_early, 4 * EARLY + 4, ts_sem.at[1])
    columns = [(x, c) for _, x, _, c in ROOTS]
    for skip in sorted({columns.count((x, c)) for x in range(4) for c in range(2)}):
        wait_rows(both(late, skipped == skip), 31 - skip + len(ROOTS), ts_sem.at[1])
    wait_rows(level < EARLY - 1, 4 * EARLY - 1, tr_sem.at[1])
    wait_rows(both(early, not_root), 4 * (8 - EARLY), tr_sem.at[2])
    wait_rows(late, 1, tr_sem.at[1])
    wait_rows(late, 4 * (8 - EARLY) - 1, tr_sem.at[2])
    others = jnp.sum(slots_b[1 : 4 * EARLY], axis=0)
    near_sum = slots_b[0] + jnp.where(early, others, 0.0)

    @pl.when(root)
    def _():
        wait_bytes(slots_d, tr_sem.at[2])
        grand[...] = near_sum + row_sum(slots_d, 0, 160)

    @pl.when(not_root)
    def _():
        grand[...] = near_sum + row_sum(slots_b, 4 * EARLY, 4 * (8 - EARLY))


def write_out(cells, acc, grand, new_density, new_momentum, new_energy, totals, pair, sem):
    stores = [
        pltpu.make_async_copy(acc.at[0], new_density, sem.at[0]),
        pltpu.make_async_copy(acc.at[1], new_energy, sem.at[0]),
    ] + [pltpu.make_async_copy(acc.at[2 + c], new_momentum.at[c], sem.at[0]) for c in range(3)]
    for store in stores:
        store.start()
    lane1 = lax.broadcasted_iota(jnp.int32, (1, 128), 1)
    both = grand[...]
    pair[0] = jnp.sum(jnp.where(lane1 < 64, both, 0.0)) / cells
    pair[1] = jnp.sum(jnp.where(lane1 < 64, 0.0, both)) / cells
    last = pltpu.make_async_copy(pair, totals, sem.at[1])
    last.start()
    pltpu.make_async_copy(acc, acc, sem.at[0]).wait()
    last.wait()


def shards(cells, density, momentum, energy, displacement, flags):
    f32, i32 = jnp.float32, jnp.int32
    anywhere = pl.BlockSpec(memory_space=pltpu.HBM)
    local = pl.BlockSpec(memory_space=pltpu.VMEM)
    inputs = [
        pltpu.with_memory_space_constraint(a, pltpu.HBM)
        for a in (density, momentum, energy, displacement, flags)
    ]
    acc, grand = pl.pallas_call(
        kernel,
        out_shape=(
            jax.ShapeDtypeStruct((5, 8, 64, 128), f32),
            jax.ShapeDtypeStruct((1, 128), f32),
        ),
        in_specs=[anywhere] * 5,
        out_specs=(local, local),
        scratch_shapes=[
            pltpu.VMEM((5, 8, 64, 128), f32),
            pltpu.VMEM((3, 8, 64, 128), i32),
            pltpu.SMEM((6,), i32),
            pltpu.VMEM((9, 64, 128), f32),
            pltpu.VMEM((9, 64, 128), f32),
            pltpu.VMEM((5, 2, 2, 64, 128), f32),
            pltpu.VMEM((64, 128), i32),
            pltpu.VMEM((11, 8, 128), f32),
            pltpu.VMEM((11, 8, 128), f32),
            pltpu.VMEM((2, 11, 8, 128), f32),
            pltpu.VMEM((12, 8, 128), f32),
            pltpu.VMEM((2, 12, 8, 128), f32),
            pltpu.VMEM((10, 8, 128), f32),
            pltpu.VMEM((3, 1, 128), f32),
            pltpu.VMEM((7, 1, 128), f32),
            pltpu.VMEM((32, 1, 128), f32),
            pltpu.VMEM((160, 1, 128), f32),
            pltpu.SemaphoreType.DMA((3,)),
            pltpu.SemaphoreType.DMA((2,)),
            pltpu.SemaphoreType.DMA((3,)),
            pltpu.SemaphoreType.DMA((1,)),
            pltpu.SemaphoreType.DMA((1,)),
            pltpu.SemaphoreType.DMA((1,)),
            pltpu.SemaphoreType.DMA((1,)),
            pltpu.SemaphoreType.DMA((2,)),
            pltpu.SemaphoreType.DMA((3,)),
            pltpu.SemaphoreType.REGULAR((3,)),
        ],
        compiler_params=pltpu.CompilerParams(
            collective_id=0, has_side_effects=True, vmem_limit_bytes=16 * 2**20
        ),
        name="remap",
    )(*inputs)
    return pl.pallas_call(
        functools.partial(write_out, cells),
        out_shape=(
            jax.ShapeDtypeStruct(density.shape, f32),
            jax.ShapeDtypeStruct(momentum.shape, f32),
            jax.ShapeDtypeStruct(energy.shape, f32),
            jax.ShapeDtypeStruct((2,), f32),
        ),
        in_specs=[local, local],
        out_specs=[anywhere] * 4,
        scratch_shapes=[pltpu.SMEM((2,), f32), pltpu.SemaphoreType.DMA((2,))],
        compiler_params=pltpu.CompilerParams(vmem_limit_bytes=4 * 2**20),
        name="write_out",
    )(acc, grand)


def solution(mesh):
    cells = float(mesh.shape["gx"] * mesh.shape["gy"] * mesh.shape["gz"] * 8 * 64 * 128)
    block = P("gx", "gy", "gz")
    three = P(None, "gx", "gy", "gz")
    return jax.shard_map(
        functools.partial(shards, cells),
        mesh=mesh,
        in_specs=(block, three, block, three, P()),
        out_specs=(block, three, block, P()),
        check_vma=False,
    )
```

```python
import functools

import jax
import jax.numpy as jnp
from jax import lax
from jax.experimental import pallas as pl
from jax.experimental.pallas import tpu as pltpu
from jax.sharding import PartitionSpec as P

MESH = pl.DeviceIdType.MESH
STEP = 1.0 / 256.0
EARLY = 3
ROOTS = (
    (0, 0, 0, 1),
    (0, 1, 0, 0),
    (0, 0, 1, 0),
    (0, 2, 0, 0),
    (0, 3, 0, 0),
    (0, 0, 2, 0),
    (0, 0, 3, 0),
    (0, 0, 0, 0),
    (0, 1, 0, 1),
    (0, 2, 0, 1),
    (0, 1, 1, 0),
    (0, 0, 1, 1),
    (1, 0, 0, 0),
    (1, 0, 0, 1),
    (1, 1, 0, 0),
    (1, 0, 1, 0),
)


def minmod(left_diff, right_diff):
    least = jnp.minimum(left_diff, right_diff)
    most = jnp.maximum(left_diff, right_diff)
    return jnp.maximum(least, jnp.minimum(most, 0.0))


def half_weight(v):
    size = jnp.abs(v)
    return 0.5 * size * (1.0 - size)


def row_sum(rows, start, count):
    sums = [rows[start + i] for i in range(10)]
    for i in range(10, count):
        sums[i % 10] = sums[i % 10] + rows[start + i]
    while len(sums) > 1:
        paired = [sums[i] + sums[i + 1] for i in range(0, len(sums) - 1, 2)]
        sums = paired + sums[len(paired) * 2 :]
    return sums[0]


def back(block):
    return pltpu.roll(block, 1, 1)


def ahead(block):
    return pltpu.roll(block, 127, 1)


def kernel(
    density,
    momentum,
    energy,
    displacement,
    flags,
    acc,
    grand,
    q,
    disp,
    flag,
    vx,
    gx_w,
    xhalo,
    xface,
    yup,
    ydown,
    yin,
    zpack,
    zin,
    zcorr,
    part,
    slots_a,
    slots_b,
    slots_d,
    load_sem,
    xs_sem,
    xr_sem,
    ys_sem,
    yr_sem,
    zs_sem,
    zr_sem,
    ts_sem,
    tr_sem,
    round_sem,
):
    px, py, pz = lax.axis_index("gx"), lax.axis_index("gy"), lax.axis_index("gz")
    nx, ny, nz = lax.axis_size("gx"), lax.axis_size("gy"), lax.axis_size("gz")
    core = pz % 2
    zl = (pz // 2) % 2
    def wait_bytes(of, sem):
        pltpu.make_async_copy(of, of, sem).wait()

    def place(x=None, y=None, z=None):
        target = {}
        if x is not None:
            target["gx"] = x
        if y is not None:
            target["gy"] = y
        if z is not None:
            target["gz"] = z
        return target

    level = py * 2 + zl
    levels = 2 * ny
    early = level < EARLY
    both = jnp.logical_and
    late = jnp.logical_not(early)

    def along_yz(dy, dz):
        chip = lax.rem(level + dz, levels)
        return place(y=chip // 2, z=lax.rem(pz + 4 * dy, nz) + 2 * (chip % 2 - zl))

    def greet(sem, peer):
        pl.semaphore_signal(sem, inc=1, device_id=peer, device_id_type=MESH)

    stage_a = [
        place(x=lax.rem(px + dx, nx), z=pz + dc * (1 - 2 * core))
        for dx in (2, 1, 3, 0)
        for dc in range(2)
        if dx or dc
    ]
    along_y = [along_yz(dy, 0) for dy in (2, 1, 3)]
    steps = [-2, 2, -1, 1]
    late_step = [
        jnp.logical_and(level + step >= EARLY, level + step < levels) for step in steps
    ]
    late_steps = sum(ok.astype(jnp.int32) for ok in late_step)
    has_across = jnp.where(core == 1, pz < nz - 1, pz > 0)
    across = place(z=lax.rem(pz + nz + 2 * core - 1, nz))

    def greet_late(sem):
        for step, ok in zip(steps, late_step):

            @pl.when(ok)
            def _():
                greet(sem, along_yz(0, step % 8))

    flag_copy = pltpu.make_async_copy(flags, flag, load_sem.at[0])
    flag_copy.start()
    halves = [pl.ds(0, 4), pl.ds(4, 4)]
    for half in halves:
        pltpu.make_async_copy(density.at[half], q.at[0, half], load_sem.at[1]).start()
        pltpu.make_async_copy(energy.at[half], q.at[1, half], load_sem.at[1]).start()
    for a in range(3):
        for half in halves:
            pltpu.make_async_copy(
                displacement.at[a, half], disp.at[a, half], load_sem.at[1]
            ).start()
    momentum_load = pltpu.make_async_copy(momentum, q.at[pl.ds(2, 3)], load_sem.at[2])
    momentum_load.start()

    barrier = pltpu.get_barrier_semaphore()

    @pl.when(late)
    def _():
        greet_late(barrier)

    for peer in stage_a + along_y:
        greet(barrier, peer)

    @pl.when(has_across)
    def _():
        greet(barrier, across)

    me_y = pz // 4
    in_column = [both(px == x, core == c) for _, x, _, c in ROOTS]
    skipped = sum(ok.astype(jnp.int32) for ok in in_column)
    at_root = [
        both(ok, both(level == t, me_y == y)) for ok, (t, _, y, _) in zip(in_column, ROOTS)
    ]
    root = functools.reduce(jnp.logical_or, at_root)

    @pl.when(root)
    def _():
        def greet_group(k, carry):
            t = 7 - k // 4
            z = 4 * lax.rem(k, 4) + 2 * lax.rem(t, 2)
            for x in range(4):
                for c in range(2):
                    greet(barrier, place(x=x, y=t // 2, z=z + c))
            return carry

        lax.fori_loop(0, 4 * (8 - EARLY), greet_group, 0)

    @pl.when(early)
    def _():
        for dz in range(1, 8):

            @pl.when(level + dz < levels)
            def _():
                for dy in range(4):
                    greet(barrier, along_yz(dy, dz))


    flag_copy.wait()
    wait_bytes(q, load_sem.at[1])

    def wait_pair(buffer, axis, sem):
        one = jnp.logical_or(first[axis], final[axis])

        @pl.when(one)
        def _():
            wait_bytes(buffer.at[0], sem)

        @pl.when(jnp.logical_not(one))
        def _():
            wait_bytes(buffer, sem)

    flag_open = [flag[i].astype(jnp.float32) for i in range(6)]
    first = [px == 0, py == 0, pz == 0]
    final = [px == nx - 1, py == ny - 1, pz == nz - 1]
    low_scale = [jnp.where(first[a], flag_open[2 * a], 1.0) for a in range(3)]
    gain = [jnp.where(first[a], flag_open[2 * a] * STEP, 0.0) for a in range(3)]
    loss = [jnp.where(final[a], flag_open[2 * a + 1] * -STEP, 0.0) for a in range(3)]

    rows = lax.broadcasted_iota(jnp.int32, (64, 128), 0)
    lanes = lax.broadcasted_iota(jnp.int32, (64, 128), 1)
    weight_y = jnp.where(rows == 0, gain[1], jnp.where(rows == 63, loss[1], 0.0))
    weight_z = jnp.where(lanes == 0, gain[2], jnp.where(lanes == 127, loss[2], 0.0))

    def fold(block):
        return jnp.sum(block.reshape(8, 8, 128), axis=0)

    def plane_sum(x, sums):
        weight = (
            1.0
            + weight_y * disp[1, x].astype(jnp.float32)
            + weight_z * disp[2, x].astype(jnp.float32)
        )
        return (sums[0] + fold(q[0, x] * weight), sums[1] + fold(q[1, x] * weight))

    weight_low = gain[0] * disp[0, 0].astype(jnp.float32)
    weight_high = loss[0] * disp[0, 7].astype(jnp.float32)
    sums = tuple(fold(q[f, 0] * weight_low + q[f, 7] * weight_high) for f in (0, 1))
    sums = lax.fori_loop(0, 8, plane_sum, sums)
    lane1 = lax.broadcasted_iota(jnp.int32, (1, 128), 1)

    def halves(low, high):
        low = jnp.sum(low, axis=0, keepdims=True)
        high = jnp.sum(high, axis=0, keepdims=True)
        return jnp.where(lane1 < 64, low + pltpu.roll(low, 64, 1), high + pltpu.roll(high, 64, 1))

    part[0] = halves(*sums)

    greeted = (
        len(stage_a)
        + len(along_y)
        + has_across.astype(jnp.int32)
        + jnp.where(early, 0, len(ROOTS))
        + jnp.where(early, 4 * level, 4 * EARLY + late_steps)
    )
    pl.semaphore_wait(barrier, greeted)

    def remote(src, dst, send_sem, recv_sem, peer):
        return pltpu.make_async_remote_copy(
            src_ref=src,
            dst_ref=dst,
            send_sem=send_sem,
            recv_sem=recv_sem,
            device_id=peer,
            device_id_type=MESH,
        )

    copies_a = [
        remote(part.at[0], slots_a.at[i], ts_sem.at[0], tr_sem.at[0], peer)
        for i, peer in enumerate(stage_a)
    ]
    slot = level * 4 + pz // 4
    arrival = tr_sem.at[jnp.where(early, 1, 2)]
    base_z = pz - 4 * me_y - 2 * zl
    places = [(t, y) for t in range(8) for y in (0, 1, 3, 2)]
    copies_b = [
        remote(
            part.at[1],
            slots_b.at[slot],
            ts_sem.at[1],
            arrival,
            place(y=t // 2, z=base_z + 4 * y + 2 * (t % 2)),
        )
        for t, y in places
    ]

    def send_b(wanted):
        for (t, y), copy in zip(places, copies_b):
            ok = wanted(t)
            if ok is not None:
                other = jnp.logical_or(level != t, me_y != y)
                pl.when(jnp.logical_and(ok, other))(copy.start)
    index = (level - EARLY) * 32 + me_y * 8 + px * 2 + core
    to_roots = [
        remote(
            part.at[0],
            slots_d.at[index],
            ts_sem.at[1],
            tr_sem.at[2],
            place(x=x, y=t // 2, z=4 * y + 2 * (t % 2) + c),
        )
        for t, x, y, c in ROOTS
    ]

    @pl.when(late)
    def _():
        to_roots[0].start()

    for copy in copies_a:
        copy.start()

    @pl.when(late)
    def _():
        for copy in to_roots[1:]:
            copy.start()
        greet_late(round_sem.at[0])
        for peer in along_y:
            greet(round_sem.at[0], peer)

    for back_step in (1, 2):

        @pl.when(jnp.logical_and(level - back_step >= 0, level - back_step < EARLY))
        def _():
            greet(round_sem.at[0], along_yz(0, 8 - back_step))

    @pl.when(early)
    def _():
        for target in range(EARLY - 1):

            @pl.when(target < level)
            def _():
                for dy in range(4):
                    greet(round_sem.at[2], along_yz(dy, lax.rem(levels + target - level, levels)))

    @pl.when(jnp.logical_not(early))
    def _():
        greet(round_sem.at[1], along_yz(0, lax.rem(levels + EARLY - 1 - level, levels)))

    momentum_load.wait()
    x_next = place(x=lax.rem(px + 1, nx))
    x_prev = place(x=lax.rem(px + nx - 1, nx))
    face_copy = remote(disp.at[0, 0], xface, xs_sem.at[1], xr_sem.at[2], x_prev)
    up_copies = [
        remote(q.at[f, pl.ds(6, 2)], xhalo.at[f, 0], xs_sem.at[0], xr_sem.at[f // 3], x_next) for f in range(5)
    ]
    down_copies = [
        remote(q.at[f, pl.ds(0, 2)], xhalo.at[f, 1], xs_sem.at[0], xr_sem.at[f // 3], x_prev)
        for f in range(5)
    ]

    @pl.when(jnp.logical_not(first[0]))
    def _():
        face_copy.start()

    for f in range(5):

        @pl.when(jnp.logical_not(final[0]))
        def _():
            up_copies[f].start()

        @pl.when(jnp.logical_not(first[0]))
        def _():
            down_copies[f].start()

    for f in range(5):
        for r in range(2):
            yup[2 * f + r] = q[f, :, 62 + r, :]
            ydown[2 * f + r] = q[f, :, r, :]
    yup[10] = jnp.zeros((8, 128), jnp.float32)
    ydown[10] = disp[1, :, 0, :].astype(jnp.float32) * STEP

    y_up = remote(yup, yin.at[0], ys_sem.at[0], yr_sem.at[0], place(y=lax.rem(py + 1, ny)))
    y_down = remote(ydown, yin.at[1], ys_sem.at[0], yr_sem.at[0], place(y=lax.rem(py + ny - 1, ny)))

    @pl.when(jnp.logical_not(first[1]))
    def _():
        y_down.start()

    @pl.when(jnp.logical_not(jnp.logical_or(final[1], early)))
    def _():
        y_up.start()

    lane8 = lax.broadcasted_iota(jnp.int32, (8, 128), 1)
    slot_of = lane8 // 4
    place4 = lane8 % 4

    def pack(source, base, half):
        packed = jnp.zeros((8, 128), jnp.float32)
        for xx in range(4):
            plane = source[base, half * 4 + xx].astype(jnp.float32)
            for t in range(8):
                k = xx * 8 + t
                moved = pltpu.roll(plane[8 * t : 8 * t + 8], (4 * k + 2) % 128, 1)
                packed = jnp.where(slot_of == k, moved, packed)
        return packed

    for f in range(5):
        for half in range(2):
            zpack[2 * f + half] = pack(q, f, half)
    for half in range(2):
        zpack[10 + half] = pack(disp, 2, half) * STEP

    z_up = remote(zpack, zin.at[0], zs_sem.at[0], zr_sem.at[0], place(z=lax.rem(pz + 1, nz)))
    z_down = remote(zpack, zin.at[1], zs_sem.at[0], zr_sem.at[0], place(z=lax.rem(pz + nz - 1, nz)))

    @pl.when(jnp.logical_not(final[2]))
    def _():
        z_up.start()

    @pl.when(jnp.logical_not(first[2]))
    def _():
        z_down.start()

    scale_y = jnp.where(
        jnp.logical_or(rows < 2, rows == 63), 0.0, STEP
    )
    scale_z = jnp.where(lanes == 0, STEP * low_scale[2], STEP)

    def planes(x, carry):
        vy = disp[1, x].astype(jnp.float32) * scale_y
        gy = half_weight(vy)
        up_y = vy > 0
        vz = disp[2, x].astype(jnp.float32) * scale_z
        right = jnp.where(lanes == 127, 0.0, jnp.maximum(ahead(vz), 0.0))
        right_w = jnp.where(lanes == 0, 0.0, 0.5 * right * (1.0 - right))
        left = jnp.minimum(vz, 0.0)
        left_w = jnp.where(
            jnp.logical_or(lanes == 0, lanes == 127), 0.0, -0.5 * left * (1.0 + left)
        )
        for f in range(5):
            value = q[f, x]
            below = back(value)
            above = ahead(value)
            slope = minmod(value - below, above - value)
            out_right = right * value + right_w * slope
            out_left = left * value + left_w * slope
            change_z = (back(out_right) - out_right) + (out_left - ahead(out_left))

            below = pltpu.roll(value, 1, 0)
            diff = value - below
            slope = minmod(diff, pltpu.roll(diff, 63, 0))
            flux = vy * jnp.where(up_y, below, value) + gy * jnp.where(
                up_y, pltpu.roll(slope, 1, 0), slope
            )
            acc[f, x] = (value + (flux - pltpu.roll(flux, 63, 0))) + change_z
        return carry

    lax.fori_loop(0, 2, planes, 0)

    @pl.when(late)
    def _():
        pl.semaphore_wait(round_sem.at[0], len(along_y) + late_steps)
        greet_late(round_sem.at[1])
        for peer in along_y:
            greet(round_sem.at[1], peer)

    lax.fori_loop(2, 3, planes, 0)

    wait_bytes(slots_a, tr_sem.at[0])
    group = part[0] + jnp.sum(slots_a[...], axis=0)
    part[1] = group
    slots_b[slot] = group

    @pl.when(late)
    def _():
        for (t, y), copy in zip(places, copies_b):
            skip = [ok for ok, spot in zip(in_column, ROOTS) if spot[0] == t and spot[2] == y]
            if skip:
                pl.when(jnp.logical_not(functools.reduce(jnp.logical_or, skip)))(copy.start)
            elif t < EARLY:
                copy.start()
        send_b(lambda t: jnp.abs(level - t) < 3 if t >= EARLY else None)

    @pl.when(early)
    def _():
        send_b(lambda t: level >= t if t < EARLY else None)

    lax.fori_loop(3, 5, planes, 0)

    @pl.when(early)
    def _():
        pl.semaphore_wait(round_sem.at[0], 2)
        y_up.start()

    @pl.when(late)
    def _():
        pl.semaphore_wait(round_sem.at[1], len(along_y) + late_steps)
        send_b(lambda t: jnp.abs(level - t) > 2 if t >= EARLY else None)

    lax.fori_loop(5, 8, planes, 0)

    @pl.when(level < EARLY - 1)
    def _():
        pl.semaphore_wait(round_sem.at[2], 4 * (EARLY - 1 - level))
        send_b(lambda t: level < t if t < EARLY else None)

    wait_pair(yin, 1, yr_sem.at[0])

    v0, v1, v63 = [disp[1, :, r, :].astype(jnp.float32) * STEP for r in (0, 1, 63)]
    v64 = jnp.where(final[1], v63 * flag_open[3], yin[1, 10])
    v0 = v0 * low_scale[1]

    def flux_row(v, behind, at, slope_behind, slope_at):
        return v * jnp.where(v > 0, behind, at) + half_weight(v) * jnp.where(
            v > 0, slope_behind, slope_at
        )

    for f in range(5):
        q0, q1, q2, q61, q62, q63 = [q[f, :, r, :] for r in (0, 1, 2, 61, 62, 63)]
        lo1 = jnp.where(first[1], q0, yin[0, 2 * f + 1])
        lo2 = jnp.where(first[1], q0, yin[0, 2 * f])
        hi0 = jnp.where(final[1], q63, yin[1, 2 * f])
        hi1 = jnp.where(final[1], q63, yin[1, 2 * f + 1])
        s0 = minmod(q0 - lo1, q1 - q0)
        s63 = minmod(q63 - q62, hi0 - q63)
        flux_0 = flux_row(v0, lo1, q0, minmod(lo1 - lo2, q0 - lo1), s0)
        flux_1 = flux_row(v1, q0, q1, s0, minmod(q1 - q0, q2 - q1))
        flux_63 = flux_row(v63, q62, q63, minmod(q62 - q61, q63 - q62), s63)
        flux_64 = flux_row(v64, q63, hi0, s63, minmod(hi0 - q63, hi1 - hi0))
        acc[f, :, 0, :] += flux_0 - flux_1
        acc[f, :, 1, :] += flux_1
        acc[f, :, 62, :] -= flux_63
        acc[f, :, 63, :] += flux_63 - flux_64

    wait_pair(zin, 2, zr_sem.at[0])

    def face(four, v):
        behind = back(four)
        diff = four - behind
        slope = minmod(diff, ahead(diff))
        flux = v * jnp.where(v > 0, behind, four) + half_weight(v) * jnp.where(
            v > 0, back(slope), slope
        )
        return slope, flux

    for half in range(2):
        own_v = zpack[10 + half]
        v_low = jnp.where(place4 == 2, own_v * low_scale[2], own_v)
        v_high = jnp.where(final[2], back(own_v) * flag_open[5], zin[1, 10 + half])
        left = jnp.minimum(v_low, 0.0)
        left_w = -0.5 * left * (1.0 + left)
        right = jnp.maximum(ahead(own_v), 0.0)
        right_w = 0.5 * right * (1.0 - right)
        for f in range(5):
            j = 2 * f + half
            own = zpack[j]
            ghost_low = jnp.where(place4 == 0, pltpu.roll(own, 126, 1), ahead(own))
            ghost_high = jnp.where(place4 == 2, back(own), pltpu.roll(own, 2, 1))
            low = jnp.where(place4 < 2, jnp.where(first[2], ghost_low, zin[0, j]), own)
            high = jnp.where(place4 < 2, own, jnp.where(final[2], ghost_high, zin[1, j]))
            slope_low, flux_low = face(low, v_low)
            slope_high, flux_high = face(high, v_high)
            by_left = left_w * jnp.where(place4 == 1, slope_high, slope_low)
            by_right = right_w * slope_low
            entering = jnp.where(v_low > 0, flux_low, 0.0)
            zcorr[j] = jnp.where(
                place4 == 0,
                -ahead(by_left),
                jnp.where(
                    place4 == 1,
                    by_left - ahead(flux_high) + ahead(left * own),
                    jnp.where(place4 == 2, entering + by_left - by_right, back(by_right)),
                ),
            )

    last_early = level == EARLY - 1
    copies_c = [
        remote(part.at[2], slots_b.at[0], ts_sem.at[1], tr_sem.at[1], along_yz(0, dz))
        for dz in range(1, 6)
    ]

    @pl.when(last_early)
    def _():
        wait_bytes(slots_b.at[pl.ds(0, 4 * EARLY - 1)], tr_sem.at[1])
        part[2] = jnp.sum(slots_b[: 4 * EARLY], axis=0)
        pl.semaphore_wait(round_sem.at[1], levels - EARLY)
        for copy in copies_c:
            copy.start()

    @pl.when(jnp.logical_not(final[0]))
    def _():
        face_copy.wait_recv()

    for i in range(9):
        if i == 0:
            v = disp[0, 0].astype(jnp.float32) * (STEP * low_scale[0])
        elif i < 8:
            v = disp[0, i].astype(jnp.float32) * STEP
        else:
            v_last = disp[0, 7].astype(jnp.float32) * (STEP * flag_open[1])
            v = jnp.where(final[0], v_last, xface[...].astype(jnp.float32) * STEP)
        vx[i] = v
        gx_w[i] = half_weight(v)

    inner = jnp.logical_not(jnp.logical_or(first[0], final[0]))
    edge_lanes = jnp.logical_or(lane8 < 2, lane8 > 125)
    for f in range(5):

        if f in (0, 3):
            group = pl.ds(f, 3 - f // 3)

            @pl.when(inner)
            def _():
                wait_bytes(xhalo.at[group], xr_sem.at[f // 3])

            @pl.when(jnp.logical_not(inner))
            def _():
                wait_bytes(xhalo.at[group, 0], xr_sem.at[f // 3])

        def tile(t, carry):
            part_rows = pl.ds(pl.multiple_of(t * 8, 8), 8)
            own = [q[f, i, part_rows] for i in range(8)]
            cell = (
                [jnp.where(first[0], own[0], xhalo[f, 0, r, part_rows]) for r in range(2)]
                + own
                + [jnp.where(final[0], own[7], xhalo[f, 1, r, part_rows]) for r in range(2)]
            )
            diff = [cell[i + 1] - cell[i] for i in range(11)]
            slope = [minmod(diff[i], diff[i + 1]) for i in range(10)]
            flux = []
            for i in range(9):
                v = vx[i, part_rows]
                g = gx_w[i, part_rows]
                flux.append(
                    v * jnp.where(v > 0, cell[i + 1], cell[i + 2])
                    + g * jnp.where(v > 0, slope[i], slope[i + 1])
                )
            for i in range(8):
                move = lax.rem(254 - 4 * ((i % 4) * 8 + t), 128)
                corr = pltpu.roll(zcorr[2 * f + i // 4], move, 1)
                corr = jnp.where(edge_lanes, corr, 0.0)
                acc[f, i, part_rows] += (flux[i] - flux[i + 1]) + corr
            return carry

        lax.fori_loop(0, 8, tile, 0)

    wait_bytes(slots_a, ts_sem.at[0])

    @pl.when(jnp.logical_not(first[0]))
    def _():
        face_copy.wait_send()

    wait_pair(yin, 1, ys_sem.at[0])
    wait_pair(zin, 2, zs_sem.at[0])

    @pl.when(inner)
    def _():
        wait_bytes(xhalo, xs_sem.at[0])

    @pl.when(jnp.logical_not(inner))
    def _():
        wait_bytes(xhalo.at[:, 0], xs_sem.at[0])

    not_root = jnp.logical_not(root)

    def wait_rows(when, count, sem):
        @pl.when(when)
        def _():
            wait_bytes(slots_d.at[pl.ds(0, count)], sem)

    wait_rows(level < EARLY - 1, 4 * EARLY - 1, ts_sem.at[1])
    wait_rows(last_early, 4 * EARLY + 4, ts_sem.at[1])
    columns = [(x, c) for _, x, _, c in ROOTS]
    for skip in sorted({columns.count((x, c)) for x in range(4) for c in range(2)}):
        wait_rows(both(late, skipped == skip), 31 - skip + len(ROOTS), ts_sem.at[1])
    wait_rows(level < EARLY - 1, 4 * EARLY - 1, tr_sem.at[1])
    wait_rows(both(early, not_root), 4 * (8 - EARLY), tr_sem.at[2])
    wait_rows(late, 1, tr_sem.at[1])
    wait_rows(late, 4 * (8 - EARLY) - 1, tr_sem.at[2])
    others = jnp.sum(slots_b[1 : 4 * EARLY], axis=0)
    near_sum = slots_b[0] + jnp.where(early, others, 0.0)

    @pl.when(root)
    def _():
        wait_bytes(slots_d, tr_sem.at[2])
        grand[...] = near_sum + row_sum(slots_d, 0, 160)

    @pl.when(not_root)
    def _():
        grand[...] = near_sum + row_sum(slots_b, 4 * EARLY, 4 * (8 - EARLY))


def write_out(cells, acc, grand, new_density, new_momentum, new_energy, totals, pair, sem):
    stores = [
        pltpu.make_async_copy(acc.at[0], new_density, sem.at[0]),
        pltpu.make_async_copy(acc.at[1], new_energy, sem.at[0]),
    ] + [pltpu.make_async_copy(acc.at[2 + c], new_momentum.at[c], sem.at[0]) for c in range(3)]
    for store in stores:
        store.start()
    lane1 = lax.broadcasted_iota(jnp.int32, (1, 128), 1)
    both = grand[...]
    pair[0] = jnp.sum(jnp.where(lane1 < 64, both, 0.0)) / cells
    pair[1] = jnp.sum(jnp.where(lane1 < 64, 0.0, both)) / cells
    last = pltpu.make_async_copy(pair, totals, sem.at[1])
    last.start()
    pltpu.make_async_copy(acc, acc, sem.at[0]).wait()
    last.wait()


def shards(cells, density, momentum, energy, displacement, flags):
    f32, i32 = jnp.float32, jnp.int32
    anywhere = pl.BlockSpec(memory_space=pltpu.HBM)
    local = pl.BlockSpec(memory_space=pltpu.VMEM)
    inputs = [
        pltpu.with_memory_space_constraint(a, pltpu.HBM)
        for a in (density, momentum, energy, displacement, flags)
    ]
    acc, grand = pl.pallas_call(
        kernel,
        out_shape=(
            jax.ShapeDtypeStruct((5, 8, 64, 128), f32),
            jax.ShapeDtypeStruct((1, 128), f32),
        ),
        in_specs=[anywhere] * 5,
        out_specs=(local, local),
        scratch_shapes=[
            pltpu.VMEM((5, 8, 64, 128), f32),
            pltpu.VMEM((3, 8, 64, 128), i32),
            pltpu.SMEM((6,), i32),
            pltpu.VMEM((9, 64, 128), f32),
            pltpu.VMEM((9, 64, 128), f32),
            pltpu.VMEM((5, 2, 2, 64, 128), f32),
            pltpu.VMEM((64, 128), i32),
            pltpu.VMEM((11, 8, 128), f32),
            pltpu.VMEM((11, 8, 128), f32),
            pltpu.VMEM((2, 11, 8, 128), f32),
            pltpu.VMEM((12, 8, 128), f32),
            pltpu.VMEM((2, 12, 8, 128), f32),
            pltpu.VMEM((10, 8, 128), f32),
            pltpu.VMEM((3, 1, 128), f32),
            pltpu.VMEM((7, 1, 128), f32),
            pltpu.VMEM((32, 1, 128), f32),
            pltpu.VMEM((160, 1, 128), f32),
            pltpu.SemaphoreType.DMA((3,)),
            pltpu.SemaphoreType.DMA((2,)),
            pltpu.SemaphoreType.DMA((3,)),
            pltpu.SemaphoreType.DMA((1,)),
            pltpu.SemaphoreType.DMA((1,)),
            pltpu.SemaphoreType.DMA((1,)),
            pltpu.SemaphoreType.DMA((1,)),
            pltpu.SemaphoreType.DMA((2,)),
            pltpu.SemaphoreType.DMA((3,)),
            pltpu.SemaphoreType.REGULAR((3,)),
        ],
        compiler_params=pltpu.CompilerParams(
            collective_id=0, has_side_effects=True, vmem_limit_bytes=16 * 2**20
        ),
        name="remap",
    )(*inputs)
    return pl.pallas_call(
        functools.partial(write_out, cells),
        out_shape=(
            jax.ShapeDtypeStruct(density.shape, f32),
            jax.ShapeDtypeStruct(momentum.shape, f32),
            jax.ShapeDtypeStruct(energy.shape, f32),
            jax.ShapeDtypeStruct((2,), f32),
        ),
        in_specs=[local, local],
        out_specs=[anywhere] * 4,
        scratch_shapes=[pltpu.SMEM((2,), f32), pltpu.SemaphoreType.DMA((2,))],
        compiler_params=pltpu.CompilerParams(vmem_limit_bytes=4 * 2**20),
        name="write_out",
    )(acc, grand)


def solution(mesh):
    cells = float(mesh.shape["gx"] * mesh.shape["gy"] * mesh.shape["gz"] * 8 * 64 * 128)
    block = P("gx", "gy", "gz")
    three = P(None, "gx", "gy", "gz")
    return jax.shard_map(
        functools.partial(shards, cells),
        mesh=mesh,
        in_specs=(block, three, block, three, P()),
        out_specs=(block, three, block, P()),
        check_vma=False,
    )
```
